32 devices in a mesh: gx: 4 (over z), gy: 2 (over core), ta: 4 (over y, x).
Axes of the slice: x: 2, y: 2, z: 4, core: 2. Of those that a mesh axis runs over, the one named last changes fastest.
Arguments:
- links: float32 [4, 2, 3, 3, 8, 4, 4, 128], P(None, None, None, None, 'gx', 'gy', 'ta'), may hold values from -1 to 1, as said below
Outputs:
- flowed: float32 [4, 2, 3, 3, 8, 4, 4, 128], P(None, None, None, None, 'gx', 'gy', 'ta')
- action_slices: float32 [4], P('ta')
The draws below stay inside these ranges and needn't reach their ends.
Inputs may be any that keep to these rules, and one draw needn't show every extreme that they name: `links`: every link is a special unitary 3x3 matrix.
All inputs are finite; a program needn't handle non-finite values.
Results may differ from the reference program's by a relative error of at most 0.0003.
Values sent between devices are 32-bit elements; how exact they have to be, the bound alone decides.
A program may use at most 64 MiB of HBM per device.

```python
import jax
import jax.numpy as jnp
from jax import lax

NZ = 128
NX = 8
NY = 4
NT = 4


def complex_times(former, latter):
    return jnp.stack([former[0] * latter[0] - former[1] * latter[1], former[0] * latter[1] + former[1] * latter[0]])


def normalized(vector):
    length = jnp.sqrt(jnp.sum(vector[0] ** 2 + vector[1] ** 2, axis=0))
    return vector / length


def draw_links(key, part):
    raw = jax.random.normal(key, (2, 3, 3, 4, NX, NY, NT, NZ), jnp.float32)
    row_zero = normalized(raw[:, 0])
    second = raw[:, 1]
    inner_real = jnp.sum(row_zero[0] * second[0] + row_zero[1] * second[1], axis=0)
    inner_imag = jnp.sum(row_zero[0] * second[1] - row_zero[1] * second[0], axis=0)
    projection = jnp.stack([inner_real * row_zero[0] - inner_imag * row_zero[1], inner_real * row_zero[1] + inner_imag * row_zero[0]])
    row_one = normalized(second - projection)
    pieces = []
    for first_col, second_col in ((1, 2), (2, 0), (0, 1)):
        cross = complex_times(row_zero[:, first_col], row_one[:, second_col]) - complex_times(row_zero[:, second_col], row_one[:, first_col])
        pieces.append(jnp.stack([cross[0], -cross[1]]))
    row_two = jnp.stack(pieces, axis=1)
    matrix = jnp.stack([row_zero, row_one, row_two], axis=1)
    return jnp.moveaxis(matrix, 3, 0)


def setup_inputs(seed: int = 0) -> dict:
    key_list = jax.random.split(jax.random.key(seed), 2)
    links = draw_links(jax.random.fold_in(key_list[1], 71), 0)
    return {"links": links}


flow_eps = 0.1
taylor_order = 6


def contract(first_part, second_part):
    return jnp.sum(first_part[:, :, None] * second_part[None, :, :], axis=1)


def matmul_pair(former, latter):
    return jnp.stack([contract(former[0], latter[0]) - contract(former[1], latter[1]),
                      contract(former[0], latter[1]) + contract(former[1], latter[0])])


def adjoint(matrix):
    return jnp.stack([jnp.swapaxes(matrix[0], 0, 1), -jnp.swapaxes(matrix[1], 0, 1)])


def trace_real(former, latter):
    return jnp.sum(former[0] * jnp.swapaxes(latter[0], 0, 1) - former[1] * jnp.swapaxes(latter[1], 0, 1), axis=(0, 1))


def unit_offset(dir_index, sign):
    return tuple(sign if k == dir_index else 0 for k in range(4))


def add_offsets(first_off, second_off):
    return tuple(first_off[k] + second_off[k] for k in range(4))


def shifted(component, offset):
    x_len = component.shape[-4] - 2
    y_len = component.shape[-3] - 2
    t_len = component.shape[-2] - 2
    view = component[..., 1 + offset[0]:1 + offset[0] + x_len, 1 + offset[1]:1 + offset[1] + y_len,
                     1 + offset[2]:1 + offset[2] + t_len, :]
    if offset[3] != 0:
        view = jnp.roll(view, -offset[3], axis=-1)
    return view


def upper_staple(padded, mu_dir, nu_dir):
    here = (0, 0, 0, 0)
    first_pair = matmul_pair(shifted(padded[nu_dir], unit_offset(mu_dir, 1)),
                             adjoint(shifted(padded[mu_dir], unit_offset(nu_dir, 1))))
    return matmul_pair(first_pair, adjoint(shifted(padded[nu_dir], here)))


def lower_corner(padded, mu_dir, nu_dir):
    back = unit_offset(nu_dir, -1)
    corner = add_offsets(unit_offset(mu_dir, 1), back)
    first_pair = matmul_pair(adjoint(shifted(padded[nu_dir], corner)), adjoint(shifted(padded[mu_dir], back)))
    return matmul_pair(first_pair, shifted(padded[nu_dir], back))


def antihermitian(matrix):
    real_part = (matrix[0] - jnp.swapaxes(matrix[0], 0, 1)) / 2.0
    imag_part = (matrix[1] + jnp.swapaxes(matrix[1], 0, 1)) / 2.0
    trace_imag = jnp.trace(matrix[1], axis1=0, axis2=1) / 3.0
    eye = jnp.eye(3, dtype=jnp.float32).reshape((3, 3) + (1,) * (matrix.ndim - 3))
    return jnp.stack([real_part, imag_part - eye * trace_imag])


def flow_force(padded, lower_fn):
    centre = padded[..., 1:-1, 1:-1, 1:-1, :]
    forces = []
    action = jnp.zeros((centre.shape[6],), jnp.float32)
    for mu_dir in range(4):
        link_here = centre[mu_dir]
        staple_sum = jnp.zeros_like(link_here)
        for nu_dir in range(4):
            if nu_dir == mu_dir:
                continue
            upper = upper_staple(padded, mu_dir, nu_dir)
            action = action + jnp.sum(1.0 - trace_real(link_here, upper) / 3.0, axis=(0, 1, 3))
            staple_sum = staple_sum + upper + lower_fn(mu_dir, nu_dir)
        omega = matmul_pair(link_here, staple_sum)
        forces.append(-flow_eps * antihermitian(omega))
    return jnp.stack(forces), action / 2.0


def polynomial_exp(generator):
    eye = jnp.eye(3, dtype=jnp.float32).reshape((3, 3) + (1,) * (generator.ndim - 3))
    identity = jnp.stack([jnp.broadcast_to(eye, generator.shape[1:]), jnp.zeros(generator.shape[1:], jnp.float32)])
    result = identity
    for order in range(taylor_order, 0, -1):
        result = identity + matmul_pair(generator, result) / order
    return result


def advance(generator, links_now):
    def one_direction(gen_dir, link_dir):
        return matmul_pair(polynomial_exp(gen_dir), link_dir)
    return jax.vmap(one_direction)(generator, links_now)


def section_force(links_now):
    extended = jnp.concatenate([links_now[..., -1:, :], links_now, links_now[..., :1, :]], axis=6)

    def slice_force(t_index):
        block = lax.dynamic_slice_in_dim(extended, t_index, 3, axis=6)
        padded = jnp.concatenate([block[..., -1:, :, :, :], block, block[..., :1, :, :, :]], axis=4)
        padded = jnp.concatenate([padded[..., -1:, :, :], padded, padded[..., :1, :, :]], axis=5)

        def lower_fn(mu_dir, nu_dir):
            return lower_corner(padded, mu_dir, nu_dir)
        return flow_force(padded, lower_fn)

    forces, action = lax.map(slice_force, jnp.arange(NT, dtype=jnp.int32))
    forces = jnp.moveaxis(forces[..., 0, :], 0, 6)
    return forces, action.reshape((NT,))


def reference(links):
    force_zero, action = section_force(links)
    section_one = advance(force_zero / 4.0, links)
    force_one, unused_one = section_force(section_one)
    section_two = advance(8.0 / 9.0 * force_one - 17.0 / 36.0 * force_zero, section_one)
    force_two, unused_two = section_force(section_two)
    flowed = advance(3.0 / 4.0 * force_two - 8.0 / 9.0 * force_one + 17.0 / 36.0 * force_zero, section_two)
    action_slices = action / (6.0 * NX * NY * NZ)
    return flowed, action_slices
```

```python
import functools

import jax
import jax.numpy as jnp
from jax import lax
from jax.experimental import pallas as pl
from jax.experimental.pallas import tpu as pltpu
from jax.sharding import PartitionSpec as P

MESH = pl.DeviceIdType.MESH
AXES = ("gx", "gy", "ta")
flow_eps = 0.1
FRESH = (1.0 / 4.0, 8.0 / 9.0, 3.0 / 4.0)
KEPT = (0.0, -17.0 / 9.0, -1.0)


def mul(a, b):
    def dot(x, y):
        return sum(x[:, k][:, None] * y[k][None] for k in range(3))

    return dot(a[0], b[0]) - dot(a[1], b[1]), dot(a[0], b[1]) + dot(a[1], b[0])


def mul_right_adjoint(a, b):
    def dot(x, y):
        return sum(x[:, k][:, None] * y[:, k][None] for k in range(3))

    return dot(a[0], b[0]) + dot(a[1], b[1]), dot(a[1], b[0]) - dot(a[0], b[1])


def mul_left_adjoint(a, b):
    def dot(x, y):
        return sum(x[k][:, None] * y[k][None] for k in range(3))

    return dot(a[0], b[0]) + dot(a[1], b[1]), dot(a[0], b[1]) - dot(a[1], b[0])


def add(a, b):
    return b if a is None else (a[0] + b[0], a[1] + b[1])


def projected(m):
    r, i = m
    third = (i[0, 0] + i[1, 1] + i[2, 2]) / 3.0
    parts = [i[j, j] - third for j in range(2)]
    for j, k in ((0, 1), (0, 2), (1, 2)):
        parts += [(r[j, k] - r[k, j]) / 2.0, (i[j, k] + i[k, j]) / 2.0]
    return jnp.stack(parts)


def exponential(g):
    h = [g[0], g[1], -(g[0] + g[1])]
    u, v, w = (g[2], g[3]), (g[4], g[5]), (g[6], g[7])
    nu, nv, nw = (z[0] * z[0] + z[1] * z[1] for z in (u, v, w))
    uw = (u[0] * w[0] - u[1] * w[1], u[0] * w[1] + u[1] * w[0])
    diag = [h[0] * h[0] + nu + nv, h[1] * h[1] + nu + nw, h[2] * h[2] + nv + nw]
    p = -0.5 * (diag[0] + diag[1] + diag[2])
    det = (
        h[0] * (h[1] * h[2] - nw)
        - h[1] * nv
        - h[2] * nu
        + 2.0 * (uw[1] * v[0] - uw[0] * v[1])
    )
    s01, s02, s12 = h[0] + h[1], h[0] + h[2], h[1] + h[2]
    square = {
        (0, 1): (
            -s01 * u[1] - (v[0] * w[0] + v[1] * w[1]),
            s01 * u[0] - (v[1] * w[0] - v[0] * w[1]),
        ),
        (0, 2): (-s02 * v[1] + uw[0], s02 * v[0] + uw[1]),
        (1, 2): (
            -s12 * w[1] - (u[0] * v[0] + u[1] * v[1]),
            s12 * w[0] - (u[0] * v[1] - u[1] * v[0]),
        ),
    }
    line = {(0, 1): u, (0, 2): v, (1, 2): w}
    ai4, br4 = det * (-1.0 / 120.0), 0.25 + p * (1.0 / 120.0)
    ai3, br3, bi3, cr3 = (
        det * (-1.0 / 60.0),
        1.0 / 3.0 + p * (1.0 / 60.0),
        ai4 * (1.0 / 3.0),
        br4 * (1.0 / 3.0),
    )
    ai2, br2, bi2, cr2, ci2 = (
        det * cr3 * -0.5,
        0.5 + 0.5 * p * cr3,
        0.5 * ai3,
        0.5 * br3,
        0.5 * bi3,
    )
    ar, ai = 1.0 + det * ci2, -det * cr2
    br, bi, cr, ci = 1.0 + p * cr2, ai2 + p * ci2, br2, bi2
    re = [[None] * 3 for _ in range(3)]
    im = [[None] * 3 for _ in range(3)]
    for j in range(3):
        re[j][j] = ar - bi * h[j] - cr * diag[j]
        im[j][j] = ai + br * h[j] - ci * diag[j]
    for j, k in line:
        x, s = line[j, k], square[j, k]
        even_r, odd_r = br * x[0], bi * x[1]
        even_i, odd_i = br * x[1], bi * x[0]
        cs = (cr * s[0], ci * s[1], cr * s[1], ci * s[0])
        re[j][k] = (even_r - odd_r) + (cs[0] - cs[1])
        im[j][k] = (even_i + odd_i) + (cs[2] + cs[3])
        re[k][j] = -(even_r + odd_r) + (cs[0] + cs[1])
        im[k][j] = (even_i - odd_i) + (cs[3] - cs[2])
    return (
        jnp.stack([jnp.stack(row) for row in re]),
        jnp.stack([jnp.stack(row) for row in im]),
    )


def runs(pairs):
    out = []
    for to, frm in pairs:
        if out and to == out[-1][0] + out[-1][2] and frm == out[-1][1] + out[-1][2]:
            out[-1][2] += 1
        else:
            out.append([to, frm, 1])
    return out


def neighbour_rows(block, offset):
    lx, ly, lt = block
    found = {}
    for row in range(lx * ly * lt):
        site = (row // (ly * lt), row // lt % ly, row % lt)
        moved = [site[k] + offset[k] for k in range(3)]
        step = tuple(moved[k] // block[k] for k in range(3))
        at = [moved[k] % block[k] for k in range(3)]
        frm = (at[0] * ly + at[1]) * lt + at[2]
        found.setdefault(step, []).append((row, frm))
    return found


def unit(k, sign):
    return tuple(sign if j == k else 0 for j in range(3))


X, Y, T, Z = 0, 1, 2, 3
PLACE = {X: (0, 0), T: (0, 1), Y: (1, 0), Z: (1, 1)}
BEHIND = {T: 0, X: 3, Y: 7}
BOTH, T_AHEAD, X_AHEAD, Y_AHEAD = 5, 2, 6, 9
CORNER = {(X, T): (11, 0), (T, X): (11, 1), (X, Y): (12, 0), (T, Y): (12, 1), (Y, X): (13, 0), (Y, T): (13, 1)}
SLOTS = 14


def face_at(k, half, d):
    pair, pos = PLACE[d]
    if not half:
        return BEHIND[k] + pair, pos
    if k == Y:
        return Y_AHEAD + pair, pos
    if pair:
        return (X_AHEAD if k == X else T_AHEAD), pos
    return BOTH, int(k == X)


def cover(pairs):
    to, frm = min(pairs)
    assert all(a - b == to - frm for a, b in pairs)
    return to, frm, max(pairs)[0] - to + 1


def plan_of(block):
    rows = block[0] * block[1] * block[2]
    remote, fills = [], []

    def send(group, pair, pairs, frm, count, slot, to, step):
        remote.append((group, pair, pairs, frm, count, slot, to, step))

    for k in range(3):
        for half, sign in ((0, -1), (1, 1)):
            group = "xyt"[k]
            for step, pairs in neighbour_rows(block, unit(k, sign)).items():
                if any(step):
                    to, frm, n = cover(pairs)
                    if k == Y:
                        send(group, 0, 2, frm, rows + n, Y_AHEAD if half else BEHIND[Y], to, step)
                    elif k == X and half:
                        send(group, 0, 2, rows + frm, n, BOTH, rows + to, step)
                        send(group, 1, 1, frm, n, X_AHEAD, to, step)
                    elif k == X:
                        send(group, 0, 2, frm, n, BEHIND[X], to, step)
                        send(group, 0, 2, rows + frm, n, BEHIND[X], rows + to, step)
                    elif half:
                        send(group, 0, 1, frm, n, BOTH, to, step)
                        send(group, 1, 1, frm, rows + n, T_AHEAD, to, step)
                    else:
                        send(group, 0, 2, frm, rows + n, BEHIND[T], to, step)
                    continue
                for d in range(4):
                    if half and d == k:
                        continue
                    slot, pos = face_at(k, half, d)
                    pair, at = PLACE[d]
                    for to, frm, n in runs(pairs):
                        fills.append((group, None, pair, at * rows + frm, slot, pos * rows + to, n))
    for (m, n), (slot, pos) in CORNER.items():
        ahead, behind = unit(m, 1), unit(n, -1)
        rows_ahead = dict(neighbour_rows(block, ahead).get((0, 0, 0), []))
        rows_behind = dict(neighbour_rows(block, behind).get((0, 0, 0), []))
        offset = tuple(ahead[j] + behind[j] for j in range(3))
        group = "c" if Y in (m, n) else "xt"
        pair, at = PLACE[n]
        from_minus, from_plus = [], []
        for step, pairs in neighbour_rows(block, offset).items():
            outer = []
            for to, frm in pairs:
                if to in rows_ahead:
                    from_minus.append((to, rows_ahead[to]))
                elif to in rows_behind:
                    from_plus.append((to, rows_behind[to]))
                else:
                    outer.append((to, frm))
            if outer:
                to, frm, count = cover(outer)
                send(group, pair, 1, at * rows + frm, count, slot, pos * rows + to, step)
        for k, half, found in ((n, 0, from_minus), (m, 1, from_plus)):
            source, side = face_at(k, half, n)
            for to, frm, count in runs(sorted(found)):
                fills.append((group, source, 0, side * rows + frm, slot, pos * rows + to, count))
    remote.sort(key=lambda item: ("xt", "c", "t", "x", "y").index(item[0]))
    return remote, fills


def kernel(
    block,
    sizes,
    plan,
    partners,
    w_hbm,
    out_ref,
    act_ref,
    first_ref,
    cur_ref,
    halo_ref,
    gen_ref,
    gen_halo_ref,
    stack_ref,
    flux_ref,
    part_ref,
    slot_ref,
    send_sem,
    recv_sem,
    act_send,
    act_recv,
    load_sem,
):
    remote, fills = plan
    rows = block[0] * block[1] * block[2]
    lanes = w_hbm.shape[-1]
    loads = []
    for d, (pair, pos) in PLACE.items():
        load = pltpu.make_async_copy(
            w_hbm.at[d], first_ref.at[pair, :, :, :, pl.ds(pos * rows, rows), :], load_sem.at[d]
        )
        load.start()
        loads.append(load)
    here = [lax.axis_index(axis) for axis in AXES]

    def device(step):
        return tuple(lax.rem(here[k] + step[k] + sizes[k], sizes[k]) for k in range(3))

    steps = sorted({item[-1] for item in remote})
    greeted = steps + partners
    barrier = pltpu.get_barrier_semaphore()
    for step in greeted:
        pl.semaphore_signal(barrier, inc=1, device_id=device(step), device_id_type=MESH)
    pl.semaphore_wait(barrier, len(greeted))
    for load in loads:
        load.wait()

    started, action_copies, stacks = [], [], {}

    def low(pos):
        return slice(pos * rows, (pos + 1) * rows)

    def whole(ref, index):
        return ref[index, 0], ref[index, 1]

    def half(ref, index, pos):
        return ref[index, 0, :, :, low(pos), :], ref[index, 1, :, :, low(pos), :]

    def stack(name):
        return stacks.setdefault(name, len(stacks))

    def keep(name, value):
        index = stack(name)
        stack_ref[index, 0], stack_ref[index, 1] = value

    def keep_half(name, pos, value):
        index = stack(name)
        stack_ref[index, 0, :, :, low(pos), :] = value[0]
        stack_ref[index, 1, :, :, low(pos), :] = value[1]

    def twice(name, value):
        keep_half(name, 0, value)
        keep_half(name, 1, value)

    def kept(name):
        return whole(stack_ref, stacks[name])

    def kept_half(name, pos):
        return half(stack_ref, stacks[name], pos)

    def roll(pair, shift):
        return tuple(pltpu.roll(x, shift % lanes, axis=3) for x in pair)

    def face(k, side, d):
        slot, pos = face_at(k, side, d)
        return half(halo_ref, slot, pos)

    for stage in range(3):
        base = first_ref if stage == 0 else cur_ref
        copies = {}
        for j, (group, pair, pairs, frm, count, slot, to, step) in enumerate(remote):
            span, into = pl.ds(pair, pairs), pl.ds(slot, pairs)
            if stage == 0:
                src = first_ref.at[span, :, pl.ds(0, 2), :, pl.ds(frm, count), :]
                dst = halo_ref.at[into, :, pl.ds(0, 2), :, pl.ds(to, count), :]
            else:
                src = gen_ref.at[stage - 1, span, :, pl.ds(frm, count), :]
                dst = gen_halo_ref.at[stage - 1, into, :, pl.ds(to, count), :]
            copy = pltpu.make_async_remote_copy(
                src_ref=src,
                dst_ref=dst,
                send_sem=send_sem.at[stage, j],
                recv_sem=recv_sem.at[stage, j],
                device_id=device(tuple(-s for s in step)),
                device_id_type=MESH,
            )
            copy.start()
            copies.setdefault(group, []).append(copy)
            started.append(copy)

        if stage == 1:
            lt = block[2]
            for t in range(lt):
                part_ref[t : t + 1, :] = sum(action[r : r + 1] for r in range(t, rows, lt))
            mine = here[0] * sizes[1] + here[1]
            for j, step in enumerate(partners):
                copy = pltpu.make_async_remote_copy(
                    src_ref=part_ref,
                    dst_ref=slot_ref.at[mine],
                    send_sem=act_send.at[j],
                    recv_sem=act_recv.at[j],
                    device_id=device(step),
                    device_id_type=MESH,
                )
                copy.start()
                action_copies.append(copy)
            slot_ref[mine] = part_ref[...]

        def fill(wanted):
            for group, source, pair, frm, slot, to, n in fills:
                if group != wanted:
                    continue
                if stage == 0:
                    ref, index = (first_ref, pair) if source is None else (halo_ref, source)
                    halo_ref[slot, :, 0:2, :, to : to + n, :] = ref[index, :, 0:2, :, frm : frm + n, :]
                elif source is None:
                    gen_halo_ref[stage - 1, slot, :, to : to + n, :] = gen_ref[
                        stage - 1, pair, :, frm : frm + n, :
                    ]
                else:
                    gen_halo_ref[stage - 1, slot, :, to : to + n, :] = gen_halo_ref[
                        stage - 1, source, :, frm : frm + n, :
                    ]

        def renew(slot):
            if stage == 0:
                ref = halo_ref.at[slot]
                r, i = ref[0, 0:2], ref[1, 0:2]
                for j in range(3):
                    k, l = (j + 1) % 3, (j + 2) % 3
                    ref[0, 2, j] = (r[0, k] * r[1, l] - i[0, k] * i[1, l]) - (
                        r[0, l] * r[1, k] - i[0, l] * i[1, k]
                    )
                    ref[1, 2, j] = (r[0, l] * i[1, k] + i[0, l] * r[1, k]) - (
                        r[0, k] * i[1, l] + i[0, k] * r[1, l]
                    )
            else:
                new = mul(exponential(gen_halo_ref[stage - 1, slot]), whole(halo_ref, slot))
                halo_ref[slot, 0], halo_ref[slot, 1] = new

        def arrive(group, slots):
            for copy in copies[group]:
                copy.wait_recv()
            fill(group)
            for slot in slots:
                renew(slot)

        def count_action(plaq):
            trace = plaq[0][0, 0] + plaq[0][1, 1] + plaq[0][2, 2]
            term = 1.0 - trace / 3.0
            return term if term.shape[0] == rows else term[:rows] + term[rows:]

        action_terms = []

        def flux_of(one, two):
            plaq = mul_right_adjoint(one, two)
            if stage == 0:
                action_terms.append(count_action(plaq))
            return projected(plaq)

        def centre(d):
            return half(base, *PLACE[d])

        if stage:
            for pair in range(2):
                before = whole(first_ref if stage == 1 else cur_ref, pair)
                moved = mul(exponential(gen_ref[stage - 1, pair]), before)
                cur_ref[pair, 0], cur_ref[pair, 1] = moved
        for d, name in ((X, "x x"), (T, "t t"), (Z, "z z")):
            twice(name, centre(d))
        for d, name in ((X, "x ahead"), (T, "t ahead"), (Y, "y z ahead")):
            keep_half(name, 1, roll(centre(d), -1))

        arrive("y", range(BEHIND[Y], Y_AHEAD + 2))
        for d, name in ((X, "x ahead"), (T, "t ahead"), (Z, "y z ahead")):
            keep_half(name, 0, face(Y, 1, d))
        twice("y behind", face(Y, 0, Y))
        yz = whole(base, 1)
        keep("yx zx", mul(yz, kept("x ahead")))
        keep("yt zt", mul(yz, kept("t ahead")))
        keep("yz zy", mul(yz, kept("y z ahead")))
        one = kept_half("yz zy", 0)
        flux = flux_of(one, kept_half("yz zy", 1))
        flux_ref[1, :, low(0), :] = flux
        flux_ref[1, :, low(1), :] = -flux
        keep_half("lower b", 0, roll(mul_left_adjoint(one, centre(Z)), 1))
        behind = face(Y, 0, Y)
        one = mul(face(Y, 0, Z), roll(behind, -1))
        keep_half("lower b", 1, mul_left_adjoint(one, behind))

        arrive("t", (BEHIND[T], BEHIND[T] + 1, T_AHEAD))
        one = mul(kept("t t"), whole(halo_ref, T_AHEAD))
        keep("ty tz", one)
        flux_t = flux_of(one, kept("yt zt"))
        flux_ref[2] = flux_t
        keep_half("xz tz", 1, kept_half("ty tz", 1))
        behind = face(T, 0, T)
        twice("t behind", behind)
        keep_half("t corner", 1, roll(behind, -1))
        keep_half("behind n", 0, behind)
        keep_half("behind m", 0, face(T, 0, X))

        fill("x")
        for copy in copies["x"]:
            copy.wait_recv()
        for slot in (BEHIND[X], BEHIND[X] + 1, X_AHEAD, BOTH):
            renew(slot)
        one = mul(kept("x x"), whole(halo_ref, X_AHEAD))
        keep("xy xz", one)
        flux_x = flux_of(one, kept("yx zx"))
        flux_ref[3] = flux_x
        keep_half("xz tz", 0, kept_half("xy xz", 1))
        keep_half("t x", 0, half(halo_ref, BOTH, 1))
        keep_half("t x", 1, half(halo_ref, BOTH, 0))
        keep("xt tx", mul(whole(base, 0), kept("t x")))
        flux = flux_of(kept_half("xt tx", 0), kept_half("xt tx", 1))
        flux_ref[0, :, low(0), :] = flux_ref[3, :, low(0), :] + flux_ref[3, :, low(1), :] + flux
        flux_ref[0, :, low(1), :] = flux_ref[2, :, low(0), :] + flux_ref[2, :, low(1), :] - flux
        behind = face(X, 0, X)
        twice("x behind", behind)
        keep_half("x corner", 1, roll(behind, -1))
        keep_half("behind n", 1, behind)
        keep_half("behind m", 1, face(X, 0, T))
        lower_a = roll(mul_left_adjoint(kept("xz tz"), kept("z z")), 1)

        arrive("c", (12, 13))
        keep_half("x corner", 0, half(halo_ref, 13, 0))
        keep_half("t corner", 0, half(halo_ref, 13, 1))
        lower_b = kept("lower b")
        one = mul(whole(halo_ref, BEHIND[X] + 1), kept("x corner"))
        lower_b = add(lower_b, mul_left_adjoint(one, kept("x behind")))
        one = mul(whole(halo_ref, BEHIND[T] + 1), kept("t corner"))
        lower_b = add(lower_b, mul_left_adjoint(one, kept("t behind")))
        one = mul(whole(halo_ref, BEHIND[Y]), whole(halo_ref, 12))
        lower_a = add(lower_a, mul_left_adjoint(one, kept("y behind")))
        keep("lower a", lower_a)

        def finish(pair, lower, upper):
            own = whole(base, pair)
            omega = projected(mul(own, lower)) + upper
            gen = (-flow_eps * FRESH[stage]) * omega
            if stage:
                gen = gen + KEPT[stage] * gen_ref[stage - 1, pair]
            if stage < 2:
                gen_ref[stage, pair] = gen
            else:
                keep("moved %d" % pair, mul(exponential(gen), own))
                for d, (p, pos) in PLACE.items():
                    if p == pair:
                        out_ref[d, 0], out_ref[d, 1] = kept_half("moved %d" % pair, pos)

        finish(1, lower_b, flux_ref[1] - flux_ref[2] - flux_ref[3])
        arrive("xt", (11,))
        one = mul(kept("behind m"), whole(halo_ref, 11))
        lower_a = add(kept("lower a"), mul_left_adjoint(one, kept("behind n")))
        finish(0, lower_a, flux_ref[0])
        if stage == 0:
            action = sum(action_terms)
    assert len(stacks) <= stack_ref.shape[0]
    for copy in started:
        copy.wait_send()
    for copy in action_copies:
        copy.wait()
    total = sum(slot_ref[j] for j in range(sizes[0] * sizes[1]))
    scale = 1.0 / (6.0 * sizes[0] * sizes[1] * block[0] * block[1] * lanes)
    total = jnp.sum(total, axis=1, keepdims=True) * scale
    act_ref[...] = jnp.broadcast_to(total, act_ref.shape)


STACKS = 26
VMEM_LIMIT = 48 * 2**20


def solution(mesh):
    sizes = tuple(mesh.shape[axis] for axis in AXES)

    def local(links):
        block = links.shape[4:7]
        lanes = links.shape[7]
        rows = block[0] * block[1] * block[2]
        plan = plan_of(block)
        partners = [
            (i, j, 0) for i in range(sizes[0]) for j in range(sizes[1]) if i or j
        ]
        count = len(plan[0])
        matrix = (2, 3, 3, rows, lanes)
        both = (2, 3, 3, 2 * rows, lanes)
        f32 = jnp.float32
        vmem = pl.BlockSpec(memory_space=pltpu.VMEM)
        flowed, action = pl.pallas_call(
            functools.partial(kernel, block, sizes, plan, partners),
            out_shape=(
                jax.ShapeDtypeStruct((4,) + matrix, f32),
                jax.ShapeDtypeStruct((block[2], lanes), f32),
            ),
            in_specs=[pl.BlockSpec(memory_space=pltpu.HBM)],
            out_specs=(vmem, vmem),
            scratch_shapes=[
                pltpu.VMEM((2,) + both, f32),
                pltpu.VMEM((2,) + both, f32),
                pltpu.VMEM((SLOTS,) + both, f32),
                pltpu.VMEM((2, 2, 8, 2 * rows, lanes), f32),
                pltpu.VMEM((2, SLOTS, 8, 2 * rows, lanes), f32),
                pltpu.VMEM((STACKS,) + both, f32),
                pltpu.VMEM((4, 8, 2 * rows, lanes), f32),
                pltpu.VMEM((block[2], lanes), f32),
                pltpu.VMEM((sizes[0] * sizes[1], block[2], lanes), f32),
                pltpu.SemaphoreType.DMA((3, count)),
                pltpu.SemaphoreType.DMA((3, count)),
                pltpu.SemaphoreType.DMA((len(partners),)),
                pltpu.SemaphoreType.DMA((len(partners),)),
                pltpu.SemaphoreType.DMA((4,)),
            ],
            compiler_params=pltpu.CompilerParams(
                collective_id=0, has_side_effects=True, vmem_limit_bytes=VMEM_LIMIT
            ),
        )(links.reshape((4,) + matrix))
        return flowed.reshape(links.shape), action[:, 0]

    spec = P(None, None, None, None, "gx", "gy", "ta", None)
    return jax.shard_map(
        local, mesh=mesh, in_specs=(spec,), out_specs=(spec, P("ta")), check_vma=False
    )
```

```python
import functools

import jax
import jax.numpy as jnp
from jax import lax
from jax.experimental import pallas as pl
from jax.experimental.pallas import tpu as pltpu
from jax.sharding import PartitionSpec as P

MESH = pl.DeviceIdType.MESH
AXES = ("gx", "gy", "ta")
flow_eps = 0.1
FRESH = (1.0 / 4.0, 8.0 / 9.0, 3.0 / 4.0)
KEPT = (0.0, -17.0 / 9.0, -1.0)


def mul(a, b):
    def dot(x, y):
        return sum(x[:, k][:, None] * y[k][None] for k in range(3))

    return dot(a[0], b[0]) - dot(a[1], b[1]), dot(a[0], b[1]) + dot(a[1], b[0])


def mul_right_adjoint(a, b):
    def dot(x, y):
        return sum(x[:, k][:, None] * y[:, k][None] for k in range(3))

    return dot(a[0], b[0]) + dot(a[1], b[1]), dot(a[1], b[0]) - dot(a[0], b[1])


def mul_left_adjoint(a, b):
    def dot(x, y):
        return sum(x[k][:, None] * y[k][None] for k in range(3))

    return dot(a[0], b[0]) + dot(a[1], b[1]), dot(a[0], b[1]) - dot(a[1], b[0])


def add(a, b):
    return b if a is None else (a[0] + b[0], a[1] + b[1])


def projected(m):
    r, i = m
    third = (i[0, 0] + i[1, 1] + i[2, 2]) / 3.0
    parts = [i[j, j] - third for j in range(2)]
    for j, k in ((0, 1), (0, 2), (1, 2)):
        parts += [(r[j, k] - r[k, j]) / 2.0, (i[j, k] + i[k, j]) / 2.0]
    return jnp.stack(parts)


def exponential(g):
    h = [g[0], g[1], -(g[0] + g[1])]
    u, v, w = (g[2], g[3]), (g[4], g[5]), (g[6], g[7])
    nu, nv, nw = (z[0] * z[0] + z[1] * z[1] for z in (u, v, w))
    uw = (u[0] * w[0] - u[1] * w[1], u[0] * w[1] + u[1] * w[0])
    diag = [h[0] * h[0] + nu + nv, h[1] * h[1] + nu + nw, h[2] * h[2] + nv + nw]
    p = -0.5 * (diag[0] + diag[1] + diag[2])
    det = (
        h[0] * (h[1] * h[2] - nw)
        - h[1] * nv
        - h[2] * nu
        + 2.0 * (uw[1] * v[0] - uw[0] * v[1])
    )
    s01, s02, s12 = h[0] + h[1], h[0] + h[2], h[1] + h[2]
    square = {
        (0, 1): (
            -s01 * u[1] - (v[0] * w[0] + v[1] * w[1]),
            s01 * u[0] - (v[1] * w[0] - v[0] * w[1]),
        ),
        (0, 2): (-s02 * v[1] + uw[0], s02 * v[0] + uw[1]),
        (1, 2): (
            -s12 * w[1] - (u[0] * v[0] + u[1] * v[1]),
            s12 * w[0] - (u[0] * v[1] - u[1] * v[0]),
        ),
    }
    line = {(0, 1): u, (0, 2): v, (1, 2): w}
    ai4, br4 = det * (-1.0 / 120.0), 0.25 + p * (1.0 / 120.0)
    ai3, br3, bi3, cr3 = (
        det * (-1.0 / 60.0),
        1.0 / 3.0 + p * (1.0 / 60.0),
        ai4 * (1.0 / 3.0),
        br4 * (1.0 / 3.0),
    )
    ai2, br2, bi2, cr2, ci2 = (
        det * cr3 * -0.5,
        0.5 + 0.5 * p * cr3,
        0.5 * ai3,
        0.5 * br3,
        0.5 * bi3,
    )
    ar, ai = 1.0 + det * ci2, -det * cr2
    br, bi, cr, ci = 1.0 + p * cr2, ai2 + p * ci2, br2, bi2
    re = [[None] * 3 for _ in range(3)]
    im = [[None] * 3 for _ in range(3)]
    for j in range(3):
        re[j][j] = ar - bi * h[j] - cr * diag[j]
        im[j][j] = ai + br * h[j] - ci * diag[j]
    for j, k in line:
        x, s = line[j, k], square[j, k]
        even_r, odd_r = br * x[0], bi * x[1]
        even_i, odd_i = br * x[1], bi * x[0]
        cs = (cr * s[0], ci * s[1], cr * s[1], ci * s[0])
        re[j][k] = (even_r - odd_r) + (cs[0] - cs[1])
        im[j][k] = (even_i + odd_i) + (cs[2] + cs[3])
        re[k][j] = -(even_r + odd_r) + (cs[0] + cs[1])
        im[k][j] = (even_i - odd_i) + (cs[3] - cs[2])
    return (
        jnp.stack([jnp.stack(row) for row in re]),
        jnp.stack([jnp.stack(row) for row in im]),
    )


def chart(x, rest):
    length = sum(y * y for y in rest)
    first = jnp.where(length < 1e-30, 1e-15, rest[0])
    length = jnp.maximum(length, 1e-30)
    scale = jnp.where(x < 0.0, 1.0 - x, 1.0) / jnp.where(x < 0.0, length, 1.0 + x)
    return [scale * y for y in [first] + rest[1:]]


def frame(y):
    q = 2.0 / (1.0 + sum(v * v for v in y))
    return q, q / (1.0 + y[0] * y[0])


def encode(w):
    r, i = w
    y = chart(r[0, 0], [i[0, 0], r[0, 1], i[0, 1], r[0, 2], i[0, 2]])
    f = frame(y)[1]
    kr = r[1, 0] + y[0] * i[1, 0] + y[1] * r[1, 1] + y[2] * i[1, 1] + y[3] * r[1, 2] + y[4] * i[1, 2]
    ki = i[1, 0] - y[0] * r[1, 0] + y[1] * i[1, 1] - y[2] * r[1, 1] + y[3] * i[1, 2] - y[4] * r[1, 2]
    mr, mi = f * (kr + y[0] * ki), f * (ki - y[0] * kr)
    g = []
    for k in (1, 2):
        u, v = y[2 * k - 1], y[2 * k]
        g += [r[1, k] - (u * mr - v * mi), i[1, k] - (u * mi + v * mr)]
    return jnp.stack(y + chart(g[0], g[1:]))


def decode(code):
    y, z = [code[k] for k in range(5)], [code[k] for k in range(5, 8)]
    q, f = frame(y)
    t = 2.0 / (1.0 + sum(v * v for v in z))
    g = [t - 1.0] + [t * v for v in z]
    kr = y[1] * g[0] + y[2] * g[1] + y[3] * g[2] + y[4] * g[3]
    ki = y[1] * g[1] - y[2] * g[0] + y[3] * g[3] - y[4] * g[2]
    mr, mi = f * (kr - y[0] * ki), f * (ki + y[0] * kr)
    r = [[q - 1.0, q * y[1], q * y[3]], [y[0] * mi - mr]]
    i = [[q * y[0], q * y[2], q * y[4]], [-mi - y[0] * mr]]
    for k in (1, 2):
        u, v = y[2 * k - 1], y[2 * k]
        r[1].append(g[2 * k - 2] - (u * mr - v * mi))
        i[1].append(g[2 * k - 1] - (u * mi + v * mr))
    r.append([])
    i.append([])
    for j in range(3):
        k, l = (j + 1) % 3, (j + 2) % 3
        r[2].append(
            (r[0][k] * r[1][l] - i[0][k] * i[1][l]) - (r[0][l] * r[1][k] - i[0][l] * i[1][k])
        )
        i[2].append(
            (r[0][l] * i[1][k] + i[0][l] * r[1][k]) - (r[0][k] * i[1][l] + i[0][k] * r[1][l])
        )
    return (
        jnp.stack([jnp.stack(row) for row in r]),
        jnp.stack([jnp.stack(row) for row in i]),
    )


def runs(pairs):
    out = []
    for to, frm in pairs:
        if out and to == out[-1][0] + out[-1][2] and frm == out[-1][1] + out[-1][2]:
            out[-1][2] += 1
        else:
            out.append([to, frm, 1])
    return out


def neighbour_rows(block, offset):
    lx, ly, lt = block
    found = {}
    for row in range(lx * ly * lt):
        site = (row // (ly * lt), row // lt % ly, row % lt)
        moved = [site[k] + offset[k] for k in range(3)]
        step = tuple(moved[k] // block[k] for k in range(3))
        at = [moved[k] % block[k] for k in range(3)]
        frm = (at[0] * ly + at[1]) * lt + at[2]
        found.setdefault(step, []).append((row, frm))
    return found


def unit(k, sign):
    return tuple(sign if j == k else 0 for j in range(3))


X, Y, T, Z = 0, 1, 2, 3
PLACE = {X: (0, 0), T: (0, 1), Y: (1, 0), Z: (1, 1)}
BEHIND = {T: 0, X: 3, Y: 7}
BOTH, T_AHEAD, X_AHEAD, Y_AHEAD = 5, 2, 6, 9
CORNER = {(X, T): (11, 0), (T, X): (11, 1), (X, Y): (12, 0), (Y, X): (12, 1), (T, Y): (13, 0), (Y, T): (13, 1)}
SEND_ORDER = ("xt", "yt", "xy", "ahead", "behind a", "behind b", "x", "y")
SLOTS = 14


def face_at(k, half, d):
    pair, pos = PLACE[d]
    if not half:
        return BEHIND[k] + pair, pos
    if k == Y:
        return Y_AHEAD + pair, pos
    if pair:
        return (X_AHEAD if k == X else T_AHEAD), pos
    return BOTH, int(k == X)


def cover(pairs):
    to, frm = min(pairs)
    assert all(a - b == to - frm for a, b in pairs)
    return to, frm, max(pairs)[0] - to + 1


def plan_of(block):
    rows = block[0] * block[1] * block[2]
    remote, fills = [], []

    def send(group, pair, pairs, frm, count, slot, to, step):
        remote.append((group, pair, pairs, frm, count, slot, to, step))

    for k in range(3):
        for half, sign in ((0, -1), (1, 1)):
            group = "xy"[k] if k < T else "ahead"
            for step, pairs in neighbour_rows(block, unit(k, sign)).items():
                if any(step):
                    to, frm, n = cover(pairs)
                    if k == Y:
                        send(group, 0, 2, frm, rows + n, Y_AHEAD if half else BEHIND[Y], to, step)
                    elif k == X and half:
                        send(group, 0, 2, rows + frm, n, BOTH, rows + to, step)
                        send(group, 1, 1, frm, n, X_AHEAD, to, step)
                    elif k == X:
                        send(group, 0, 2, frm, n, BEHIND[X], to, step)
                        send(group, 0, 2, rows + frm, n, BEHIND[X], rows + to, step)
                    elif half:
                        send(group, 0, 1, frm, n, BOTH, to, step)
                        send(group, 1, 1, frm, rows + n, T_AHEAD, to, step)
                    else:
                        send("behind a", 0, 1, frm, rows + n, BEHIND[T], to, step)
                        send("behind b", 1, 1, frm, rows + n, BEHIND[T] + 1, to, step)
                    continue
                for d in range(4):
                    if half and d == k:
                        continue
                    slot, pos = face_at(k, half, d)
                    pair, at = PLACE[d]
                    if k == T and not half:
                        group = "behind b" if pair else "behind a"
                    for to, frm, n in runs(pairs):
                        fills.append((group, None, pair, at * rows + frm, slot, pos * rows + to, n))
    for (m, n), (slot, pos) in CORNER.items():
        ahead, behind = unit(m, 1), unit(n, -1)
        rows_ahead = dict(neighbour_rows(block, ahead).get((0, 0, 0), []))
        rows_behind = dict(neighbour_rows(block, behind).get((0, 0, 0), []))
        offset = tuple(ahead[j] + behind[j] for j in range(3))
        group = "xt" if Y not in (m, n) else "yt" if T in (m, n) else "xy"
        pair, at = PLACE[n]
        from_minus, from_plus = [], []
        for step, pairs in neighbour_rows(block, offset).items():
            outer = []
            for to, frm in pairs:
                if to in rows_ahead:
                    from_minus.append((to, rows_ahead[to]))
                elif to in rows_behind:
                    from_plus.append((to, rows_behind[to]))
                else:
                    outer.append((to, frm))
            if outer:
                to, frm, count = cover(outer)
                send(group, pair, 1, at * rows + frm, count, slot, pos * rows + to, step)
        for k, half, found in ((n, 0, from_minus), (m, 1, from_plus)):
            source, side = face_at(k, half, n)
            for to, frm, count in runs(sorted(found)):
                fills.append((group, source, 0, side * rows + frm, slot, pos * rows + to, count))
    remote.sort(key=lambda item: SEND_ORDER.index(item[0]))
    return remote, fills


def kernel(
    block,
    sizes,
    plan,
    partners,
    w_hbm,
    out_ref,
    act_ref,
    first_ref,
    cur_ref,
    halo_ref,
    gen_ref,
    gen_halo_ref,
    stack_ref,
    flux_ref,
    part_ref,
    slot_ref,
    send_sem,
    recv_sem,
    act_send,
    act_recv,
    load_sem,
):
    remote, fills = plan
    rows = block[0] * block[1] * block[2]
    lanes = w_hbm.shape[-1]
    loads = []
    for d, (pair, pos) in PLACE.items():
        load = pltpu.make_async_copy(
            w_hbm.at[d], first_ref.at[pair, :, :, :, pl.ds(pos * rows, rows), :], load_sem.at[d]
        )
        load.start()
        loads.append(load)
    here = [lax.axis_index(axis) for axis in AXES]

    def device(step):
        return tuple(lax.rem(here[k] + step[k] + sizes[k], sizes[k]) for k in range(3))

    steps = sorted({item[-1] for item in remote})
    greeted = steps + partners
    barrier = pltpu.get_barrier_semaphore()
    for step in greeted:
        pl.semaphore_signal(barrier, inc=1, device_id=device(step), device_id_type=MESH)
    for load in loads:
        load.wait()
    for pair in range(2):
        gen_ref[0, pair] = encode((first_ref[pair, 0], first_ref[pair, 1]))
    pl.semaphore_wait(barrier, len(greeted))

    last = lax.rem(here[1], 2) == 1
    started, action_copies, stacks = [], [], {}

    def low(pos):
        return slice(pos * rows, (pos + 1) * rows)

    def whole(ref, index):
        return ref[index, 0], ref[index, 1]

    def half(ref, index, pos):
        return ref[index, 0, :, :, low(pos), :], ref[index, 1, :, :, low(pos), :]

    def stack(name):
        return stacks.setdefault(name, len(stacks))

    def keep(name, value):
        index = stack(name)
        stack_ref[index, 0], stack_ref[index, 1] = value

    def keep_half(name, pos, value):
        index = stack(name)
        stack_ref[index, 0, :, :, low(pos), :] = value[0]
        stack_ref[index, 1, :, :, low(pos), :] = value[1]

    def twice(name, value):
        keep_half(name, 0, value)
        keep_half(name, 1, value)

    def kept(name):
        return whole(stack_ref, stacks[name])

    def kept_half(name, pos):
        return half(stack_ref, stacks[name], pos)

    def roll(pair, shift):
        return tuple(pltpu.roll(x, shift % lanes, axis=3) for x in pair)

    def face(k, side, d):
        slot, pos = face_at(k, side, d)
        return half(halo_ref, slot, pos)

    for stage in range(3):
        base = first_ref if stage == 0 else cur_ref
        copies, held = {}, []
        for j, (group, pair, pairs, frm, count, slot, to, step) in enumerate(remote):
            span, into = pl.ds(pair, pairs), pl.ds(slot, pairs)
            src = gen_ref.at[stage, span, :, pl.ds(frm, count), :]
            dst = gen_halo_ref.at[stage, into, :, pl.ds(to, count), :]
            copy = pltpu.make_async_remote_copy(
                src_ref=src,
                dst_ref=dst,
                send_sem=send_sem.at[stage, j],
                recv_sem=recv_sem.at[stage, j],
                device_id=device(tuple(-s for s in step)),
                device_id_type=MESH,
            )
            copies.setdefault(group, []).append(copy)
            started.append(copy)
            if stage in HELD and group in HELD_GROUPS:
                pl.when(jnp.logical_not(last))(copy.start)
                held.append(copy)
            else:
                copy.start()

        if stage == 1:
            lt = block[2]
            for t in range(lt):
                part_ref[t : t + 1, :] = sum(action[r : r + 1] for r in range(t, rows, lt))
            mine = here[0] * sizes[1] + here[1]
            for j, step in enumerate(partners):
                copy = pltpu.make_async_remote_copy(
                    src_ref=part_ref,
                    dst_ref=slot_ref.at[mine],
                    send_sem=act_send.at[j],
                    recv_sem=act_recv.at[j],
                    device_id=device(step),
                    device_id_type=MESH,
                )
                copy.start()
                action_copies.append(copy)
            slot_ref[mine] = part_ref[...]

        def fill(wanted):
            for group, source, pair, frm, slot, to, n in fills:
                if group != wanted:
                    continue
                ref = gen_ref.at[stage, pair] if source is None else gen_halo_ref.at[stage, source]
                gen_halo_ref[stage, slot, :, to : to + n, :] = ref[:, frm : frm + n, :]

        def renew(slot):
            code = gen_halo_ref[stage, slot]
            if stage == 0:
                new = decode(code)
            else:
                new = mul(exponential(code), whole(halo_ref, slot))
            halo_ref[slot, 0], halo_ref[slot, 1] = new

        def arrive(group, slots):
            if group != "y":
                for copy in copies[group]:
                    copy.wait_recv()
            if group not in ("x", "xy", "yt", "xt"):
                fill(group)
            for slot in slots:
                renew(slot)

        def count_action(plaq):
            trace = plaq[0][0, 0] + plaq[0][1, 1] + plaq[0][2, 2]
            term = 1.0 - trace / 3.0
            return term if term.shape[0] == rows else term[:rows] + term[rows:]

        action_terms = []

        def flux_of(one, two):
            plaq = mul_right_adjoint(one, two)
            if stage == 0:
                action_terms.append(count_action(plaq))
            return projected(plaq)

        def centre(d):
            return half(base, *PLACE[d])

        if stage:
            for pair in range(2):
                before = whole(first_ref if stage == 1 else cur_ref, pair)
                moved = mul(exponential(gen_ref[stage, pair]), before)
                cur_ref[pair, 0], cur_ref[pair, 1] = moved
        for d, name in ((X, "x x"), (T, "t t"), (Z, "z z")):
            twice(name, centre(d))
        for d, name in ((X, "x ahead"), (T, "t ahead"), (Y, "y z ahead")):
            keep_half(name, 1, roll(centre(d), -1))

        for copy in copies["y"]:
            copy.wait_recv()
        if held:

            @pl.when(last)
            def _():
                for copy in held:
                    copy.start()

        arrive("y", range(BEHIND[Y], Y_AHEAD + 2))
        for d, name in ((X, "x ahead"), (T, "t ahead"), (Z, "y z ahead")):
            keep_half(name, 0, face(Y, 1, d))
        behind = face(Y, 0, Y)
        twice("y behind", behind)
        yz = whole(base, 1)
        keep("yx zx", mul(yz, kept("x ahead")))
        keep("yt zt", mul(yz, kept("t ahead")))
        keep("yz zy", mul(yz, kept("y z ahead")))
        one = kept_half("yz zy", 0)
        flux = flux_of(one, kept_half("yz zy", 1))
        flux_ref[1, :, low(0), :] = flux
        flux_ref[1, :, low(1), :] = -flux
        keep_half("lower b", 0, roll(mul_left_adjoint(one, centre(Z)), 1))
        one = mul(face(Y, 0, Z), roll(behind, -1))
        keep_half("lower b", 1, mul_left_adjoint(one, behind))

        fill("x")

        def sum_into(name, value):
            keep(name, add(kept(name) if name in begun else None, value))
            begun.add(name)

        begun = {"lower b"}

        def x_faces():
            for slot in (BEHIND[X], BEHIND[X] + 1, X_AHEAD):
                renew(slot)
            keep("xy xz", mul(kept("x x"), whole(halo_ref, X_AHEAD)))
            flux_ref[3] = flux_of(kept("xy xz"), kept("yx zx"))
            keep_half("xz tz", 0, kept_half("xy xz", 1))
            behind = face(X, 0, X)
            twice("x behind", behind)
            keep_half("x corner", 1, roll(behind, -1))
            keep_half("behind n", 1, behind)
            keep_half("behind m", 1, face(X, 0, T))

        def t_ahead():
            renew(T_AHEAD)
            keep("ty tz", mul(kept("t t"), whole(halo_ref, T_AHEAD)))
            flux_ref[2] = flux_of(kept("ty tz"), kept("yt zt"))
            keep_half("xz tz", 1, kept_half("ty tz", 1))

        def x_and_t_ahead():
            renew(BOTH)
            keep_half("t x", 0, half(halo_ref, BOTH, 1))
            keep_half("t x", 1, half(halo_ref, BOTH, 0))
            keep("xt tx", mul(whole(base, 0), kept("t x")))
            flux = flux_of(kept_half("xt tx", 0), kept_half("xt tx", 1))
            flux_ref[0, :, low(0), :] = flux_ref[3, :, low(0), :] + flux_ref[3, :, low(1), :] + flux
            flux_ref[0, :, low(1), :] = flux_ref[2, :, low(0), :] + flux_ref[2, :, low(1), :] - flux
            flux_ref[1] = flux_ref[1] - flux_ref[2] - flux_ref[3]
            sum_into("lower a", roll(mul_left_adjoint(kept("xz tz"), kept("z z")), 1))

        def xy_corner():
            fill("xy")
            renew(12)
            keep_half("y corner", 0, half(halo_ref, 12, 0))
            keep_half("x corner", 0, half(halo_ref, 12, 1))
            one = mul(whole(halo_ref, BEHIND[X] + 1), kept("x corner"))
            sum_into("lower b", mul_left_adjoint(one, kept("x behind")))

        def t_behind():
            renew(BEHIND[T])
            behind = face(T, 0, T)
            twice("t behind", behind)
            keep_half("t corner", 1, roll(behind, -1))
            keep_half("behind n", 0, behind)
            keep_half("behind m", 0, face(T, 0, X))

        def yt_corner():
            fill("yt")
            renew(13)
            keep_half("y corner", 1, half(halo_ref, 13, 0))
            keep_half("t corner", 0, half(halo_ref, 13, 1))

        def y_lower():
            one = mul(whole(halo_ref, BEHIND[Y]), kept("y corner"))
            sum_into("lower a", mul_left_adjoint(one, kept("y behind")))

        def t_lower():
            renew(BEHIND[T] + 1)
            one = mul(whole(halo_ref, BEHIND[T] + 1), kept("t corner"))
            sum_into("lower b", mul_left_adjoint(one, kept("t behind")))

        def xt_lower():
            fill("xt")
            renew(11)
            one = mul(kept("behind m"), whole(halo_ref, 11))
            sum_into("lower a", mul_left_adjoint(one, kept("behind n")))

        def finish(pair, name):
            own = whole(base, pair)
            omega = projected(mul(own, kept(name))) + flux_ref[pair]
            gen = (-flow_eps * FRESH[stage]) * omega
            if stage:
                gen = gen + KEPT[stage] * gen_ref[stage, pair]
            if stage < 2:
                gen_ref[stage + 1, pair] = gen
            else:
                keep("moved", mul(exponential(gen), own))
                for d, (p, pos) in PLACE.items():
                    if p == pair:
                        out_ref[d, 0], out_ref[d, 1] = kept_half("moved", pos)

        tasks = [
            (x_faces, {"x"}),
            (t_ahead, {"ahead"}),
            (x_and_t_ahead, {"x", "ahead"}),
            (xy_corner, {"x", "xy"}),
            (t_behind, {"behind a"}),
            (yt_corner, {"yt", "ahead", "behind a"}),
            (y_lower, {"x", "xy", "yt", "ahead", "behind a"}),
            (t_lower, {"behind a", "behind b", "yt", "ahead"}),
            (lambda: finish(1, "lower b"), {"x", "xy", "ahead", "behind a", "behind b", "yt"}),
            (xt_lower, {"xt", "x", "ahead", "behind a"}),
            (lambda: finish(0, "lower a"), {"x", "xy", "ahead", "behind a", "yt", "xt"}),
        ]
        here_now = set()
        for groups in ORDER[stage]:
            for group in groups:
                arrive(group, ())
                here_now.add(group)
            ready = [task for task, needs in tasks if needs <= here_now]
            tasks = [(task, needs) for task, needs in tasks if not needs <= here_now]
            for task in ready:
                task()
        assert not tasks
        if stage == 0:
            action = sum(action_terms)
    assert len(stacks) <= stack_ref.shape[0]
    for copy in started:
        copy.wait_send()
    for copy in action_copies:
        copy.wait()
    total = sum(slot_ref[j] for j in range(sizes[0] * sizes[1]))
    scale = 1.0 / (6.0 * sizes[0] * sizes[1] * block[0] * block[1] * lanes)
    total = jnp.sum(total, axis=1, keepdims=True) * scale
    act_ref[...] = jnp.broadcast_to(total, act_ref.shape)


STACKS = 26
HELD = ()
STEPS = (("ahead",), ("x", "xy"), ("behind a", "yt"), ("behind b",), ("xt",))
ORDER = (STEPS, STEPS, STEPS)
HELD_GROUPS = ("ahead", "behind a", "behind b")
VMEM_LIMIT = 48 * 2**20


def solution(mesh):
    sizes = tuple(mesh.shape[axis] for axis in AXES)

    def local(links):
        block = links.shape[4:7]
        lanes = links.shape[7]
        rows = block[0] * block[1] * block[2]
        plan = plan_of(block)
        partners = [
            (i, j, 0) for i in range(sizes[0]) for j in range(sizes[1]) if i or j
        ]
        count = len(plan[0])
        matrix = (2, 3, 3, rows, lanes)
        both = (2, 3, 3, 2 * rows, lanes)
        f32 = jnp.float32
        vmem = pl.BlockSpec(memory_space=pltpu.VMEM)
        flowed, action = pl.pallas_call(
            functools.partial(kernel, block, sizes, plan, partners),
            out_shape=(
                jax.ShapeDtypeStruct((4,) + matrix, f32),
                jax.ShapeDtypeStruct((block[2], lanes), f32),
            ),
            in_specs=[pl.BlockSpec(memory_space=pltpu.HBM)],
            out_specs=(vmem, vmem),
            scratch_shapes=[
                pltpu.VMEM((2,) + both, f32),
                pltpu.VMEM((2,) + both, f32),
                pltpu.VMEM((SLOTS,) + both, f32),
                pltpu.VMEM((3, 2, 8, 2 * rows, lanes), f32),
                pltpu.VMEM((3, SLOTS, 8, 2 * rows, lanes), f32),
                pltpu.VMEM((STACKS,) + both, f32),
                pltpu.VMEM((4, 8, 2 * rows, lanes), f32),
                pltpu.VMEM((block[2], lanes), f32),
                pltpu.VMEM((sizes[0] * sizes[1], block[2], lanes), f32),
                pltpu.SemaphoreType.DMA((3, count)),
                pltpu.SemaphoreType.DMA((3, count)),
                pltpu.SemaphoreType.DMA((len(partners),)),
                pltpu.SemaphoreType.DMA((len(partners),)),
                pltpu.SemaphoreType.DMA((4,)),
            ],
            compiler_params=pltpu.CompilerParams(
                collective_id=0, has_side_effects=True, vmem_limit_bytes=VMEM_LIMIT
            ),
        )(links.reshape((4,) + matrix))
        return flowed.reshape(links.shape), action[:, 0]

    spec = P(None, None, None, None, "gx", "gy", "ta", None)
    return jax.shard_map(
        local, mesh=mesh, in_specs=(spec,), out_specs=(spec, P("ta")), check_vma=False
    )
```

```python
import functools

import jax
import jax.numpy as jnp
from jax import lax
from jax.experimental import pallas as pl
from jax.experimental.pallas import tpu as pltpu
from jax.sharding import PartitionSpec as P

MESH = pl.DeviceIdType.MESH
AXES = ("gx", "gy", "ta")
flow_eps = 0.1
FRESH = (1.0 / 4.0, 8.0 / 9.0, 3.0 / 4.0)
KEPT = (0.0, -17.0 / 9.0, -1.0)


def mul(a, b):
    def dot(x, y):
        return sum(x[:, k][:, None] * y[k][None] for k in range(3))

    return dot(a[0], b[0]) - dot(a[1], b[1]), dot(a[0], b[1]) + dot(a[1], b[0])


def mul_right_adjoint(a, b):
    def dot(x, y):
        return sum(x[:, k][:, None] * y[:, k][None] for k in range(3))

    return dot(a[0], b[0]) + dot(a[1], b[1]), dot(a[1], b[0]) - dot(a[0], b[1])


def mul_left_adjoint(a, b):
    def dot(x, y):
        return sum(x[k][:, None] * y[k][None] for k in range(3))

    return dot(a[0], b[0]) + dot(a[1], b[1]), dot(a[0], b[1]) - dot(a[1], b[0])


def add(a, b):
    return b if a is None else (a[0] + b[0], a[1] + b[1])


def projected(m):
    r, i = m
    third = (i[0, 0] + i[1, 1] + i[2, 2]) / 3.0
    parts = [i[j, j] - third for j in range(2)]
    for j, k in ((0, 1), (0, 2), (1, 2)):
        parts += [(r[j, k] - r[k, j]) / 2.0, (i[j, k] + i[k, j]) / 2.0]
    return jnp.stack(parts)


def exponential(g):
    h = [g[0], g[1], -(g[0] + g[1])]
    u, v, w = (g[2], g[3]), (g[4], g[5]), (g[6], g[7])
    nu, nv, nw = (z[0] * z[0] + z[1] * z[1] for z in (u, v, w))
    uw = (u[0] * w[0] - u[1] * w[1], u[0] * w[1] + u[1] * w[0])
    diag = [h[0] * h[0] + nu + nv, h[1] * h[1] + nu + nw, h[2] * h[2] + nv + nw]
    p = -0.5 * (diag[0] + diag[1] + diag[2])
    det = (
        h[0] * (h[1] * h[2] - nw)
        - h[1] * nv
        - h[2] * nu
        + 2.0 * (uw[1] * v[0] - uw[0] * v[1])
    )
    s01, s02, s12 = h[0] + h[1], h[0] + h[2], h[1] + h[2]
    square = {
        (0, 1): (
            -s01 * u[1] - (v[0] * w[0] + v[1] * w[1]),
            s01 * u[0] - (v[1] * w[0] - v[0] * w[1]),
        ),
        (0, 2): (-s02 * v[1] + uw[0], s02 * v[0] + uw[1]),
        (1, 2): (
            -s12 * w[1] - (u[0] * v[0] + u[1] * v[1]),
            s12 * w[0] - (u[0] * v[1] - u[1] * v[0]),
        ),
    }
    line = {(0, 1): u, (0, 2): v, (1, 2): w}
    ai4, br4 = det * (-1.0 / 120.0), 0.25 + p * (1.0 / 120.0)
    ai3, br3, bi3, cr3 = (
        det * (-1.0 / 60.0),
        1.0 / 3.0 + p * (1.0 / 60.0),
        ai4 * (1.0 / 3.0),
        br4 * (1.0 / 3.0),
    )
    ai2, br2, bi2, cr2, ci2 = (
        det * cr3 * -0.5,
        0.5 + 0.5 * p * cr3,
        0.5 * ai3,
        0.5 * br3,
        0.5 * bi3,
    )
    ar, ai = 1.0 + det * ci2, -det * cr2
    br, bi, cr, ci = 1.0 + p * cr2, ai2 + p * ci2, br2, bi2
    re = [[None] * 3 for _ in range(3)]
    im = [[None] * 3 for _ in range(3)]
    for j in range(3):
        re[j][j] = ar - bi * h[j] - cr * diag[j]
        im[j][j] = ai + br * h[j] - ci * diag[j]
    for j, k in line:
        x, s = line[j, k], square[j, k]
        even_r, odd_r = br * x[0], bi * x[1]
        even_i, odd_i = br * x[1], bi * x[0]
        cs = (cr * s[0], ci * s[1], cr * s[1], ci * s[0])
        re[j][k] = (even_r - odd_r) + (cs[0] - cs[1])
        im[j][k] = (even_i + odd_i) + (cs[2] + cs[3])
        re[k][j] = -(even_r + odd_r) + (cs[0] + cs[1])
        im[k][j] = (even_i - odd_i) + (cs[3] - cs[2])
    return (
        jnp.stack([jnp.stack(row) for row in re]),
        jnp.stack([jnp.stack(row) for row in im]),
    )


def chart(x, rest):
    length = sum(y * y for y in rest)
    first = jnp.where(length < 1e-30, 1e-15, rest[0])
    length = jnp.maximum(length, 1e-30)
    scale = jnp.where(x < 0.0, 1.0 - x, 1.0) / jnp.where(x < 0.0, length, 1.0 + x)
    return [scale * y for y in [first] + rest[1:]]


def frame(y):
    q = 2.0 / (1.0 + sum(v * v for v in y))
    return q, q / (1.0 + y[0] * y[0])


def encode(w):
    r, i = w
    y = chart(r[0, 0], [i[0, 0], r[0, 1], i[0, 1], r[0, 2], i[0, 2]])
    f = frame(y)[1]
    kr = r[1, 0] + y[0] * i[1, 0] + y[1] * r[1, 1] + y[2] * i[1, 1] + y[3] * r[1, 2] + y[4] * i[1, 2]
    ki = i[1, 0] - y[0] * r[1, 0] + y[1] * i[1, 1] - y[2] * r[1, 1] + y[3] * i[1, 2] - y[4] * r[1, 2]
    mr, mi = f * (kr + y[0] * ki), f * (ki - y[0] * kr)
    g = []
    for k in (1, 2):
        u, v = y[2 * k - 1], y[2 * k]
        g += [r[1, k] - (u * mr - v * mi), i[1, k] - (u * mi + v * mr)]
    return jnp.stack(y + chart(g[0], g[1:]))


def decode(code):
    y, z = [code[k] for k in range(5)], [code[k] for k in range(5, 8)]
    q, f = frame(y)
    t = 2.0 / (1.0 + sum(v * v for v in z))
    g = [t - 1.0] + [t * v for v in z]
    kr = y[1] * g[0] + y[2] * g[1] + y[3] * g[2] + y[4] * g[3]
    ki = y[1] * g[1] - y[2] * g[0] + y[3] * g[3] - y[4] * g[2]
    mr, mi = f * (kr - y[0] * ki), f * (ki + y[0] * kr)
    r = [[q - 1.0, q * y[1], q * y[3]], [y[0] * mi - mr]]
    i = [[q * y[0], q * y[2], q * y[4]], [-mi - y[0] * mr]]
    for k in (1, 2):
        u, v = y[2 * k - 1], y[2 * k]
        r[1].append(g[2 * k - 2] - (u * mr - v * mi))
        i[1].append(g[2 * k - 1] - (u * mi + v * mr))
    r.append([])
    i.append([])
    for j in range(3):
        k, l = (j + 1) % 3, (j + 2) % 3
        r[2].append(
            (r[0][k] * r[1][l] - i[0][k] * i[1][l]) - (r[0][l] * r[1][k] - i[0][l] * i[1][k])
        )
        i[2].append(
            (r[0][l] * i[1][k] + i[0][l] * r[1][k]) - (r[0][k] * i[1][l] + i[0][k] * r[1][l])
        )
    return (
        jnp.stack([jnp.stack(row) for row in r]),
        jnp.stack([jnp.stack(row) for row in i]),
    )


def runs(pairs):
    out = []
    for to, frm in pairs:
        if out and to == out[-1][0] + out[-1][2] and frm == out[-1][1] + out[-1][2]:
            out[-1][2] += 1
        else:
            out.append([to, frm, 1])
    return out


def neighbour_rows(block, offset):
    lx, ly, lt = block
    found = {}
    for row in range(lx * ly * lt):
        site = (row // (ly * lt), row // lt % ly, row % lt)
        moved = [site[k] + offset[k] for k in range(3)]
        step = tuple(moved[k] // block[k] for k in range(3))
        at = [moved[k] % block[k] for k in range(3)]
        frm = (at[0] * ly + at[1]) * lt + at[2]
        found.setdefault(step, []).append((row, frm))
    return found


def unit(k, sign):
    return tuple(sign if j == k else 0 for j in range(3))


X, Y, T, Z = 0, 1, 2, 3
PLACE = {X: (0, 0), T: (0, 1), Y: (1, 0), Z: (1, 1)}
BEHIND = {T: 0, X: 3, Y: 7}
BOTH, T_AHEAD, X_AHEAD, Y_AHEAD = 5, 2, 6, 9
CORNER = {(X, T): (11, 0), (T, X): (11, 1), (X, Y): (12, 0), (Y, X): (12, 1), (T, Y): (13, 0), (Y, T): (13, 1)}
SEND_ORDER = ("xt", "yt", "xy", "ahead", "behind a", "behind b", "x", "y")
SLOTS = 14


def face_at(k, half, d):
    pair, pos = PLACE[d]
    if not half:
        return BEHIND[k] + pair, pos
    if k == Y:
        return Y_AHEAD + pair, pos
    if pair:
        return (X_AHEAD if k == X else T_AHEAD), pos
    return BOTH, int(k == X)


def cover(pairs):
    to, frm = min(pairs)
    assert all(a - b == to - frm for a, b in pairs)
    return to, frm, max(pairs)[0] - to + 1


def plan_of(block):
    rows = block[0] * block[1] * block[2]
    remote, fills = [], []

    def send(group, pair, pairs, frm, count, slot, to, step):
        remote.append((group, pair, pairs, frm, count, slot, to, step))

    for k in range(3):
        for half, sign in ((0, -1), (1, 1)):
            group = "xy"[k] if k < T else "ahead"
            for step, pairs in neighbour_rows(block, unit(k, sign)).items():
                if any(step):
                    to, frm, n = cover(pairs)
                    if k == Y:
                        send(group, 0, 2, frm, rows + n, Y_AHEAD if half else BEHIND[Y], to, step)
                    elif k == X and half:
                        send(group, 0, 2, rows + frm, n, BOTH, rows + to, step)
                        send(group, 1, 1, frm, n, X_AHEAD, to, step)
                    elif k == X:
                        send(group, 0, 2, frm, n, BEHIND[X], to, step)
                        send(group, 0, 2, rows + frm, n, BEHIND[X], rows + to, step)
                    elif half:
                        send(group, 0, 1, frm, n, BOTH, to, step)
                        send(group, 1, 1, frm, rows + n, T_AHEAD, to, step)
                    else:
                        send("behind a", 0, 1, frm, rows + n, BEHIND[T], to, step)
                        send("behind b", 1, 1, frm, rows + n, BEHIND[T] + 1, to, step)
                    continue
                for d in range(4):
                    if half and d == k:
                        continue
                    slot, pos = face_at(k, half, d)
                    pair, at = PLACE[d]
                    if k == T and not half:
                        group = "behind b" if pair else "behind a"
                    for to, frm, n in runs(pairs):
                        fills.append((group, None, pair, at * rows + frm, slot, pos * rows + to, n))
    for (m, n), (slot, pos) in CORNER.items():
        ahead, behind = unit(m, 1), unit(n, -1)
        rows_ahead = dict(neighbour_rows(block, ahead).get((0, 0, 0), []))
        rows_behind = dict(neighbour_rows(block, behind).get((0, 0, 0), []))
        offset = tuple(ahead[j] + behind[j] for j in range(3))
        group = "xt" if Y not in (m, n) else "yt" if T in (m, n) else "xy"
        pair, at = PLACE[n]
        from_minus, from_plus = [], []
        for step, pairs in neighbour_rows(block, offset).items():
            outer = []
            for to, frm in pairs:
                if to in rows_ahead:
                    from_minus.append((to, rows_ahead[to]))
                elif to in rows_behind:
                    from_plus.append((to, rows_behind[to]))
                else:
                    outer.append((to, frm))
            if outer:
                to, frm, count = cover(outer)
                send(group, pair, 1, at * rows + frm, count, slot, pos * rows + to, step)
        for k, half, found in ((n, 0, from_minus), (m, 1, from_plus)):
            source, side = face_at(k, half, n)
            for to, frm, count in runs(sorted(found)):
                fills.append((group, source, 0, side * rows + frm, slot, pos * rows + to, count))
    remote.sort(key=lambda item: SEND_ORDER.index(item[0]))
    return remote, fills


def kernel(
    block,
    sizes,
    plan,
    partners,
    w_hbm,
    out_ref,
    act_ref,
    first_ref,
    cur_ref,
    halo_ref,
    gen_ref,
    gen_halo_ref,
    stack_ref,
    flux_ref,
    part_ref,
    slot_ref,
    send_sem,
    recv_sem,
    act_sem,
    load_sem,
):
    remote, fills = plan
    rows = block[0] * block[1] * block[2]
    lanes = w_hbm.shape[-1]
    for d, (pair, pos) in PLACE.items():
        load = pltpu.make_async_copy(
            w_hbm.at[d], first_ref.at[pair, :, :, :, pl.ds(pos * rows, rows), :], load_sem.at[0]
        )
        load.start()
    here = [lax.axis_index(axis) for axis in AXES]

    def device(step):
        return tuple(lax.rem(here[k] + step[k] + sizes[k], sizes[k]) for k in range(3))

    steps = sorted({item[-1] for item in remote})
    greeted = steps + partners
    barrier = pltpu.get_barrier_semaphore()
    for step in greeted:
        pl.semaphore_signal(barrier, inc=1, device_id=device(step), device_id_type=MESH)
    pltpu.make_async_copy(first_ref, first_ref, load_sem.at[0]).wait()
    for pair in range(2):
        gen_ref[0, pair] = encode((first_ref[pair, 0], first_ref[pair, 1]))
    pl.semaphore_wait(barrier, len(greeted))

    units, stacks = {}, {}

    def wait_bytes(count, sem):
        depth = max(k for k in range(1, 2 * rows + 1) if count % k == 0 and count // k <= SLOTS)
        span = gen_halo_ref.at[0, pl.ds(0, count // depth), :, pl.ds(0, depth), :]
        pltpu.make_async_copy(span, span, sem).wait()

    def wait_sent(units):
        for group, count in units.items():
            wait_bytes(count, send_sem.at[SEND_ORDER.index(group)])


    def low(pos):
        return slice(pos * rows, (pos + 1) * rows)

    def whole(ref, index):
        return ref[index, 0], ref[index, 1]

    def half(ref, index, pos):
        return ref[index, 0, :, :, low(pos), :], ref[index, 1, :, :, low(pos), :]

    def stack(name):
        return stacks.setdefault(name, len(stacks))

    def keep(name, value):
        index = stack(name)
        stack_ref[index, 0], stack_ref[index, 1] = value

    def keep_half(name, pos, value):
        index = stack(name)
        stack_ref[index, 0, :, :, low(pos), :] = value[0]
        stack_ref[index, 1, :, :, low(pos), :] = value[1]

    def twice(name, value):
        keep_half(name, 0, value)
        keep_half(name, 1, value)

    def kept(name):
        return whole(stack_ref, stacks[name])

    def kept_half(name, pos):
        return half(stack_ref, stacks[name], pos)

    def roll(pair, shift):
        return tuple(pltpu.roll(x, shift % lanes, axis=3) for x in pair)

    def face(k, side, d):
        slot, pos = face_at(k, side, d)
        return half(halo_ref, slot, pos)

    for stage in range(3):
        base = first_ref if stage == 0 else cur_ref
        wait_sent(units)
        units = {}
        for group, pair, pairs, frm, count, slot, to, step in remote:
            span, into = pl.ds(pair, pairs), pl.ds(slot, pairs)
            src = gen_ref.at[stage, span, :, pl.ds(frm, count), :]
            dst = gen_halo_ref.at[stage, into, :, pl.ds(to, count), :]
            copy = pltpu.make_async_remote_copy(
                src_ref=src,
                dst_ref=dst,
                send_sem=send_sem.at[SEND_ORDER.index(group)],
                recv_sem=recv_sem.at[stage % 2, SEND_ORDER.index(group)],
                device_id=device(tuple(-s for s in step)),
                device_id_type=MESH,
            )
            units[group] = units.get(group, 0) + pairs * count
            copy.start()

        if stage == 1:
            lt = block[2]
            for t in range(lt):
                part_ref[t : t + 1, :] = sum(action[r : r + 1] for r in range(t, rows, lt))
            mine = here[0] * sizes[1] + here[1]
            for step in partners:
                copy = pltpu.make_async_remote_copy(
                    src_ref=part_ref,
                    dst_ref=slot_ref.at[mine],
                    send_sem=act_sem.at[0],
                    recv_sem=act_sem.at[1],
                    device_id=device(step),
                    device_id_type=MESH,
                )
                copy.start()
            slot_ref[mine] = part_ref[...]

        def fill(wanted):
            for group, source, pair, frm, slot, to, n in fills:
                if group != wanted:
                    continue
                ref = gen_ref.at[stage, pair] if source is None else gen_halo_ref.at[stage, source]
                gen_halo_ref[stage, slot, :, to : to + n, :] = ref[:, frm : frm + n, :]

        def renew(slot):
            code = gen_halo_ref[stage, slot]
            if stage == 0:
                new = decode(code)
            else:
                new = mul(exponential(code), whole(halo_ref, slot))
            halo_ref[slot, 0], halo_ref[slot, 1] = new

        def arrive(group, slots):
            if group in units:
                wait_bytes(units[group], recv_sem.at[stage % 2, SEND_ORDER.index(group)])
            if group not in ("x", "xy", "yt", "xt"):
                fill(group)
            for slot in slots:
                renew(slot)

        def count_action(plaq):
            trace = plaq[0][0, 0] + plaq[0][1, 1] + plaq[0][2, 2]
            term = 1.0 - trace / 3.0
            return term if term.shape[0] == rows else term[:rows] + term[rows:]

        action_terms = []

        def flux_of(one, two):
            plaq = mul_right_adjoint(one, two)
            if stage == 0:
                action_terms.append(count_action(plaq))
            return projected(plaq)

        def centre(d):
            return half(base, *PLACE[d])

        if stage:
            for pair in range(2):
                before = whole(first_ref if stage == 1 else cur_ref, pair)
                moved = mul(exponential(gen_ref[stage, pair]), before)
                cur_ref[pair, 0], cur_ref[pair, 1] = moved
        for d, name in ((X, "x x"), (T, "t t"), (Z, "z z")):
            twice(name, centre(d))
        for d, name in ((X, "x ahead"), (T, "t ahead"), (Y, "y z ahead")):
            keep_half(name, 1, roll(centre(d), -1))

        arrive("y", range(BEHIND[Y], Y_AHEAD + 2))
        for d, name in ((X, "x ahead"), (T, "t ahead"), (Z, "y z ahead")):
            keep_half(name, 0, face(Y, 1, d))
        behind = face(Y, 0, Y)
        twice("y behind", behind)
        yz = whole(base, 1)
        keep("yx zx", mul(yz, kept("x ahead")))
        keep("yt zt", mul(yz, kept("t ahead")))
        keep("yz zy", mul(yz, kept("y z ahead")))
        one = kept_half("yz zy", 0)
        flux = flux_of(one, kept_half("yz zy", 1))
        flux_ref[1, :, low(0), :] = flux
        flux_ref[1, :, low(1), :] = -flux
        keep_half("lower b", 0, roll(mul_left_adjoint(one, centre(Z)), 1))
        one = mul(face(Y, 0, Z), roll(behind, -1))
        keep_half("lower b", 1, mul_left_adjoint(one, behind))

        fill("x")

        def sum_into(name, value):
            keep(name, add(kept(name) if name in begun else None, value))
            begun.add(name)

        begun = {"lower b"}

        def x_faces():
            for slot in (BEHIND[X], BEHIND[X] + 1, X_AHEAD):
                renew(slot)
            keep("xy xz", mul(kept("x x"), whole(halo_ref, X_AHEAD)))
            flux_ref[3] = flux_of(kept("xy xz"), kept("yx zx"))
            keep_half("xz tz", 0, kept_half("xy xz", 1))
            behind = face(X, 0, X)
            twice("x behind", behind)
            keep_half("x corner", 1, roll(behind, -1))
            keep_half("behind n", 1, behind)
            keep_half("behind m", 1, face(X, 0, T))

        def t_ahead():
            renew(T_AHEAD)
            keep("ty tz", mul(kept("t t"), whole(halo_ref, T_AHEAD)))
            flux_ref[2] = flux_of(kept("ty tz"), kept("yt zt"))
            keep_half("xz tz", 1, kept_half("ty tz", 1))

        def x_and_t_ahead():
            renew(BOTH)
            keep_half("t x", 0, half(halo_ref, BOTH, 1))
            keep_half("t x", 1, half(halo_ref, BOTH, 0))
            keep("xt tx", mul(whole(base, 0), kept("t x")))
            flux = flux_of(kept_half("xt tx", 0), kept_half("xt tx", 1))
            flux_ref[0, :, low(0), :] = flux_ref[3, :, low(0), :] + flux_ref[3, :, low(1), :] + flux
            flux_ref[0, :, low(1), :] = flux_ref[2, :, low(0), :] + flux_ref[2, :, low(1), :] - flux
            flux_ref[1] = flux_ref[1] - flux_ref[2] - flux_ref[3]
            sum_into("lower a", roll(mul_left_adjoint(kept("xz tz"), kept("z z")), 1))

        def xy_corner():
            fill("xy")
            renew(12)
            keep_half("y corner", 0, half(halo_ref, 12, 0))
            keep_half("x corner", 0, half(halo_ref, 12, 1))
            one = mul(whole(halo_ref, BEHIND[X] + 1), kept("x corner"))
            sum_into("lower b", mul_left_adjoint(one, kept("x behind")))

        def t_behind():
            renew(BEHIND[T])
            behind = face(T, 0, T)
            twice("t behind", behind)
            keep_half("t corner", 1, roll(behind, -1))
            keep_half("behind n", 0, behind)
            keep_half("behind m", 0, face(T, 0, X))

        def yt_corner():
            fill("yt")
            renew(13)
            keep_half("y corner", 1, half(halo_ref, 13, 0))
            keep_half("t corner", 0, half(halo_ref, 13, 1))

        def y_lower():
            one = mul(whole(halo_ref, BEHIND[Y]), kept("y corner"))
            sum_into("lower a", mul_left_adjoint(one, kept("y behind")))

        def t_lower():
            renew(BEHIND[T] + 1)
            one = mul(whole(halo_ref, BEHIND[T] + 1), kept("t corner"))
            sum_into("lower b", mul_left_adjoint(one, kept("t behind")))

        def xt_lower():
            fill("xt")
            renew(11)
            one = mul(kept("behind m"), whole(halo_ref, 11))
            sum_into("lower a", mul_left_adjoint(one, kept("behind n")))

        def finish(pair, name):
            own = whole(base, pair)
            omega = projected(mul(own, kept(name))) + flux_ref[pair]
            gen = (-flow_eps * FRESH[stage]) * omega
            if stage:
                gen = gen + KEPT[stage] * gen_ref[stage, pair]
            if stage < 2:
                gen_ref[stage + 1, pair] = gen
            else:
                keep("moved", mul(exponential(gen), own))
                for d, (p, pos) in PLACE.items():
                    if p == pair:
                        out_ref[d, 0], out_ref[d, 1] = kept_half("moved", pos)

        tasks = [
            (x_faces, {"x"}),
            (t_ahead, {"ahead"}),
            (x_and_t_ahead, {"x", "ahead"}),
            (xy_corner, {"x", "xy"}),
            (t_behind, {"behind a"}),
            (yt_corner, {"yt", "ahead", "behind a"}),
            (y_lower, {"x", "xy", "yt", "ahead", "behind a"}),
            (t_lower, {"behind a", "behind b", "yt", "ahead"}),
            (lambda: finish(1, "lower b"), {"x", "xy", "ahead", "behind a", "behind b", "yt"}),
            (xt_lower, {"xt", "x", "ahead", "behind a"}),
            (lambda: finish(0, "lower a"), {"x", "xy", "ahead", "behind a", "yt", "xt"}),
        ]
        here_now = set()
        for groups in ORDER[stage]:
            for group in groups:
                arrive(group, ())
                here_now.add(group)
            ready = [task for task, needs in tasks if needs <= here_now]
            tasks = [(task, needs) for task, needs in tasks if not needs <= here_now]
            for task in ready:
                task()
        assert not tasks
        if stage == 0:
            action = sum(action_terms)
    assert len(stacks) <= stack_ref.shape[0]
    wait_sent(units)
    for k in range(2 if partners else 0):
        span = slot_ref.at[pl.ds(0, len(partners))]
        pltpu.make_async_copy(span, span, act_sem.at[k]).wait()
    total = sum(slot_ref[j] for j in range(sizes[0] * sizes[1]))
    scale = 1.0 / (6.0 * sizes[0] * sizes[1] * block[0] * block[1] * lanes)
    total = jnp.sum(total, axis=1, keepdims=True) * scale
    act_ref[...] = jnp.broadcast_to(total, act_ref.shape)


STACKS = 26
STEPS = (("ahead",), ("x", "xy"), ("behind a", "yt"), ("behind b",), ("xt",))
ORDER = (STEPS, STEPS, STEPS)
VMEM_LIMIT = 55000 * 1024


def solution(mesh):
    sizes = tuple(mesh.shape[axis] for axis in AXES)

    def local(links):
        block = links.shape[4:7]
        lanes = links.shape[7]
        rows = block[0] * block[1] * block[2]
        plan = plan_of(block)
        partners = [
            (i, j, 0) for i in range(sizes[0]) for j in range(sizes[1]) if i or j
        ]
        matrix = (2, 3, 3, rows, lanes)
        both = (2, 3, 3, 2 * rows, lanes)
        f32 = jnp.float32
        vmem = pl.BlockSpec(memory_space=pltpu.VMEM)
        flowed, action = pl.pallas_call(
            functools.partial(kernel, block, sizes, plan, partners),
            out_shape=(
                jax.ShapeDtypeStruct((4,) + matrix, f32),
                jax.ShapeDtypeStruct((block[2], lanes), f32),
            ),
            in_specs=[pl.BlockSpec(memory_space=pltpu.HBM)],
            out_specs=(vmem, vmem),
            scratch_shapes=[
                pltpu.VMEM((2,) + both, f32),
                pltpu.VMEM((2,) + both, f32),
                pltpu.VMEM((SLOTS,) + both, f32),
                pltpu.VMEM((3, 2, 8, 2 * rows, lanes), f32),
                pltpu.VMEM((3, SLOTS, 8, 2 * rows, lanes), f32),
                pltpu.VMEM((STACKS,) + both, f32),
                pltpu.VMEM((4, 8, 2 * rows, lanes), f32),
                pltpu.VMEM((block[2], lanes), f32),
                pltpu.VMEM((sizes[0] * sizes[1], block[2], lanes), f32),
                pltpu.SemaphoreType.DMA((len(SEND_ORDER),)),
                pltpu.SemaphoreType.DMA((2, len(SEND_ORDER))),
                pltpu.SemaphoreType.DMA((2,)),
                pltpu.SemaphoreType.DMA((1,)),
            ],
            compiler_params=pltpu.CompilerParams(
                collective_id=0, has_side_effects=True, vmem_limit_bytes=VMEM_LIMIT
            ),
        )(links.reshape((4,) + matrix))
        return flowed.reshape(links.shape), action[:, 0]

    spec = P(None, None, None, None, "gx", "gy", "ta", None)
    return jax.shard_map(
        local, mesh=mesh, in_specs=(spec,), out_specs=(spec, P("ta")), check_vma=False
    )
```

```python
import functools

import jax
import jax.numpy as jnp
from jax import lax
from jax.experimental import pallas as pl
from jax.experimental.pallas import tpu as pltpu
from jax.sharding import PartitionSpec as P

MESH = pl.DeviceIdType.MESH
AXES = ("gx", "gy", "ta")
flow_eps = 0.1
FRESH = (1.0 / 4.0, 8.0 / 9.0, 3.0 / 4.0)
KEPT = (0.0, -17.0 / 9.0, -1.0)


def mul(a, b):
    def dot(x, y):
        return sum(x[:, k][:, None] * y[k][None] for k in range(3))

    return dot(a[0], b[0]) - dot(a[1], b[1]), dot(a[0], b[1]) + dot(a[1], b[0])


def mul_right_adjoint(a, b):
    def dot(x, y):
        return sum(x[:, k][:, None] * y[:, k][None] for k in range(3))

    return dot(a[0], b[0]) + dot(a[1], b[1]), dot(a[1], b[0]) - dot(a[0], b[1])


def mul_left_adjoint(a, b):
    def dot(x, y):
        return sum(x[k][:, None] * y[k][None] for k in range(3))

    return dot(a[0], b[0]) + dot(a[1], b[1]), dot(a[0], b[1]) - dot(a[1], b[0])


def add(a, b):
    return b if a is None else (a[0] + b[0], a[1] + b[1])


def projected(m):
    r, i = m
    third = (i[0, 0] + i[1, 1] + i[2, 2]) / 3.0
    parts = [i[j, j] - third for j in range(2)]
    for j, k in ((0, 1), (0, 2), (1, 2)):
        parts += [(r[j, k] - r[k, j]) / 2.0, (i[j, k] + i[k, j]) / 2.0]
    return jnp.stack(parts)


def exponential(g):
    h = [g[0], g[1], -(g[0] + g[1])]
    u, v, w = (g[2], g[3]), (g[4], g[5]), (g[6], g[7])
    nu, nv, nw = (z[0] * z[0] + z[1] * z[1] for z in (u, v, w))
    uw = (u[0] * w[0] - u[1] * w[1], u[0] * w[1] + u[1] * w[0])
    diag = [h[0] * h[0] + nu + nv, h[1] * h[1] + nu + nw, h[2] * h[2] + nv + nw]
    p = -0.5 * (diag[0] + diag[1] + diag[2])
    det = (
        h[0] * (h[1] * h[2] - nw)
        - h[1] * nv
        - h[2] * nu
        + 2.0 * (uw[1] * v[0] - uw[0] * v[1])
    )
    s01, s02, s12 = h[0] + h[1], h[0] + h[2], h[1] + h[2]
    square = {
        (0, 1): (
            -s01 * u[1] - (v[0] * w[0] + v[1] * w[1]),
            s01 * u[0] - (v[1] * w[0] - v[0] * w[1]),
        ),
        (0, 2): (-s02 * v[1] + uw[0], s02 * v[0] + uw[1]),
        (1, 2): (
            -s12 * w[1] - (u[0] * v[0] + u[1] * v[1]),
            s12 * w[0] - (u[0] * v[1] - u[1] * v[0]),
        ),
    }
    line = {(0, 1): u, (0, 2): v, (1, 2): w}
    ai4, br4 = det * (-1.0 / 120.0), 0.25 + p * (1.0 / 120.0)
    ai3, br3, bi3, cr3 = (
        det * (-1.0 / 60.0),
        1.0 / 3.0 + p * (1.0 / 60.0),
        ai4 * (1.0 / 3.0),
        br4 * (1.0 / 3.0),
    )
    ai2, br2, bi2, cr2, ci2 = (
        det * cr3 * -0.5,
        0.5 + 0.5 * p * cr3,
        0.5 * ai3,
        0.5 * br3,
        0.5 * bi3,
    )
    ar, ai = 1.0 + det * ci2, -det * cr2
    br, bi, cr, ci = 1.0 + p * cr2, ai2 + p * ci2, br2, bi2
    re = [[None] * 3 for _ in range(3)]
    im = [[None] * 3 for _ in range(3)]
    for j in range(3):
        re[j][j] = ar - bi * h[j] - cr * diag[j]
        im[j][j] = ai + br * h[j] - ci * diag[j]
    for j, k in line:
        x, s = line[j, k], square[j, k]
        even_r, odd_r = br * x[0], bi * x[1]
        even_i, odd_i = br * x[1], bi * x[0]
        cs = (cr * s[0], ci * s[1], cr * s[1], ci * s[0])
        re[j][k] = (even_r - odd_r) + (cs[0] - cs[1])
        im[j][k] = (even_i + odd_i) + (cs[2] + cs[3])
        re[k][j] = -(even_r + odd_r) + (cs[0] + cs[1])
        im[k][j] = (even_i - odd_i) + (cs[3] - cs[2])
    return (
        jnp.stack([jnp.stack(row) for row in re]),
        jnp.stack([jnp.stack(row) for row in im]),
    )


def chart(x, rest):
    length = sum(y * y for y in rest)
    first = jnp.where(length < 1e-30, 1e-15, rest[0])
    length = jnp.maximum(length, 1e-30)
    scale = jnp.where(x < 0.0, 1.0 - x, 1.0) / jnp.where(x < 0.0, length, 1.0 + x)
    return [scale * y for y in [first] + rest[1:]]


def frame(y):
    q = 2.0 / (1.0 + sum(v * v for v in y))
    return q, q / (1.0 + y[0] * y[0])


def encode(w):
    r, i = w
    y = chart(r[0, 0], [i[0, 0], r[0, 1], i[0, 1], r[0, 2], i[0, 2]])
    f = frame(y)[1]
    kr = r[1, 0] + y[0] * i[1, 0] + y[1] * r[1, 1] + y[2] * i[1, 1] + y[3] * r[1, 2] + y[4] * i[1, 2]
    ki = i[1, 0] - y[0] * r[1, 0] + y[1] * i[1, 1] - y[2] * r[1, 1] + y[3] * i[1, 2] - y[4] * r[1, 2]
    mr, mi = f * (kr + y[0] * ki), f * (ki - y[0] * kr)
    g = []
    for k in (1, 2):
        u, v = y[2 * k - 1], y[2 * k]
        g += [r[1, k] - (u * mr - v * mi), i[1, k] - (u * mi + v * mr)]
    return jnp.stack(y + chart(g[0], g[1:]))


def decode(code):
    y, z = [code[k] for k in range(5)], [code[k] for k in range(5, 8)]
    q, f = frame(y)
    t = 2.0 / (1.0 + sum(v * v for v in z))
    g = [t - 1.0] + [t * v for v in z]
    kr = y[1] * g[0] + y[2] * g[1] + y[3] * g[2] + y[4] * g[3]
    ki = y[1] * g[1] - y[2] * g[0] + y[3] * g[3] - y[4] * g[2]
    mr, mi = f * (kr - y[0] * ki), f * (ki + y[0] * kr)
    r = [[q - 1.0, q * y[1], q * y[3]], [y[0] * mi - mr]]
    i = [[q * y[0], q * y[2], q * y[4]], [-mi - y[0] * mr]]
    for k in (1, 2):
        u, v = y[2 * k - 1], y[2 * k]
        r[1].append(g[2 * k - 2] - (u * mr - v * mi))
        i[1].append(g[2 * k - 1] - (u * mi + v * mr))
    r.append([])
    i.append([])
    for j in range(3):
        k, l = (j + 1) % 3, (j + 2) % 3
        r[2].append(
            (r[0][k] * r[1][l] - i[0][k] * i[1][l]) - (r[0][l] * r[1][k] - i[0][l] * i[1][k])
        )
        i[2].append(
            (r[0][l] * i[1][k] + i[0][l] * r[1][k]) - (r[0][k] * i[1][l] + i[0][k] * r[1][l])
        )
    return (
        jnp.stack([jnp.stack(row) for row in r]),
        jnp.stack([jnp.stack(row) for row in i]),
    )


def runs(pairs):
    out = []
    for to, frm in pairs:
        if out and to == out[-1][0] + out[-1][2] and frm == out[-1][1] + out[-1][2]:
            out[-1][2] += 1
        else:
            out.append([to, frm, 1])
    return out


def neighbour_rows(block, offset):
    lx, ly, lt = block
    found = {}
    for row in range(lx * ly * lt):
        site = (row // (ly * lt), row // lt % ly, row % lt)
        moved = [site[k] + offset[k] for k in range(3)]
        step = tuple(moved[k] // block[k] for k in range(3))
        at = [moved[k] % block[k] for k in range(3)]
        frm = (at[0] * ly + at[1]) * lt + at[2]
        found.setdefault(step, []).append((row, frm))
    return found


def unit(k, sign):
    return tuple(sign if j == k else 0 for j in range(3))


X, Y, T, Z = 0, 1, 2, 3
PLACE = {X: (0, 0), T: (0, 1), Y: (1, 0), Z: (1, 1)}
BEHIND = {T: 0, Y: 6}
T_AHEAD, X_PACK, MIXED, Y_AHEAD, XT = 2, 3, 5, 8, 10
SLOTS = 11
SEND_ORDER = ("xt", "yt", "xy", "ahead", "behind a", "behind b", "x", "y")


def cover(pairs):
    to, frm = min(pairs)
    assert all(a - b == to - frm for a, b in pairs)
    return to, frm, max(pairs)[0] - to + 1


def local_runs(block, k, sign):
    return runs(neighbour_rows(block, unit(k, sign)).get((0, 0, 0), []))


def plan_of(block):
    rows = block[0] * block[1] * block[2]
    n = rows // block[0]
    assert block[0] > 1 and block[1] > 1 and block[2] == 1
    remote, fills, corners = [], [], {}

    def send(group, pair, pairs, frm, count, slot, to, step):
        remote.append((group, pair, pairs, frm, count, slot, to, step))

    for k in range(3):
        for half, sign in ((0, -1), (1, 1)):
            for step, pairs in neighbour_rows(block, unit(k, sign)).items():
                if not any(step):
                    continue
                to, frm, count = cover(pairs)
                if k == Y:
                    slot = Y_AHEAD if half else BEHIND[Y]
                    send("y", 0, 2, frm, rows + count, slot, to, step)
                elif k == X and half:
                    send("x", 0, 2, rows + frm, n, X_PACK, 3 * n, step)
                    send("x", 1, 1, frm, n, X_PACK + 1, 2 * n, step)
                elif k == X:
                    send("x", 0, 2, frm, n, X_PACK, 0, step)
                    send("x", 0, 2, rows + frm, n, X_PACK, n, step)
                elif half:
                    send("ahead", 0, 1, frm, rows, MIXED, 0, step)
                    send("ahead", 1, 1, frm, 2 * rows, T_AHEAD, 0, step)
                else:
                    send("behind a", 0, 1, frm, 2 * rows, BEHIND[T], 0, step)
                    send("behind b", 1, 1, frm, 2 * rows, BEHIND[T] + 1, 0, step)
    for half, sign in ((0, -1), (1, 1)):
        for d, (pair, at) in PLACE.items():
            for to, frm, count in local_runs(block, Y, sign):
                slot = (Y_AHEAD if half else BEHIND[Y]) + pair
                fills.append(("y", None, pair, at * rows + frm, slot, at * rows + to, count))
    free = {"xy": (X_PACK, 2 * n, 3 * n), "yt": (MIXED, rows, 2 * rows)}
    for m, n_dir in ((X, T), (T, X), (X, Y), (Y, X), (T, Y), (Y, T)):
        ahead, behind = unit(m, 1), unit(n_dir, -1)
        rows_ahead = dict(neighbour_rows(block, ahead).get((0, 0, 0), []))
        rows_behind = dict(neighbour_rows(block, behind).get((0, 0, 0), []))
        offset = tuple(ahead[j] + behind[j] for j in range(3))
        group = "xt" if Y not in (m, n_dir) else "yt" if T in (m, n_dir) else "xy"
        pair, at = PLACE[n_dir]
        from_minus, from_plus, placed = [], [], []
        for step, pairs in neighbour_rows(block, offset).items():
            outer = []
            for to, frm in pairs:
                if to in rows_ahead:
                    from_minus.append((to, rows_ahead[to]))
                elif to in rows_behind:
                    from_plus.append((to, rows_behind[to]))
                else:
                    outer.append((to, frm))
            for to, frm, count in runs(outer):
                if group == "xt":
                    slot, row = XT, int(m == T) * rows + to
                else:
                    slot, row, end = free[group]
                    free[group] = slot, row + count, end
                    assert row + count <= end
                    placed.append((to, slot, row, count))
                send(group, pair, 1, at * rows + frm, count, slot, row, step)
        corners[m, n_dir] = placed, runs(sorted(from_minus)), runs(sorted(from_plus))
    for to, frm, count in corners[X, T][1]:
        fills.append(("xt", BEHIND[T], 0, rows + frm, XT, to, count))
    for to, frm, count in corners[T, X][2]:
        fills.append(("xt", MIXED, 0, frm, XT, rows + to, count))
    remote.sort(key=lambda item: SEND_ORDER.index(item[0]))
    return remote, fills, corners


def kernel(
    block,
    sizes,
    plan,
    partners,
    w_hbm,
    out_ref,
    act_ref,
    first_ref,
    cur_ref,
    halo_ref,
    gen_ref,
    gen_halo_ref,
    stack_ref,
    flux_ref,
    part_ref,
    slot_ref,
    send_sem,
    recv_sem,
    act_sem,
    load_sem,
):
    remote, fills, corners = plan
    rows = block[0] * block[1] * block[2]
    n = rows // block[0]
    lanes = w_hbm.shape[-1]
    for d, (pair, pos) in PLACE.items():
        load = pltpu.make_async_copy(
            w_hbm.at[d], first_ref.at[pair, :, :, :, pl.ds(pos * rows, rows), :], load_sem.at[0]
        )
        load.start()
    here = [lax.axis_index(axis) for axis in AXES]

    def device(step):
        return tuple(lax.rem(here[k] + step[k] + sizes[k], sizes[k]) for k in range(3))

    steps = sorted({item[-1] for item in remote})
    greeted = steps + partners
    barrier = pltpu.get_barrier_semaphore()
    for step in greeted:
        pl.semaphore_signal(barrier, inc=1, device_id=device(step), device_id_type=MESH)
    pltpu.make_async_copy(first_ref, first_ref, load_sem.at[0]).wait()
    for pair in range(2):
        gen_ref[0, pair] = encode((first_ref[pair, 0], first_ref[pair, 1]))
    pl.semaphore_wait(barrier, len(greeted))

    units, stacks = {}, {}

    def wait_bytes(count, sem):
        depth = max(k for k in range(1, 2 * rows + 1) if count % k == 0 and count // k <= SLOTS)
        span = gen_halo_ref.at[0, pl.ds(0, count // depth), :, pl.ds(0, depth), :]
        pltpu.make_async_copy(span, span, sem).wait()

    def wait_sent(units):
        for group, count in units.items():
            wait_bytes(count, send_sem.at[SEND_ORDER.index(group)])


    def low(pos):
        return slice(pos * rows, (pos + 1) * rows)

    def whole(ref, index):
        return ref[index, 0], ref[index, 1]

    def half(ref, index, pos):
        return ref[index, 0, :, :, low(pos), :], ref[index, 1, :, :, low(pos), :]

    def stack(name):
        return stacks.setdefault(name, len(stacks))

    def keep(name, value):
        index = stack(name)
        stack_ref[index, 0], stack_ref[index, 1] = value

    def keep_half(name, pos, value):
        index = stack(name)
        stack_ref[index, 0, :, :, low(pos), :] = value[0]
        stack_ref[index, 1, :, :, low(pos), :] = value[1]

    def twice(name, value):
        keep_half(name, 0, value)
        keep_half(name, 1, value)

    def kept(name):
        return whole(stack_ref, stacks[name])

    def kept_half(name, pos):
        return half(stack_ref, stacks[name], pos)

    def roll(pair, shift):
        return tuple(pltpu.roll(x, shift % lanes, axis=3) for x in pair)

    def face(k, side, d):
        pair, pos = PLACE[d]
        return half(halo_ref, (Y_AHEAD if side else BEHIND[k]) + pair, pos)

    def copy_rows(name, to, ref, index, frm, count):
        slot = stack(name)
        stack_ref[slot, :, :, :, to : to + count, :] = ref[index, :, :, :, frm : frm + count, :]

    for stage in range(3):
        base = first_ref if stage == 0 else cur_ref
        wait_sent(units)
        units = {}
        for group, pair, pairs, frm, count, slot, to, step in remote:
            span, into = pl.ds(pair, pairs), pl.ds(slot, pairs)
            src = gen_ref.at[stage, span, :, pl.ds(frm, count), :]
            dst = gen_halo_ref.at[stage, into, :, pl.ds(to, count), :]
            copy = pltpu.make_async_remote_copy(
                src_ref=src,
                dst_ref=dst,
                send_sem=send_sem.at[SEND_ORDER.index(group)],
                recv_sem=recv_sem.at[stage % 2, SEND_ORDER.index(group)],
                device_id=device(tuple(-s for s in step)),
                device_id_type=MESH,
            )
            units[group] = units.get(group, 0) + pairs * count
            copy.start()

        if stage == 1:
            lt = block[2]
            for t in range(lt):
                part_ref[t : t + 1, :] = sum(action[r : r + 1] for r in range(t, rows, lt))
            mine = here[0] * sizes[1] + here[1]
            for step in partners:
                copy = pltpu.make_async_remote_copy(
                    src_ref=part_ref,
                    dst_ref=slot_ref.at[mine],
                    send_sem=act_sem.at[0],
                    recv_sem=act_sem.at[1],
                    device_id=device(step),
                    device_id_type=MESH,
                )
                copy.start()
            slot_ref[mine] = part_ref[...]

        def fill(wanted):
            for group, source, pair, frm, slot, to, count in fills:
                if group != wanted:
                    continue
                ref = gen_ref.at[stage, pair] if source is None else gen_halo_ref.at[stage, source]
                gen_halo_ref[stage, slot, :, to : to + count, :] = ref[:, frm : frm + count, :]

        def renew(slot):
            code = gen_halo_ref[stage, slot]
            if stage == 0:
                new = decode(code)
            else:
                new = mul(exponential(code), whole(halo_ref, slot))
            halo_ref[slot, 0], halo_ref[slot, 1] = new

        def arrive(group, slots):
            if group in units:
                wait_bytes(units[group], recv_sem.at[stage % 2, SEND_ORDER.index(group)])
            if group != "xt":
                fill(group)
            for slot in slots:
                renew(slot)

        def count_action(plaq):
            trace = plaq[0][0, 0] + plaq[0][1, 1] + plaq[0][2, 2]
            term = 1.0 - trace / 3.0
            return term if term.shape[0] == rows else term[:rows] + term[rows:]

        action_terms = []

        def flux_of(one, two):
            plaq = mul_right_adjoint(one, two)
            if stage == 0:
                action_terms.append(count_action(plaq))
            return projected(plaq)

        def centre(d):
            return half(base, *PLACE[d])

        if stage:
            for pair in range(2):
                before = whole(first_ref if stage == 1 else cur_ref, pair)
                moved = mul(exponential(gen_ref[stage, pair]), before)
                cur_ref[pair, 0], cur_ref[pair, 1] = moved
        for d, name in ((X, "x x"), (T, "t t"), (Z, "z z")):
            twice(name, centre(d))
        for d, name in ((X, "x ahead"), (T, "t ahead"), (Y, "y z ahead")):
            keep_half(name, 1, roll(centre(d), -1))

        for d, (pair, pos) in PLACE.items():
            for to, frm, count in local_runs(block, X, -1):
                copy_rows(("xb a", "xb b")[pair], pos * rows + to, base, pair, pos * rows + frm, count)
            if d == X:
                continue
            for to, frm, count in local_runs(block, X, 1):
                name, at = ("t x", 0) if d == T else ("xa yz", pos * rows)
                copy_rows(name, at + to, base, pair, pos * rows + frm, count)

        arrive("y", range(BEHIND[Y], Y_AHEAD + 2))
        for d, name in ((X, "x ahead"), (T, "t ahead"), (Z, "y z ahead")):
            keep_half(name, 0, face(Y, 1, d))
        behind = face(Y, 0, Y)
        twice("y behind", behind)
        yz = whole(base, 1)
        keep("yx zx", mul(yz, kept("x ahead")))
        keep("yt zt", mul(yz, kept("t ahead")))
        keep("yz zy", mul(yz, kept("y z ahead")))
        one = kept_half("yz zy", 0)
        flux = flux_of(one, kept_half("yz zy", 1))
        flux_ref[1, :, low(0), :] = flux
        flux_ref[1, :, low(1), :] = -flux
        keep_half("lower b", 0, roll(mul_left_adjoint(one, centre(Z)), 1))
        one = mul(face(Y, 0, Z), roll(behind, -1))
        keep_half("lower b", 1, mul_left_adjoint(one, behind))

        def sum_into(name, value):
            keep(name, add(kept(name) if name in begun else None, value))
            begun.add(name)

        begun = {"lower b"}

        def x_faces():
            for slot in (X_PACK, X_PACK + 1):
                renew(slot)
            to = cover(sum((p for q, p in neighbour_rows(block, unit(X, 1)).items() if any(q)), []))[0]
            copy_rows("xa yz", to, halo_ref, X_PACK + 1, 2 * n, n)
            copy_rows("xa yz", rows + to, halo_ref, X_PACK + 1, 3 * n, n)
            copy_rows("t x", to, halo_ref, X_PACK, 3 * n, n)
            to = cover(sum((p for q, p in neighbour_rows(block, unit(X, -1)).items() if any(q)), []))[0]
            for pos in range(2):
                copy_rows("xb a", pos * rows + to, halo_ref, X_PACK, pos * n, n)
                copy_rows("xb b", pos * rows + to, halo_ref, X_PACK + 1, pos * n, n)
            keep("xy xz", mul(kept("x x"), kept("xa yz")))
            flux_ref[3] = flux_of(kept("xy xz"), kept("yx zx"))
            keep_half("xz tz", 0, kept_half("xy xz", 1))
            behind = kept_half("xb a", 0)
            twice("x behind", behind)
            keep_half("x corner", 1, roll(behind, -1))
            keep_half("behind n", 1, behind)
            keep_half("behind m", 1, kept_half("xb a", 1))

        def corner(name, at, m, n_dir, minus, plus):
            placed, from_minus, from_plus = corners[m, n_dir]
            for to, slot, row, count in placed:
                copy_rows(name, at + to, halo_ref, slot, row, count)
            for found, source in ((from_minus, minus), (from_plus, plus)):
                for to, frm, count in found:
                    copy_rows(name, at + to, source[0], source[1], source[2] + frm, count)

        def xy_corner():
            corner("y corner", 0, X, Y, (halo_ref, BEHIND[Y] + 1, 0), (stack_ref, stacks["xa yz"], 0))
            corner("x corner", 0, Y, X, (stack_ref, stacks["xb a"], 0), (halo_ref, Y_AHEAD, 0))
            one = mul(kept("xb b"), kept("x corner"))
            sum_into("lower b", mul_left_adjoint(one, kept("x behind")))

        def t_ahead():
            renew(T_AHEAD)
            renew(MIXED)
            keep("ty tz", mul(kept("t t"), whole(halo_ref, T_AHEAD)))
            flux_ref[2] = flux_of(kept("ty tz"), kept("yt zt"))
            keep_half("xz tz", 1, kept_half("ty tz", 1))
            keep_half("t x", 1, half(halo_ref, MIXED, 0))
            corner("y corner", rows, T, Y, None, (halo_ref, T_AHEAD, 0))

        def x_and_t_ahead():
            keep("xt tx", mul(whole(base, 0), kept("t x")))
            flux = flux_of(kept_half("xt tx", 0), kept_half("xt tx", 1))
            flux_ref[0, :, low(0), :] = flux_ref[3, :, low(0), :] + flux_ref[3, :, low(1), :] + flux
            flux_ref[0, :, low(1), :] = flux_ref[2, :, low(0), :] + flux_ref[2, :, low(1), :] - flux
            flux_ref[1] = flux_ref[1] - flux_ref[2] - flux_ref[3]
            sum_into("lower a", roll(mul_left_adjoint(kept("xz tz"), kept("z z")), 1))

        def t_behind():
            renew(BEHIND[T])
            behind = face(T, 0, T)
            twice("t behind", behind)
            keep_half("t corner", 1, roll(behind, -1))
            keep_half("behind n", 0, behind)
            keep_half("behind m", 0, face(T, 0, X))
            corner("t corner", 0, Y, T, (halo_ref, BEHIND[T], rows), None)

        def y_lower():
            one = mul(whole(halo_ref, BEHIND[Y]), kept("y corner"))
            sum_into("lower a", mul_left_adjoint(one, kept("y behind")))

        def t_lower():
            renew(BEHIND[T] + 1)
            one = mul(whole(halo_ref, BEHIND[T] + 1), kept("t corner"))
            sum_into("lower b", mul_left_adjoint(one, kept("t behind")))

        def xt_lower():
            fill("xt")
            renew(XT)
            one = mul(kept("behind m"), whole(halo_ref, XT))
            sum_into("lower a", mul_left_adjoint(one, kept("behind n")))

        def finish(pair, name):
            own = whole(base, pair)
            omega = projected(mul(own, kept(name))) + flux_ref[pair]
            gen = (-flow_eps * FRESH[stage]) * omega
            if stage:
                gen = gen + KEPT[stage] * gen_ref[stage, pair]
            if stage < 2:
                gen_ref[stage + 1, pair] = gen
            else:
                keep("moved", mul(exponential(gen), own))
                for d, (p, pos) in PLACE.items():
                    if p == pair:
                        out_ref[d, 0], out_ref[d, 1] = kept_half("moved", pos)

        tasks = [
            (t_ahead, {"ahead", "yt"}),
            (x_faces, {"x", "xy"}),
            (x_and_t_ahead, {"x", "xy", "ahead", "yt"}),
            (xy_corner, {"x", "xy"}),
            (y_lower, {"x", "xy", "yt", "ahead"}),
            (t_behind, {"behind a", "ahead", "yt"}),
            (t_lower, {"behind a", "behind b", "yt", "ahead"}),
            (lambda: finish(1, "lower b"), {"x", "xy", "ahead", "behind a", "behind b", "yt"}),
            (xt_lower, {"xt", "x", "xy", "ahead", "yt", "behind a"}),
            (lambda: finish(0, "lower a"), {"x", "xy", "ahead", "behind a", "yt", "xt"}),
        ]
        here_now = set()
        for groups in ORDER[stage]:
            for group in groups:
                arrive(group, ())
                here_now.add(group)
            ready = [task for task, needs in tasks if needs <= here_now]
            tasks = [(task, needs) for task, needs in tasks if not needs <= here_now]
            for task in ready:
                task()
        assert not tasks
        if stage == 0:
            action = sum(action_terms)
    assert len(stacks) <= stack_ref.shape[0]
    wait_sent(units)
    for k in range(2 if partners else 0):
        span = slot_ref.at[pl.ds(0, len(partners))]
        pltpu.make_async_copy(span, span, act_sem.at[k]).wait()
    total = sum(slot_ref[j] for j in range(sizes[0] * sizes[1]))
    scale = 1.0 / (6.0 * sizes[0] * sizes[1] * block[0] * block[1] * lanes)
    total = jnp.sum(total, axis=1, keepdims=True) * scale
    act_ref[...] = jnp.broadcast_to(total, act_ref.shape)


STACKS = 30
STEPS = (("ahead", "yt"), ("x", "xy"), ("behind a",), ("behind b",), ("xt",))
ORDER = (STEPS, STEPS, STEPS)
VMEM_LIMIT = 55000 * 1024


def solution(mesh):
    sizes = tuple(mesh.shape[axis] for axis in AXES)

    def local(links):
        block = links.shape[4:7]
        lanes = links.shape[7]
        rows = block[0] * block[1] * block[2]
        plan = plan_of(block)
        partners = [
            (i, j, 0) for i in range(sizes[0]) for j in range(sizes[1]) if i or j
        ]
        matrix = (2, 3, 3, rows, lanes)
        both = (2, 3, 3, 2 * rows, lanes)
        f32 = jnp.float32
        vmem = pl.BlockSpec(memory_space=pltpu.VMEM)
        flowed, action = pl.pallas_call(
            functools.partial(kernel, block, sizes, plan, partners),
            out_shape=(
                jax.ShapeDtypeStruct((4,) + matrix, f32),
                jax.ShapeDtypeStruct((block[2], lanes), f32),
            ),
            in_specs=[pl.BlockSpec(memory_space=pltpu.HBM)],
            out_specs=(vmem, vmem),
            scratch_shapes=[
                pltpu.VMEM((2,) + both, f32),
                pltpu.VMEM((2,) + both, f32),
                pltpu.VMEM((SLOTS,) + both, f32),
                pltpu.VMEM((3, 2, 8, 2 * rows, lanes), f32),
                pltpu.VMEM((3, SLOTS, 8, 2 * rows, lanes), f32),
                pltpu.VMEM((STACKS,) + both, f32),
                pltpu.VMEM((4, 8, 2 * rows, lanes), f32),
                pltpu.VMEM((block[2], lanes), f32),
                pltpu.VMEM((sizes[0] * sizes[1], block[2], lanes), f32),
                pltpu.SemaphoreType.DMA((len(SEND_ORDER),)),
                pltpu.SemaphoreType.DMA((2, len(SEND_ORDER))),
                pltpu.SemaphoreType.DMA((2,)),
                pltpu.SemaphoreType.DMA((1,)),
            ],
            compiler_params=pltpu.CompilerParams(
                collective_id=0, has_side_effects=True, vmem_limit_bytes=VMEM_LIMIT
            ),
        )(links.reshape((4,) + matrix))
        return flowed.reshape(links.shape), action[:, 0]

    spec = P(None, None, None, None, "gx", "gy", "ta", None)
    return jax.shard_map(
        local, mesh=mesh, in_specs=(spec,), out_specs=(spec, P("ta")), check_vma=False
    )
```

```python
import functools

import jax
import jax.numpy as jnp
from jax import lax
from jax.experimental import pallas as pl
from jax.experimental.pallas import tpu as pltpu
from jax.sharding import PartitionSpec as P

MESH = pl.DeviceIdType.MESH
AXES = ("gx", "gy", "ta")
flow_eps = 0.1
FRESH = (1.0 / 4.0, 8.0 / 9.0, 3.0 / 4.0)
KEPT = (0.0, -17.0 / 9.0, -1.0)


def mul(a, b):
    def dot(x, y):
        return sum(x[:, k][:, None] * y[k][None] for k in range(3))

    return dot(a[0], b[0]) - dot(a[1], b[1]), dot(a[0], b[1]) + dot(a[1], b[0])


def mul_right_adjoint(a, b):
    def dot(x, y):
        return sum(x[:, k][:, None] * y[:, k][None] for k in range(3))

    return dot(a[0], b[0]) + dot(a[1], b[1]), dot(a[1], b[0]) - dot(a[0], b[1])


def mul_left_adjoint(a, b):
    def dot(x, y):
        return sum(x[k][:, None] * y[k][None] for k in range(3))

    return dot(a[0], b[0]) + dot(a[1], b[1]), dot(a[0], b[1]) - dot(a[1], b[0])


def add(a, b):
    return b if a is None else (a[0] + b[0], a[1] + b[1])


def projected(m):
    r, i = m
    third = (i[0, 0] + i[1, 1] + i[2, 2]) / 3.0
    parts = [i[j, j] - third for j in range(2)]
    for j, k in ((0, 1), (0, 2), (1, 2)):
        parts += [(r[j, k] - r[k, j]) / 2.0, (i[j, k] + i[k, j]) / 2.0]
    return jnp.stack(parts)


def exponential(g):
    h = [g[0], g[1], -(g[0] + g[1])]
    u, v, w = (g[2], g[3]), (g[4], g[5]), (g[6], g[7])
    nu, nv, nw = (z[0] * z[0] + z[1] * z[1] for z in (u, v, w))
    uw = (u[0] * w[0] - u[1] * w[1], u[0] * w[1] + u[1] * w[0])
    diag = [h[0] * h[0] + nu + nv, h[1] * h[1] + nu + nw, h[2] * h[2] + nv + nw]
    p = -0.5 * (diag[0] + diag[1] + diag[2])
    det = (
        h[0] * (h[1] * h[2] - nw)
        - h[1] * nv
        - h[2] * nu
        + 2.0 * (uw[1] * v[0] - uw[0] * v[1])
    )
    s01, s02, s12 = h[0] + h[1], h[0] + h[2], h[1] + h[2]
    square = {
        (0, 1): (
            -s01 * u[1] - (v[0] * w[0] + v[1] * w[1]),
            s01 * u[0] - (v[1] * w[0] - v[0] * w[1]),
        ),
        (0, 2): (-s02 * v[1] + uw[0], s02 * v[0] + uw[1]),
        (1, 2): (
            -s12 * w[1] - (u[0] * v[0] + u[1] * v[1]),
            s12 * w[0] - (u[0] * v[1] - u[1] * v[0]),
        ),
    }
    line = {(0, 1): u, (0, 2): v, (1, 2): w}
    ai4, br4 = det * (-1.0 / 120.0), 0.25 + p * (1.0 / 120.0)
    ai3, br3, bi3, cr3 = (
        det * (-1.0 / 60.0),
        1.0 / 3.0 + p * (1.0 / 60.0),
        ai4 * (1.0 / 3.0),
        br4 * (1.0 / 3.0),
    )
    ai2, br2, bi2, cr2, ci2 = (
        det * cr3 * -0.5,
        0.5 + 0.5 * p * cr3,
        0.5 * ai3,
        0.5 * br3,
        0.5 * bi3,
    )
    ar, ai = 1.0 + det * ci2, -det * cr2
    br, bi, cr, ci = 1.0 + p * cr2, ai2 + p * ci2, br2, bi2
    re = [[None] * 3 for _ in range(3)]
    im = [[None] * 3 for _ in range(3)]
    for j in range(3):
        re[j][j] = ar - bi * h[j] - cr * diag[j]
        im[j][j] = ai + br * h[j] - ci * diag[j]
    for j, k in line:
        x, s = line[j, k], square[j, k]
        even_r, odd_r = br * x[0], bi * x[1]
        even_i, odd_i = br * x[1], bi * x[0]
        cs = (cr * s[0], ci * s[1], cr * s[1], ci * s[0])
        re[j][k] = (even_r - odd_r) + (cs[0] - cs[1])
        im[j][k] = (even_i + odd_i) + (cs[2] + cs[3])
        re[k][j] = -(even_r + odd_r) + (cs[0] + cs[1])
        im[k][j] = (even_i - odd_i) + (cs[3] - cs[2])
    return (
        jnp.stack([jnp.stack(row) for row in re]),
        jnp.stack([jnp.stack(row) for row in im]),
    )


def chart(x, rest):
    length = sum(y * y for y in rest)
    first = jnp.where(length < 1e-30, 1e-15, rest[0])
    length = jnp.maximum(length, 1e-30)
    scale = jnp.where(x < 0.0, 1.0 - x, 1.0) / jnp.where(x < 0.0, length, 1.0 + x)
    return [scale * y for y in [first] + rest[1:]]


def frame(y):
    q = 2.0 / (1.0 + sum(v * v for v in y))
    return q, q / (1.0 + y[0] * y[0])


def encode(w):
    r, i = w
    y = chart(r[0, 0], [i[0, 0], r[0, 1], i[0, 1], r[0, 2], i[0, 2]])
    f = frame(y)[1]
    kr = r[1, 0] + y[0] * i[1, 0] + y[1] * r[1, 1] + y[2] * i[1, 1] + y[3] * r[1, 2] + y[4] * i[1, 2]
    ki = i[1, 0] - y[0] * r[1, 0] + y[1] * i[1, 1] - y[2] * r[1, 1] + y[3] * i[1, 2] - y[4] * r[1, 2]
    mr, mi = f * (kr + y[0] * ki), f * (ki - y[0] * kr)
    g = []
    for k in (1, 2):
        u, v = y[2 * k - 1], y[2 * k]
        g += [r[1, k] - (u * mr - v * mi), i[1, k] - (u * mi + v * mr)]
    return jnp.stack(y + chart(g[0], g[1:]))


def decode(code):
    y, z = [code[k] for k in range(5)], [code[k] for k in range(5, 8)]
    q, f = frame(y)
    t = 2.0 / (1.0 + sum(v * v for v in z))
    g = [t - 1.0] + [t * v for v in z]
    kr = y[1] * g[0] + y[2] * g[1] + y[3] * g[2] + y[4] * g[3]
    ki = y[1] * g[1] - y[2] * g[0] + y[3] * g[3] - y[4] * g[2]
    mr, mi = f * (kr - y[0] * ki), f * (ki + y[0] * kr)
    r = [[q - 1.0, q * y[1], q * y[3]], [y[0] * mi - mr]]
    i = [[q * y[0], q * y[2], q * y[4]], [-mi - y[0] * mr]]
    for k in (1, 2):
        u, v = y[2 * k - 1], y[2 * k]
        r[1].append(g[2 * k - 2] - (u * mr - v * mi))
        i[1].append(g[2 * k - 1] - (u * mi + v * mr))
    r.append([])
    i.append([])
    for j in range(3):
        k, l = (j + 1) % 3, (j + 2) % 3
        r[2].append(
            (r[0][k] * r[1][l] - i[0][k] * i[1][l]) - (r[0][l] * r[1][k] - i[0][l] * i[1][k])
        )
        i[2].append(
            (r[0][l] * i[1][k] + i[0][l] * r[1][k]) - (r[0][k] * i[1][l] + i[0][k] * r[1][l])
        )
    return (
        jnp.stack([jnp.stack(row) for row in r]),
        jnp.stack([jnp.stack(row) for row in i]),
    )


def runs(pairs):
    out = []
    for to, frm in pairs:
        if out and to == out[-1][0] + out[-1][2] and frm == out[-1][1] + out[-1][2]:
            out[-1][2] += 1
        else:
            out.append([to, frm, 1])
    return out


def neighbour_rows(block, offset):
    lx, ly, lt = block
    found = {}
    for row in range(lx * ly * lt):
        site = (row // (ly * lt), row // lt % ly, row % lt)
        moved = [site[k] + offset[k] for k in range(3)]
        step = tuple(moved[k] // block[k] for k in range(3))
        at = [moved[k] % block[k] for k in range(3)]
        frm = (at[0] * ly + at[1]) * lt + at[2]
        found.setdefault(step, []).append((row, frm))
    return found


def unit(k, sign):
    return tuple(sign if j == k else 0 for j in range(3))


X, Y, T, Z = 0, 1, 2, 3
PLACE = {X: (0, 0), T: (0, 1), Y: (1, 0), Z: (1, 1)}
BEHIND = {T: 0, Y: 6}
T_AHEAD, X_PACK, MIXED, Y_AHEAD, XT = 2, 3, 5, 8, 10
SLOTS = 11
SEND_ORDER = ("xt", "yt", "xy", "ahead", "behind a", "behind b", "x", "y")


def cover(pairs):
    to, frm = min(pairs)
    assert all(a - b == to - frm for a, b in pairs)
    return to, frm, max(pairs)[0] - to + 1


def local_runs(block, k, sign):
    return runs(neighbour_rows(block, unit(k, sign)).get((0, 0, 0), []))


def plan_of(block):
    rows = block[0] * block[1] * block[2]
    n = rows // block[0]
    assert block[0] > 1 and block[1] > 1 and block[2] == 1
    remote, fills, corners = [], [], {}

    def send(group, pair, pairs, frm, count, slot, to, step):
        remote.append((group, pair, pairs, frm, count, slot, to, step))

    for k in range(3):
        for half, sign in ((0, -1), (1, 1)):
            for step, pairs in neighbour_rows(block, unit(k, sign)).items():
                if not any(step):
                    continue
                to, frm, count = cover(pairs)
                if k == Y:
                    slot = Y_AHEAD if half else BEHIND[Y]
                    send("y", 0, 2, frm, rows + count, slot, to, step)
                elif k == X and half:
                    send("x", 0, 2, rows + frm, n, X_PACK, 3 * n, step)
                    send("x", 1, 1, frm, n, X_PACK + 1, 2 * n, step)
                elif k == X:
                    send("x", 0, 2, frm, n, X_PACK, 0, step)
                    send("x", 0, 2, rows + frm, n, X_PACK, n, step)
                elif half:
                    send("ahead", 0, 1, frm, rows, MIXED, 0, step)
                    send("ahead", 1, 1, frm, 2 * rows, T_AHEAD, 0, step)
                else:
                    send("behind a", 0, 1, frm, 2 * rows, BEHIND[T], 0, step)
                    send("behind b", 1, 1, frm, 2 * rows, BEHIND[T] + 1, 0, step)
    for half, sign in ((0, -1), (1, 1)):
        for d, (pair, at) in PLACE.items():
            for to, frm, count in local_runs(block, Y, sign):
                slot = (Y_AHEAD if half else BEHIND[Y]) + pair
                fills.append(("y", None, pair, at * rows + frm, slot, at * rows + to, count))
    free = {"xy": (X_PACK, 2 * n, 3 * n), "yt": (MIXED, rows, 2 * rows)}
    for m, n_dir in ((X, T), (T, X), (X, Y), (Y, X), (T, Y), (Y, T)):
        ahead, behind = unit(m, 1), unit(n_dir, -1)
        rows_ahead = dict(neighbour_rows(block, ahead).get((0, 0, 0), []))
        rows_behind = dict(neighbour_rows(block, behind).get((0, 0, 0), []))
        offset = tuple(ahead[j] + behind[j] for j in range(3))
        group = "xt" if Y not in (m, n_dir) else "yt" if T in (m, n_dir) else "xy"
        pair, at = PLACE[n_dir]
        from_minus, from_plus, placed = [], [], []
        for step, pairs in neighbour_rows(block, offset).items():
            outer = []
            for to, frm in pairs:
                if to in rows_ahead:
                    from_minus.append((to, rows_ahead[to]))
                elif to in rows_behind:
                    from_plus.append((to, rows_behind[to]))
                else:
                    outer.append((to, frm))
            for to, frm, count in runs(outer):
                if group == "xt":
                    slot, row = XT, int(m == T) * rows + to
                else:
                    slot, row, end = free[group]
                    free[group] = slot, row + count, end
                    assert row + count <= end
                    placed.append((to, slot, row, count))
                send(group, pair, 1, at * rows + frm, count, slot, row, step)
        corners[m, n_dir] = placed, runs(sorted(from_minus)), runs(sorted(from_plus))
    for to, frm, count in corners[X, T][1]:
        fills.append(("xt", BEHIND[T], 0, rows + frm, XT, to, count))
    for to, frm, count in corners[T, X][2]:
        fills.append(("xt", MIXED, 0, frm, XT, rows + to, count))
    remote.sort(key=lambda item: SEND_ORDER.index(item[0]))
    return remote, fills, corners


def kernel(
    block,
    sizes,
    plan,
    partners,
    w_hbm,
    out_ref,
    act_ref,
    first_ref,
    cur_ref,
    halo_ref,
    gen_ref,
    gen_halo_ref,
    stack_ref,
    flux_ref,
    part_ref,
    slot_ref,
    send_sem,
    recv_sem,
    act_sem,
    load_sem,
):
    remote, fills, corners = plan
    rows = block[0] * block[1] * block[2]
    n = rows // block[0]
    lanes = w_hbm.shape[-1]
    here = [lax.axis_index(axis) for axis in AXES]

    def device(step):
        return tuple(lax.rem(here[k] + step[k] + sizes[k], sizes[k]) for k in range(3))

    steps = [item[-1] for item in remote] + partners
    greeted = sorted({tuple(s % size for s, size in zip(step, sizes)) for step in steps})
    barrier = pltpu.get_barrier_semaphore()
    for step in reversed(greeted):
        pl.semaphore_signal(barrier, inc=1, device_id=device(step), device_id_type=MESH)
    for d, (pair, pos) in PLACE.items():
        load = pltpu.make_async_copy(
            w_hbm.at[d], first_ref.at[pair, :, :, :, pl.ds(pos * rows, rows), :], load_sem.at[0]
        )
        load.start()
    pltpu.make_async_copy(first_ref, first_ref, load_sem.at[0]).wait()
    for pair in range(2):
        gen_ref[0, pair] = encode((first_ref[pair, 0], first_ref[pair, 1]))
    pl.semaphore_wait(barrier, len(greeted))

    units, stacks = {}, {}

    def wait_bytes(count, sem):
        depth = max(k for k in range(1, 2 * rows + 1) if count % k == 0 and count // k <= SLOTS)
        span = gen_halo_ref.at[0, pl.ds(0, count // depth), :, pl.ds(0, depth), :]
        pltpu.make_async_copy(span, span, sem).wait()

    def wait_sent(units):
        for group, count in units.items():
            wait_bytes(count, send_sem.at[SEND_ORDER.index(group)])


    def low(pos):
        return slice(pos * rows, (pos + 1) * rows)

    def whole(ref, index):
        return ref[index, 0], ref[index, 1]

    def half(ref, index, pos):
        return ref[index, 0, :, :, low(pos), :], ref[index, 1, :, :, low(pos), :]

    def stack(name):
        return stacks.setdefault(name, len(stacks))

    def keep(name, value):
        index = stack(name)
        stack_ref[index, 0], stack_ref[index, 1] = value

    def keep_half(name, pos, value):
        index = stack(name)
        stack_ref[index, 0, :, :, low(pos), :] = value[0]
        stack_ref[index, 1, :, :, low(pos), :] = value[1]

    def twice(name, value):
        keep_half(name, 0, value)
        keep_half(name, 1, value)

    def kept(name):
        return whole(stack_ref, stacks[name])

    def kept_half(name, pos):
        return half(stack_ref, stacks[name], pos)

    def roll(pair, shift):
        return tuple(pltpu.roll(x, shift % lanes, axis=3) for x in pair)

    def face(k, side, d):
        pair, pos = PLACE[d]
        return half(halo_ref, (Y_AHEAD if side else BEHIND[k]) + pair, pos)

    def copy_rows(name, to, ref, index, frm, count):
        slot = stack(name)
        stack_ref[slot, :, :, :, to : to + count, :] = ref[index, :, :, :, frm : frm + count, :]

    for stage in range(3):
        base = first_ref if stage == 0 else cur_ref
        wait_sent(units)
        units = {}
        for group, pair, pairs, frm, count, slot, to, step in remote:
            span, into = pl.ds(pair, pairs), pl.ds(slot, pairs)
            src = gen_ref.at[stage, span, :, pl.ds(frm, count), :]
            dst = gen_halo_ref.at[stage, into, :, pl.ds(to, count), :]
            copy = pltpu.make_async_remote_copy(
                src_ref=src,
                dst_ref=dst,
                send_sem=send_sem.at[SEND_ORDER.index(group)],
                recv_sem=recv_sem.at[stage % 2, SEND_ORDER.index(group)],
                device_id=device(tuple(-s for s in step)),
                device_id_type=MESH,
            )
            units[group] = units.get(group, 0) + pairs * count
            copy.start()

        if stage == 1:
            lt = block[2]
            for t in range(lt):
                part_ref[t : t + 1, :] = sum(action[r : r + 1] for r in range(t, rows, lt))
            mine = here[0] * sizes[1] + here[1]
            for step in partners:
                copy = pltpu.make_async_remote_copy(
                    src_ref=part_ref,
                    dst_ref=slot_ref.at[mine],
                    send_sem=act_sem.at[0],
                    recv_sem=act_sem.at[1],
                    device_id=device(step),
                    device_id_type=MESH,
                )
                copy.start()
            slot_ref[mine] = part_ref[...]

        def fill(wanted):
            for group, source, pair, frm, slot, to, count in fills:
                if group != wanted:
                    continue
                ref = gen_ref.at[stage, pair] if source is None else gen_halo_ref.at[stage, source]
                gen_halo_ref[stage, slot, :, to : to + count, :] = ref[:, frm : frm + count, :]

        def renew(slot):
            code = gen_halo_ref[stage, slot]
            if stage == 0:
                new = decode(code)
            else:
                new = mul(exponential(code), whole(halo_ref, slot))
            halo_ref[slot, 0], halo_ref[slot, 1] = new

        def arrive(group, slots):
            if group in units:
                wait_bytes(units[group], recv_sem.at[stage % 2, SEND_ORDER.index(group)])
            if group != "xt":
                fill(group)
            for slot in slots:
                renew(slot)

        def count_action(plaq):
            trace = plaq[0][0, 0] + plaq[0][1, 1] + plaq[0][2, 2]
            term = 1.0 - trace / 3.0
            return term if term.shape[0] == rows else term[:rows] + term[rows:]

        action_terms = []

        def flux_of(one, two):
            plaq = mul_right_adjoint(one, two)
            if stage == 0:
                action_terms.append(count_action(plaq))
            return projected(plaq)

        def centre(d):
            return half(base, *PLACE[d])

        if stage:
            for pair in range(2):
                before = whole(first_ref if stage == 1 else cur_ref, pair)
                moved = mul(exponential(gen_ref[stage, pair]), before)
                cur_ref[pair, 0], cur_ref[pair, 1] = moved
        for d, name in ((X, "x x"), (T, "t t"), (Z, "z z")):
            twice(name, centre(d))
        for d, name in ((X, "x ahead"), (T, "t ahead"), (Y, "y z ahead")):
            keep_half(name, 1, roll(centre(d), -1))

        for d, (pair, pos) in PLACE.items():
            for to, frm, count in local_runs(block, X, -1):
                copy_rows(("xb a", "xb b")[pair], pos * rows + to, base, pair, pos * rows + frm, count)
            if d == X:
                continue
            for to, frm, count in local_runs(block, X, 1):
                name, at = ("t x", 0) if d == T else ("xa yz", pos * rows)
                copy_rows(name, at + to, base, pair, pos * rows + frm, count)

        arrive("y", range(BEHIND[Y], Y_AHEAD + 2))
        for d, name in ((X, "x ahead"), (T, "t ahead"), (Z, "y z ahead")):
            keep_half(name, 0, face(Y, 1, d))
        behind = face(Y, 0, Y)
        twice("y behind", behind)
        yz = whole(base, 1)
        keep("yx zx", mul(yz, kept("x ahead")))
        keep("yt zt", mul(yz, kept("t ahead")))
        keep("yz zy", mul(yz, kept("y z ahead")))
        one = kept_half("yz zy", 0)
        flux = flux_of(one, kept_half("yz zy", 1))
        flux_ref[1, :, low(0), :] = flux
        flux_ref[1, :, low(1), :] = -flux
        keep_half("lower b", 0, roll(mul_left_adjoint(one, centre(Z)), 1))
        one = mul(face(Y, 0, Z), roll(behind, -1))
        keep_half("lower b", 1, mul_left_adjoint(one, behind))

        def sum_into(name, value):
            keep(name, add(kept(name) if name in begun else None, value))
            begun.add(name)

        begun = {"lower b"}

        def x_faces():
            for slot in (X_PACK, X_PACK + 1):
                renew(slot)
            to = cover(sum((p for q, p in neighbour_rows(block, unit(X, 1)).items() if any(q)), []))[0]
            copy_rows("xa yz", to, halo_ref, X_PACK + 1, 2 * n, n)
            copy_rows("xa yz", rows + to, halo_ref, X_PACK + 1, 3 * n, n)
            copy_rows("t x", to, halo_ref, X_PACK, 3 * n, n)
            to = cover(sum((p for q, p in neighbour_rows(block, unit(X, -1)).items() if any(q)), []))[0]
            for pos in range(2):
                copy_rows("xb a", pos * rows + to, halo_ref, X_PACK, pos * n, n)
                copy_rows("xb b", pos * rows + to, halo_ref, X_PACK + 1, pos * n, n)
            keep("xy xz", mul(kept("x x"), kept("xa yz")))
            flux_ref[3] = flux_of(kept("xy xz"), kept("yx zx"))
            keep_half("xz tz", 0, kept_half("xy xz", 1))
            behind = kept_half("xb a", 0)
            twice("x behind", behind)
            keep_half("x corner", 1, roll(behind, -1))
            keep_half("behind n", 1, behind)
            keep_half("behind m", 1, kept_half("xb a", 1))

        def corner(name, at, m, n_dir, minus, plus):
            placed, from_minus, from_plus = corners[m, n_dir]
            for to, slot, row, count in placed:
                copy_rows(name, at + to, halo_ref, slot, row, count)
            for found, source in ((from_minus, minus), (from_plus, plus)):
                for to, frm, count in found:
                    copy_rows(name, at + to, source[0], source[1], source[2] + frm, count)

        def xy_corner():
            corner("y corner", 0, X, Y, (halo_ref, BEHIND[Y] + 1, 0), (stack_ref, stacks["xa yz"], 0))
            corner("x corner", 0, Y, X, (stack_ref, stacks["xb a"], 0), (halo_ref, Y_AHEAD, 0))
            one = mul(kept("xb b"), kept("x corner"))
            sum_into("lower b", mul_left_adjoint(one, kept("x behind")))

        def t_ahead():
            renew(T_AHEAD)
            renew(MIXED)
            keep("ty tz", mul(kept("t t"), whole(halo_ref, T_AHEAD)))
            flux_ref[2] = flux_of(kept("ty tz"), kept("yt zt"))
            keep_half("xz tz", 1, kept_half("ty tz", 1))
            keep_half("t x", 1, half(halo_ref, MIXED, 0))
            corner("y corner", rows, T, Y, None, (halo_ref, T_AHEAD, 0))

        def x_and_t_ahead():
            keep("xt tx", mul(whole(base, 0), kept("t x")))
            flux = flux_of(kept_half("xt tx", 0), kept_half("xt tx", 1))
            flux_ref[0, :, low(0), :] = flux_ref[3, :, low(0), :] + flux_ref[3, :, low(1), :] + flux
            flux_ref[0, :, low(1), :] = flux_ref[2, :, low(0), :] + flux_ref[2, :, low(1), :] - flux
            flux_ref[1] = flux_ref[1] - flux_ref[2] - flux_ref[3]
            sum_into("lower a", roll(mul_left_adjoint(kept("xz tz"), kept("z z")), 1))

        def t_behind():
            renew(BEHIND[T])
            behind = face(T, 0, T)
            twice("t behind", behind)
            keep_half("t corner", 1, roll(behind, -1))
            keep_half("behind n", 0, behind)
            keep_half("behind m", 0, face(T, 0, X))
            corner("t corner", 0, Y, T, (halo_ref, BEHIND[T], rows), None)

        def y_lower():
            one = mul(whole(halo_ref, BEHIND[Y]), kept("y corner"))
            sum_into("lower a", mul_left_adjoint(one, kept("y behind")))

        def t_lower():
            renew(BEHIND[T] + 1)
            one = mul(whole(halo_ref, BEHIND[T] + 1), kept("t corner"))
            sum_into("lower b", mul_left_adjoint(one, kept("t behind")))

        def xt_lower():
            fill("xt")
            renew(XT)
            one = mul(kept("behind m"), whole(halo_ref, XT))
            sum_into("lower a", mul_left_adjoint(one, kept("behind n")))

        def finish(pair, name):
            own = whole(base, pair)
            omega = projected(mul(own, kept(name))) + flux_ref[pair]
            gen = (-flow_eps * FRESH[stage]) * omega
            if stage:
                gen = gen + KEPT[stage] * gen_ref[stage, pair]
            if stage < 2:
                gen_ref[stage + 1, pair] = gen
            else:
                keep("moved", mul(exponential(gen), own))
                for d, (p, pos) in PLACE.items():
                    if p == pair:
                        out_ref[d, 0], out_ref[d, 1] = kept_half("moved", pos)

        tasks = [
            (t_ahead, {"ahead", "yt"}),
            (x_faces, {"x", "xy"}),
            (x_and_t_ahead, {"x", "xy", "ahead", "yt"}),
            (xy_corner, {"x", "xy"}),
            (y_lower, {"x", "xy", "yt", "ahead"}),
            (t_behind, {"behind a", "ahead", "yt"}),
            (t_lower, {"behind a", "behind b", "yt", "ahead"}),
            (lambda: finish(1, "lower b"), {"x", "xy", "ahead", "behind a", "behind b", "yt"}),
            (xt_lower, {"xt", "x", "xy", "ahead", "yt", "behind a"}),
            (lambda: finish(0, "lower a"), {"x", "xy", "ahead", "behind a", "yt", "xt"}),
        ]
        here_now = set()
        for groups in ORDER[stage]:
            for group in groups:
                arrive(group, ())
                here_now.add(group)
            ready = [task for task, needs in tasks if needs <= here_now]
            tasks = [(task, needs) for task, needs in tasks if not needs <= here_now]
            for task in ready:
                task()
        assert not tasks
        if stage == 0:
            action = sum(action_terms)
    assert len(stacks) <= stack_ref.shape[0]
    wait_sent(units)
    for k in range(2 if partners else 0):
        span = slot_ref.at[pl.ds(0, len(partners))]
        pltpu.make_async_copy(span, span, act_sem.at[k]).wait()
    total = sum(slot_ref[j] for j in range(sizes[0] * sizes[1]))
    scale = 1.0 / (6.0 * sizes[0] * sizes[1] * block[0] * block[1] * lanes)
    total = jnp.sum(total, axis=1, keepdims=True) * scale
    act_ref[...] = jnp.broadcast_to(total, act_ref.shape)


STACKS = 30
STEPS = (("ahead", "yt"), ("x", "xy"), ("behind a",), ("behind b",), ("xt",))
ORDER = (STEPS, STEPS, STEPS)
VMEM_LIMIT = 55000 * 1024


def solution(mesh):
    sizes = tuple(mesh.shape[axis] for axis in AXES)

    def local(links):
        block = links.shape[4:7]
        lanes = links.shape[7]
        rows = block[0] * block[1] * block[2]
        plan = plan_of(block)
        partners = [
            (i, j, 0) for i in range(sizes[0]) for j in range(sizes[1]) if i or j
        ]
        matrix = (2, 3, 3, rows, lanes)
        both = (2, 3, 3, 2 * rows, lanes)
        f32 = jnp.float32
        vmem = pl.BlockSpec(memory_space=pltpu.VMEM)
        flowed, action = pl.pallas_call(
            functools.partial(kernel, block, sizes, plan, partners),
            out_shape=(
                jax.ShapeDtypeStruct((4,) + matrix, f32),
                jax.ShapeDtypeStruct((block[2], lanes), f32),
            ),
            in_specs=[pl.BlockSpec(memory_space=pltpu.HBM)],
            out_specs=(vmem, vmem),
            scratch_shapes=[
                pltpu.VMEM((2,) + both, f32),
                pltpu.VMEM((2,) + both, f32),
                pltpu.VMEM((SLOTS,) + both, f32),
                pltpu.VMEM((3, 2, 8, 2 * rows, lanes), f32),
                pltpu.VMEM((3, SLOTS, 8, 2 * rows, lanes), f32),
                pltpu.VMEM((STACKS,) + both, f32),
                pltpu.VMEM((4, 8, 2 * rows, lanes), f32),
                pltpu.VMEM((block[2], lanes), f32),
                pltpu.VMEM((sizes[0] * sizes[1], block[2], lanes), f32),
                pltpu.SemaphoreType.DMA((len(SEND_ORDER),)),
                pltpu.SemaphoreType.DMA((2, len(SEND_ORDER))),
                pltpu.SemaphoreType.DMA((2,)),
                pltpu.SemaphoreType.DMA((1,)),
            ],
            compiler_params=pltpu.CompilerParams(
                collective_id=0, has_side_effects=True, vmem_limit_bytes=VMEM_LIMIT
            ),
        )(links.reshape((4,) + matrix))
        return flowed.reshape(links.shape), action[:, 0]

    spec = P(None, None, None, None, "gx", "gy", "ta", None)
    return jax.shard_map(
        local, mesh=mesh, in_specs=(spec,), out_specs=(spec, P("ta")), check_vma=False
    )
```

```python
import functools

import jax
import jax.numpy as jnp
from jax import lax
from jax.experimental import pallas as pl
from jax.experimental.pallas import tpu as pltpu
from jax.sharding import PartitionSpec as P

MESH = pl.DeviceIdType.MESH
AXES = ("gx", "gy", "ta")
flow_eps = 0.1
FRESH = (1.0 / 4.0, 8.0 / 9.0, 3.0 / 4.0)
KEPT = (0.0, -17.0 / 9.0, -1.0)


def mul(a, b):
    def dot(x, y):
        return sum(x[:, k][:, None] * y[k][None] for k in range(3))

    return dot(a[0], b[0]) - dot(a[1], b[1]), dot(a[0], b[1]) + dot(a[1], b[0])


def mul_right_adjoint(a, b):
    def dot(x, y):
        return sum(x[:, k][:, None] * y[:, k][None] for k in range(3))

    return dot(a[0], b[0]) + dot(a[1], b[1]), dot(a[1], b[0]) - dot(a[0], b[1])


def mul_left_adjoint(a, b):
    def dot(x, y):
        return sum(x[k][:, None] * y[k][None] for k in range(3))

    return dot(a[0], b[0]) + dot(a[1], b[1]), dot(a[0], b[1]) - dot(a[1], b[0])


def add(a, b):
    return b if a is None else (a[0] + b[0], a[1] + b[1])


def projected(m):
    r, i = m
    third = (i[0, 0] + i[1, 1] + i[2, 2]) / 3.0
    parts = [i[j, j] - third for j in range(2)]
    for j, k in ((0, 1), (0, 2), (1, 2)):
        parts += [(r[j, k] - r[k, j]) / 2.0, (i[j, k] + i[k, j]) / 2.0]
    return jnp.stack(parts)


def exponential(g):
    h = [g[0], g[1], -(g[0] + g[1])]
    u, v, w = (g[2], g[3]), (g[4], g[5]), (g[6], g[7])
    nu, nv, nw = (z[0] * z[0] + z[1] * z[1] for z in (u, v, w))
    uw = (u[0] * w[0] - u[1] * w[1], u[0] * w[1] + u[1] * w[0])
    diag = [h[0] * h[0] + nu + nv, h[1] * h[1] + nu + nw, h[2] * h[2] + nv + nw]
    p = -0.5 * (diag[0] + diag[1] + diag[2])
    det = (
        h[0] * (h[1] * h[2] - nw)
        - h[1] * nv
        - h[2] * nu
        + 2.0 * (uw[1] * v[0] - uw[0] * v[1])
    )
    s01, s02, s12 = h[0] + h[1], h[0] + h[2], h[1] + h[2]
    square = {
        (0, 1): (
            -s01 * u[1] - (v[0] * w[0] + v[1] * w[1]),
            s01 * u[0] - (v[1] * w[0] - v[0] * w[1]),
        ),
        (0, 2): (-s02 * v[1] + uw[0], s02 * v[0] + uw[1]),
        (1, 2): (
            -s12 * w[1] - (u[0] * v[0] + u[1] * v[1]),
            s12 * w[0] - (u[0] * v[1] - u[1] * v[0]),
        ),
    }
    line = {(0, 1): u, (0, 2): v, (1, 2): w}
    ai4, br4 = det * (-1.0 / 120.0), 0.25 + p * (1.0 / 120.0)
    ai3, br3, bi3, cr3 = (
        det * (-1.0 / 60.0),
        1.0 / 3.0 + p * (1.0 / 60.0),
        ai4 * (1.0 / 3.0),
        br4 * (1.0 / 3.0),
    )
    ai2, br2, bi2, cr2, ci2 = (
        det * cr3 * -0.5,
        0.5 + 0.5 * p * cr3,
        0.5 * ai3,
        0.5 * br3,
        0.5 * bi3,
    )
    ar, ai = 1.0 + det * ci2, -det * cr2
    br, bi, cr, ci = 1.0 + p * cr2, ai2 + p * ci2, br2, bi2
    re = [[None] * 3 for _ in range(3)]
    im = [[None] * 3 for _ in range(3)]
    for j in range(3):
        re[j][j] = ar - bi * h[j] - cr * diag[j]
        im[j][j] = ai + br * h[j] - ci * diag[j]
    for j, k in line:
        x, s = line[j, k], square[j, k]
        even_r, odd_r = br * x[0], bi * x[1]
        even_i, odd_i = br * x[1], bi * x[0]
        cs = (cr * s[0], ci * s[1], cr * s[1], ci * s[0])
        re[j][k] = (even_r - odd_r) + (cs[0] - cs[1])
        im[j][k] = (even_i + odd_i) + (cs[2] + cs[3])
        re[k][j] = -(even_r + odd_r) + (cs[0] + cs[1])
        im[k][j] = (even_i - odd_i) + (cs[3] - cs[2])
    return (
        jnp.stack([jnp.stack(row) for row in re]),
        jnp.stack([jnp.stack(row) for row in im]),
    )


def chart(x, rest):
    length = sum(y * y for y in rest)
    first = jnp.where(length < 1e-30, 1e-15, rest[0])
    length = jnp.maximum(length, 1e-30)
    scale = jnp.where(x < 0.0, 1.0 - x, 1.0) / jnp.where(x < 0.0, length, 1.0 + x)
    return [scale * y for y in [first] + rest[1:]]


def frame(y):
    q = 2.0 / (1.0 + sum(v * v for v in y))
    return q, q / (1.0 + y[0] * y[0])


def encode(w):
    r, i = w
    y = chart(r[0, 0], [i[0, 0], r[0, 1], i[0, 1], r[0, 2], i[0, 2]])
    f = frame(y)[1]
    kr = r[1, 0] + y[0] * i[1, 0] + y[1] * r[1, 1] + y[2] * i[1, 1] + y[3] * r[1, 2] + y[4] * i[1, 2]
    ki = i[1, 0] - y[0] * r[1, 0] + y[1] * i[1, 1] - y[2] * r[1, 1] + y[3] * i[1, 2] - y[4] * r[1, 2]
    mr, mi = f * (kr + y[0] * ki), f * (ki - y[0] * kr)
    g = []
    for k in (1, 2):
        u, v = y[2 * k - 1], y[2 * k]
        g += [r[1, k] - (u * mr - v * mi), i[1, k] - (u * mi + v * mr)]
    return jnp.stack(y + chart(g[0], g[1:]))


def decode(code):
    y, z = [code[k] for k in range(5)], [code[k] for k in range(5, 8)]
    q, f = frame(y)
    t = 2.0 / (1.0 + sum(v * v for v in z))
    g = [t - 1.0] + [t * v for v in z]
    kr = y[1] * g[0] + y[2] * g[1] + y[3] * g[2] + y[4] * g[3]
    ki = y[1] * g[1] - y[2] * g[0] + y[3] * g[3] - y[4] * g[2]
    mr, mi = f * (kr - y[0] * ki), f * (ki + y[0] * kr)
    r = [[q - 1.0, q * y[1], q * y[3]], [y[0] * mi - mr]]
    i = [[q * y[0], q * y[2], q * y[4]], [-mi - y[0] * mr]]
    for k in (1, 2):
        u, v = y[2 * k - 1], y[2 * k]
        r[1].append(g[2 * k - 2] - (u * mr - v * mi))
        i[1].append(g[2 * k - 1] - (u * mi + v * mr))
    r.append([])
    i.append([])
    for j in range(3):
        k, l = (j + 1) % 3, (j + 2) % 3
        r[2].append(
            (r[0][k] * r[1][l] - i[0][k] * i[1][l]) - (r[0][l] * r[1][k] - i[0][l] * i[1][k])
        )
        i[2].append(
            (r[0][l] * i[1][k] + i[0][l] * r[1][k]) - (r[0][k] * i[1][l] + i[0][k] * r[1][l])
        )
    return (
        jnp.stack([jnp.stack(row) for row in r]),
        jnp.stack([jnp.stack(row) for row in i]),
    )


def runs(pairs):
    out = []
    for to, frm in pairs:
        if out and to == out[-1][0] + out[-1][2] and frm == out[-1][1] + out[-1][2]:
            out[-1][2] += 1
        else:
            out.append([to, frm, 1])
    return out


def neighbour_rows(block, offset):
    lx, ly, lt = block
    found = {}
    for row in range(lx * ly * lt):
        site = (row // (ly * lt), row // lt % ly, row % lt)
        moved = [site[k] + offset[k] for k in range(3)]
        step = tuple(moved[k] // block[k] for k in range(3))
        at = [moved[k] % block[k] for k in range(3)]
        frm = (at[0] * ly + at[1]) * lt + at[2]
        found.setdefault(step, []).append((row, frm))
    return found


def unit(k, sign):
    return tuple(sign if j == k else 0 for j in range(3))


X, Y, T, Z = 0, 1, 2, 3
PLACE = {X: (0, 0), T: (0, 1), Y: (1, 0), Z: (1, 1)}
BEHIND = {T: 0, Y: 6}
T_AHEAD, X_PACK, MIXED, Y_AHEAD, XT = 2, 3, 5, 8, 10
SLOTS = 11
SEND_ORDER = ("xt", "yt", "xy", "ahead", "behind a", "behind b", "x", "y")


def cover(pairs):
    to, frm = min(pairs)
    assert all(a - b == to - frm for a, b in pairs)
    return to, frm, max(pairs)[0] - to + 1


def local_runs(block, k, sign):
    return runs(neighbour_rows(block, unit(k, sign)).get((0, 0, 0), []))


def plan_of(block):
    rows = block[0] * block[1] * block[2]
    n = rows // block[0]
    assert block[0] > 1 and block[1] > 1 and block[2] == 1
    remote, fills, corners = [], [], {}

    def send(group, pair, pairs, frm, count, slot, to, step):
        remote.append((group, pair, pairs, frm, count, slot, to, step))

    for k in range(3):
        for half, sign in ((0, -1), (1, 1)):
            for step, pairs in neighbour_rows(block, unit(k, sign)).items():
                if not any(step):
                    continue
                to, frm, count = cover(pairs)
                if k == Y:
                    slot = Y_AHEAD if half else BEHIND[Y]
                    send("y", 0, 2, frm, rows + count, slot, to, step)
                elif k == X and half:
                    send("x", 0, 2, rows + frm, n, X_PACK, 3 * n, step)
                    send("x", 1, 1, frm, n, X_PACK + 1, 2 * n, step)
                elif k == X:
                    send("x", 0, 2, frm, n, X_PACK, 0, step)
                    send("x", 0, 2, rows + frm, n, X_PACK, n, step)
                elif half:
                    send("ahead", 0, 1, frm, rows, MIXED, 0, step)
                    send("ahead", 1, 1, frm, 2 * rows, T_AHEAD, 0, step)
                else:
                    send("behind a", 0, 1, frm, 2 * rows, BEHIND[T], 0, step)
                    send("behind b", 1, 1, frm, 2 * rows, BEHIND[T] + 1, 0, step)
    for half, sign in ((0, -1), (1, 1)):
        for d, (pair, at) in PLACE.items():
            for to, frm, count in local_runs(block, Y, sign):
                slot = (Y_AHEAD if half else BEHIND[Y]) + pair
                fills.append(("y", None, pair, at * rows + frm, slot, at * rows + to, count))
    free = {"xy": (X_PACK, 2 * n, 3 * n), "t": (XT, 0, 2 * rows)}
    for m, n_dir in ((X, T), (T, X), (X, Y), (Y, X), (T, Y), (Y, T)):
        ahead, behind = unit(m, 1), unit(n_dir, -1)
        rows_ahead = dict(neighbour_rows(block, ahead).get((0, 0, 0), []))
        rows_behind = dict(neighbour_rows(block, behind).get((0, 0, 0), []))
        offset = tuple(ahead[j] + behind[j] for j in range(3))
        group = "xt" if Y not in (m, n_dir) else "yt" if T in (m, n_dir) else "xy"
        pair, at = PLACE[n_dir]
        from_minus, from_plus, placed = [], [], []
        for step, pairs in neighbour_rows(block, offset).items():
            outer = []
            for to, frm in pairs:
                if to in rows_ahead:
                    from_minus.append((to, rows_ahead[to]))
                elif to in rows_behind:
                    from_plus.append((to, rows_behind[to]))
                else:
                    outer.append((to, frm))
            for to, frm, count in runs(outer):
                space = "xy" if group == "xy" else "t"
                slot, row, end = free[space]
                free[space] = slot, row + count, end
                assert row + count <= end
                placed.append((to, slot, row, count))
                send(group, pair, 1, at * rows + frm, count, slot, row, step)
        corners[m, n_dir] = placed, runs(sorted(from_minus)), runs(sorted(from_plus))
    remote.sort(key=lambda item: SEND_ORDER.index(item[0]))
    return remote, fills, corners


def kernel(
    block,
    sizes,
    plan,
    partners,
    w_hbm,
    out_ref,
    act_ref,
    first_ref,
    cur_ref,
    halo_ref,
    gen_ref,
    gen_halo_ref,
    stack_ref,
    flux_ref,
    part_ref,
    slot_ref,
    send_sem,
    recv_sem,
    act_sem,
    load_sem,
):
    remote, fills, corners = plan
    rows = block[0] * block[1] * block[2]
    n = rows // block[0]
    lanes = w_hbm.shape[-1]
    here = [lax.axis_index(axis) for axis in AXES]

    def device(step):
        return tuple(lax.rem(here[k] + step[k] + sizes[k], sizes[k]) for k in range(3))

    steps = [item[-1] for item in remote] + partners
    greeted = sorted({tuple(s % size for s, size in zip(step, sizes)) for step in steps})
    barrier = pltpu.get_barrier_semaphore()
    for step in reversed(greeted):
        pl.semaphore_signal(barrier, inc=1, device_id=device(step), device_id_type=MESH)
    for d, (pair, pos) in PLACE.items():
        load = pltpu.make_async_copy(
            w_hbm.at[d], first_ref.at[pair, :, :, :, pl.ds(pos * rows, rows), :], load_sem.at[0]
        )
        load.start()
    pltpu.make_async_copy(first_ref, first_ref, load_sem.at[0]).wait()
    for pair in range(2):
        gen_ref[0, pair] = encode((first_ref[pair, 0], first_ref[pair, 1]))
    pl.semaphore_wait(barrier, len(greeted))

    units, stacks = {}, {}

    def wait_bytes(count, sem):
        depth = max(k for k in range(1, 2 * rows + 1) if count % k == 0 and count // k <= SLOTS)
        span = gen_halo_ref.at[0, pl.ds(0, count // depth), :, pl.ds(0, depth), :]
        pltpu.make_async_copy(span, span, sem).wait()

    def wait_sent(units):
        for group, count in units.items():
            wait_bytes(count, send_sem.at[SEND_ORDER.index(group)])


    def low(pos):
        return slice(pos * rows, (pos + 1) * rows)

    def whole(ref, index):
        return ref[index, 0], ref[index, 1]

    def half(ref, index, pos):
        return ref[index, 0, :, :, low(pos), :], ref[index, 1, :, :, low(pos), :]

    def stack(name):
        return stacks.setdefault(name, len(stacks))

    def keep(name, value):
        index = stack(name)
        stack_ref[index, 0], stack_ref[index, 1] = value

    def keep_half(name, pos, value):
        index = stack(name)
        stack_ref[index, 0, :, :, low(pos), :] = value[0]
        stack_ref[index, 1, :, :, low(pos), :] = value[1]

    def twice(name, value):
        keep_half(name, 0, value)
        keep_half(name, 1, value)

    def kept(name):
        return whole(stack_ref, stacks[name])

    def kept_half(name, pos):
        return half(stack_ref, stacks[name], pos)

    def roll(pair, shift):
        return tuple(pltpu.roll(x, shift % lanes, axis=3) for x in pair)

    def face(k, side, d):
        pair, pos = PLACE[d]
        return half(halo_ref, (Y_AHEAD if side else BEHIND[k]) + pair, pos)

    def copy_rows(name, to, ref, index, frm, count):
        slot = stack(name)
        stack_ref[slot, :, :, :, to : to + count, :] = ref[index, :, :, :, frm : frm + count, :]

    for stage in range(3):
        base = first_ref if stage == 0 else cur_ref
        wait_sent(units)
        units = {}
        for group, pair, pairs, frm, count, slot, to, step in remote:
            span, into = pl.ds(pair, pairs), pl.ds(slot, pairs)
            src = gen_ref.at[stage, span, :, pl.ds(frm, count), :]
            dst = gen_halo_ref.at[stage, into, :, pl.ds(to, count), :]
            copy = pltpu.make_async_remote_copy(
                src_ref=src,
                dst_ref=dst,
                send_sem=send_sem.at[SEND_ORDER.index(group)],
                recv_sem=recv_sem.at[stage % 2, SEND_ORDER.index(group)],
                device_id=device(tuple(-s for s in step)),
                device_id_type=MESH,
            )
            units[group] = units.get(group, 0) + pairs * count
            copy.start()

        if stage == 1:
            lt = block[2]
            for t in range(lt):
                part_ref[t : t + 1, :] = sum(action[r : r + 1] for r in range(t, rows, lt))
            mine = here[0] * sizes[1] + here[1]
            for step in partners:
                copy = pltpu.make_async_remote_copy(
                    src_ref=part_ref,
                    dst_ref=slot_ref.at[mine],
                    send_sem=act_sem.at[0],
                    recv_sem=act_sem.at[1],
                    device_id=device(step),
                    device_id_type=MESH,
                )
                copy.start()
            slot_ref[mine] = part_ref[...]

        def fill(wanted):
            for group, source, pair, frm, slot, to, count in fills:
                if group != wanted:
                    continue
                ref = gen_ref.at[stage, pair] if source is None else gen_halo_ref.at[stage, source]
                gen_halo_ref[stage, slot, :, to : to + count, :] = ref[:, frm : frm + count, :]

        def renew(slot, count=2 * rows):
            code = gen_halo_ref[stage, slot, :, 0:count, :]
            if stage == 0:
                new = decode(code)
            else:
                old = halo_ref[slot, :, :, :, 0:count, :]
                new = mul(exponential(code), (old[0], old[1]))
            halo_ref[slot, 0, :, :, 0:count, :] = new[0]
            halo_ref[slot, 1, :, :, 0:count, :] = new[1]

        def arrive(group, slots):
            if group in units:
                wait_bytes(units[group], recv_sem.at[stage % 2, SEND_ORDER.index(group)])
            fill(group)
            for slot in slots:
                renew(slot)

        def count_action(plaq):
            trace = plaq[0][0, 0] + plaq[0][1, 1] + plaq[0][2, 2]
            term = 1.0 - trace / 3.0
            return term if term.shape[0] == rows else term[:rows] + term[rows:]

        action_terms = []

        def flux_of(one, two):
            plaq = mul_right_adjoint(one, two)
            if stage == 0:
                action_terms.append(count_action(plaq))
            return projected(plaq)

        def centre(d):
            return half(base, *PLACE[d])

        if stage:
            for pair in range(2):
                before = whole(first_ref if stage == 1 else cur_ref, pair)
                moved = mul(exponential(gen_ref[stage, pair]), before)
                cur_ref[pair, 0], cur_ref[pair, 1] = moved
        for d, name in ((X, "x x"), (T, "t t"), (Z, "z z")):
            twice(name, centre(d))
        for d, name in ((X, "x ahead"), (T, "t ahead"), (Y, "y z ahead")):
            keep_half(name, 1, roll(centre(d), -1))

        for d, (pair, pos) in PLACE.items():
            for to, frm, count in local_runs(block, X, -1):
                copy_rows(("xb a", "xb b")[pair], pos * rows + to, base, pair, pos * rows + frm, count)
            if d == X:
                continue
            for to, frm, count in local_runs(block, X, 1):
                name, at = ("t x", 0) if d == T else ("xa yz", pos * rows)
                copy_rows(name, at + to, base, pair, pos * rows + frm, count)

        arrive("y", range(BEHIND[Y], Y_AHEAD + 2))
        for d, name in ((X, "x ahead"), (T, "t ahead"), (Z, "y z ahead")):
            keep_half(name, 0, face(Y, 1, d))
        behind = face(Y, 0, Y)
        twice("y behind", behind)
        yz = whole(base, 1)
        keep("yx zx", mul(yz, kept("x ahead")))
        keep("yt zt", mul(yz, kept("t ahead")))
        keep("yz zy", mul(yz, kept("y z ahead")))
        one = kept_half("yz zy", 0)
        flux = flux_of(one, kept_half("yz zy", 1))
        flux_ref[1, :, low(0), :] = flux
        flux_ref[1, :, low(1), :] = -flux
        keep_half("lower b", 0, roll(mul_left_adjoint(one, centre(Z)), 1))
        one = mul(face(Y, 0, Z), roll(behind, -1))
        keep_half("lower b", 1, mul_left_adjoint(one, behind))

        def sum_into(name, value):
            keep(name, add(kept(name) if name in begun else None, value))
            begun.add(name)

        begun = {"lower b"}

        def x_faces():
            for slot in (X_PACK, X_PACK + 1):
                renew(slot)
            to = cover(sum((p for q, p in neighbour_rows(block, unit(X, 1)).items() if any(q)), []))[0]
            copy_rows("xa yz", to, halo_ref, X_PACK + 1, 2 * n, n)
            copy_rows("xa yz", rows + to, halo_ref, X_PACK + 1, 3 * n, n)
            copy_rows("t x", to, halo_ref, X_PACK, 3 * n, n)
            to = cover(sum((p for q, p in neighbour_rows(block, unit(X, -1)).items() if any(q)), []))[0]
            for pos in range(2):
                copy_rows("xb a", pos * rows + to, halo_ref, X_PACK, pos * n, n)
                copy_rows("xb b", pos * rows + to, halo_ref, X_PACK + 1, pos * n, n)
            keep("xy xz", mul(kept("x x"), kept("xa yz")))
            flux_ref[3] = flux_of(kept("xy xz"), kept("yx zx"))
            keep_half("xz tz", 0, kept_half("xy xz", 1))
            behind = kept_half("xb a", 0)
            twice("x behind", behind)
            keep_half("x corner", 1, roll(behind, -1))
            keep_half("behind n", 1, behind)
            keep_half("behind m", 1, kept_half("xb a", 1))

        def outer(name, at, m, n_dir):
            for to, slot, row, count in corners[m, n_dir][0]:
                copy_rows(name, at + to, halo_ref, slot, row, count)

        def inner(name, at, m, n_dir, minus, plus):
            for found, source in zip(corners[m, n_dir][1:], (minus, plus)):
                for to, frm, count in found:
                    copy_rows(name, at + to, source[0], source[1], source[2] + frm, count)

        def xy_corner():
            outer("y corner", 0, X, Y)
            outer("x corner", 0, Y, X)
            inner("y corner", 0, X, Y, (halo_ref, BEHIND[Y] + 1, 0), (stack_ref, stacks["xa yz"], 0))
            inner("x corner", 0, Y, X, (stack_ref, stacks["xb a"], 0), (halo_ref, Y_AHEAD, 0))
            one = mul(kept("xb b"), kept("x corner"))
            sum_into("lower b", mul_left_adjoint(one, kept("x behind")))

        def t_ahead():
            renew(T_AHEAD)
            renew(MIXED, rows)
            keep("ty tz", mul(kept("t t"), whole(halo_ref, T_AHEAD)))
            flux_ref[2] = flux_of(kept("ty tz"), kept("yt zt"))
            keep_half("xz tz", 1, kept_half("ty tz", 1))
            keep_half("t x", 1, half(halo_ref, MIXED, 0))
            inner("y corner", rows, T, Y, None, (halo_ref, T_AHEAD, 0))
            inner("xt corner", rows, T, X, None, (halo_ref, MIXED, 0))

        def x_and_t_ahead():
            keep("xt tx", mul(whole(base, 0), kept("t x")))
            flux = flux_of(kept_half("xt tx", 0), kept_half("xt tx", 1))
            flux_ref[0, :, low(0), :] = flux_ref[3, :, low(0), :] + flux_ref[3, :, low(1), :] + flux
            flux_ref[0, :, low(1), :] = flux_ref[2, :, low(0), :] + flux_ref[2, :, low(1), :] - flux
            flux_ref[1] = flux_ref[1] - flux_ref[2] - flux_ref[3]
            sum_into("lower a", roll(mul_left_adjoint(kept("xz tz"), kept("z z")), 1))

        def t_behind():
            renew(BEHIND[T])
            behind = face(T, 0, T)
            twice("t behind", behind)
            keep_half("t corner", 1, roll(behind, -1))
            keep_half("behind n", 0, behind)
            keep_half("behind m", 0, face(T, 0, X))
            inner("t corner", 0, Y, T, (halo_ref, BEHIND[T], rows), None)
            inner("xt corner", 0, X, T, (halo_ref, BEHIND[T], rows), None)

        def t_corners():
            renew(XT)
            outer("y corner", rows, T, Y)
            outer("t corner", 0, Y, T)
            outer("xt corner", 0, X, T)
            outer("xt corner", rows, T, X)

        def y_lower():
            one = mul(whole(halo_ref, BEHIND[Y]), kept("y corner"))
            sum_into("lower a", mul_left_adjoint(one, kept("y behind")))

        def t_lower():
            renew(BEHIND[T] + 1)
            one = mul(whole(halo_ref, BEHIND[T] + 1), kept("t corner"))
            sum_into("lower b", mul_left_adjoint(one, kept("t behind")))

        def xt_lower():
            one = mul(kept("behind m"), kept("xt corner"))
            sum_into("lower a", mul_left_adjoint(one, kept("behind n")))

        def finish(pair, name):
            own = whole(base, pair)
            omega = projected(mul(own, kept(name))) + flux_ref[pair]
            gen = (-flow_eps * FRESH[stage]) * omega
            if stage:
                gen = gen + KEPT[stage] * gen_ref[stage, pair]
            if stage < 2:
                gen_ref[stage + 1, pair] = gen
            else:
                keep("moved", mul(exponential(gen), own))
                for d, (p, pos) in PLACE.items():
                    if p == pair:
                        out_ref[d, 0], out_ref[d, 1] = kept_half("moved", pos)

        late = {"x", "xy", "ahead", "behind a", "behind b", "yt", "xt"}
        tasks = [
            (t_ahead, {"ahead"}),
            (x_faces, {"x", "xy"}),
            (x_and_t_ahead, {"x", "xy", "ahead"}),
            (xy_corner, {"x", "xy"}),
            (t_behind, {"behind a", "ahead"}),
            (t_corners, {"yt", "xt"}),
            (y_lower, late - {"behind b"}),
            (xt_lower, late - {"behind b"}),
            (lambda: finish(0, "lower a"), late - {"behind b"}),
            (t_lower, late),
            (lambda: finish(1, "lower b"), late),
        ]
        here_now = set()
        for groups in ORDER[stage]:
            for group in groups:
                arrive(group, ())
                here_now.add(group)
            ready = [task for task, needs in tasks if needs <= here_now]
            tasks = [(task, needs) for task, needs in tasks if not needs <= here_now]
            for task in ready:
                task()
        assert not tasks
        if stage == 0:
            action = sum(action_terms)
    assert len(stacks) <= stack_ref.shape[0]
    wait_sent(units)
    for k in range(2 if partners else 0):
        span = slot_ref.at[pl.ds(0, len(partners))]
        pltpu.make_async_copy(span, span, act_sem.at[k]).wait()
    total = sum(slot_ref[j] for j in range(sizes[0] * sizes[1]))
    scale = 1.0 / (6.0 * sizes[0] * sizes[1] * block[0] * block[1] * lanes)
    total = jnp.sum(total, axis=1, keepdims=True) * scale
    act_ref[...] = jnp.broadcast_to(total, act_ref.shape)


STACKS = 30
STEPS = (("ahead",), ("x", "xy"), ("behind a", "yt", "xt"), ("behind b",))
ORDER = (STEPS, STEPS, STEPS)
VMEM_LIMIT = 55000 * 1024


def solution(mesh):
    sizes = tuple(mesh.shape[axis] for axis in AXES)

    def local(links):
        block = links.shape[4:7]
        lanes = links.shape[7]
        rows = block[0] * block[1] * block[2]
        plan = plan_of(block)
        partners = [
            (i, j, 0) for i in range(sizes[0]) for j in range(sizes[1]) if i or j
        ]
        matrix = (2, 3, 3, rows, lanes)
        both = (2, 3, 3, 2 * rows, lanes)
        f32 = jnp.float32
        vmem = pl.BlockSpec(memory_space=pltpu.VMEM)
        flowed, action = pl.pallas_call(
            functools.partial(kernel, block, sizes, plan, partners),
            out_shape=(
                jax.ShapeDtypeStruct((4,) + matrix, f32),
                jax.ShapeDtypeStruct((block[2], lanes), f32),
            ),
            in_specs=[pl.BlockSpec(memory_space=pltpu.HBM)],
            out_specs=(vmem, vmem),
            scratch_shapes=[
                pltpu.VMEM((2,) + both, f32),
                pltpu.VMEM((2,) + both, f32),
                pltpu.VMEM((SLOTS,) + both, f32),
                pltpu.VMEM((3, 2, 8, 2 * rows, lanes), f32),
                pltpu.VMEM((3, SLOTS, 8, 2 * rows, lanes), f32),
                pltpu.VMEM((STACKS,) + both, f32),
                pltpu.VMEM((4, 8, 2 * rows, lanes), f32),
                pltpu.VMEM((block[2], lanes), f32),
                pltpu.VMEM((sizes[0] * sizes[1], block[2], lanes), f32),
                pltpu.SemaphoreType.DMA((len(SEND_ORDER),)),
                pltpu.SemaphoreType.DMA((2, len(SEND_ORDER))),
                pltpu.SemaphoreType.DMA((2,)),
                pltpu.SemaphoreType.DMA((1,)),
            ],
            compiler_params=pltpu.CompilerParams(
                collective_id=0, has_side_effects=True, vmem_limit_bytes=VMEM_LIMIT
            ),
        )(links.reshape((4,) + matrix))
        return flowed.reshape(links.shape), action[:, 0]

    spec = P(None, None, None, None, "gx", "gy", "ta", None)
    return jax.shard_map(
        local, mesh=mesh, in_specs=(spec,), out_specs=(spec, P("ta")), check_vma=False
    )
```

```python
import functools

import jax
import jax.numpy as jnp
from jax import lax
from jax.experimental import pallas as pl
from jax.experimental.pallas import tpu as pltpu
from jax.sharding import PartitionSpec as P

MESH = pl.DeviceIdType.MESH
AXES = ("gx", "gy", "ta")
flow_eps = 0.1
FRESH = (1.0 / 4.0, 8.0 / 9.0, 3.0 / 4.0)
KEPT = (0.0, -17.0 / 9.0, -1.0)


def mul(a, b):
    def dot(x, y):
        return sum(x[:, k][:, None] * y[k][None] for k in range(3))

    return dot(a[0], b[0]) - dot(a[1], b[1]), dot(a[0], b[1]) + dot(a[1], b[0])


def mul_right_adjoint(a, b):
    def dot(x, y):
        return sum(x[:, k][:, None] * y[:, k][None] for k in range(3))

    return dot(a[0], b[0]) + dot(a[1], b[1]), dot(a[1], b[0]) - dot(a[0], b[1])


def mul_left_adjoint(a, b):
    def dot(x, y):
        return sum(x[k][:, None] * y[k][None] for k in range(3))

    return dot(a[0], b[0]) + dot(a[1], b[1]), dot(a[0], b[1]) - dot(a[1], b[0])


def add(a, b):
    return b if a is None else (a[0] + b[0], a[1] + b[1])


def projected(m):
    r, i = m
    third = (i[0, 0] + i[1, 1] + i[2, 2]) / 3.0
    parts = [i[j, j] - third for j in range(2)]
    for j, k in ((0, 1), (0, 2), (1, 2)):
        parts += [(r[j, k] - r[k, j]) / 2.0, (i[j, k] + i[k, j]) / 2.0]
    return jnp.stack(parts)


def exponential(g):
    h = [g[0], g[1], -(g[0] + g[1])]
    u, v, w = (g[2], g[3]), (g[4], g[5]), (g[6], g[7])
    nu, nv, nw = (z[0] * z[0] + z[1] * z[1] for z in (u, v, w))
    uw = (u[0] * w[0] - u[1] * w[1], u[0] * w[1] + u[1] * w[0])
    diag = [h[0] * h[0] + nu + nv, h[1] * h[1] + nu + nw, h[2] * h[2] + nv + nw]
    p = -0.5 * (diag[0] + diag[1] + diag[2])
    det = (
        h[0] * (h[1] * h[2] - nw)
        - h[1] * nv
        - h[2] * nu
        + 2.0 * (uw[1] * v[0] - uw[0] * v[1])
    )
    s01, s02, s12 = h[0] + h[1], h[0] + h[2], h[1] + h[2]
    square = {
        (0, 1): (
            -s01 * u[1] - (v[0] * w[0] + v[1] * w[1]),
            s01 * u[0] - (v[1] * w[0] - v[0] * w[1]),
        ),
        (0, 2): (-s02 * v[1] + uw[0], s02 * v[0] + uw[1]),
        (1, 2): (
            -s12 * w[1] - (u[0] * v[0] + u[1] * v[1]),
            s12 * w[0] - (u[0] * v[1] - u[1] * v[0]),
        ),
    }
    line = {(0, 1): u, (0, 2): v, (1, 2): w}
    ai4, br4 = det * (-1.0 / 120.0), 0.25 + p * (1.0 / 120.0)
    ai3, br3, bi3, cr3 = (
        det * (-1.0 / 60.0),
        1.0 / 3.0 + p * (1.0 / 60.0),
        ai4 * (1.0 / 3.0),
        br4 * (1.0 / 3.0),
    )
    ai2, br2, bi2, cr2, ci2 = (
        det * cr3 * -0.5,
        0.5 + 0.5 * p * cr3,
        0.5 * ai3,
        0.5 * br3,
        0.5 * bi3,
    )
    ar, ai = 1.0 + det * ci2, -det * cr2
    br, bi, cr, ci = 1.0 + p * cr2, ai2 + p * ci2, br2, bi2
    re = [[None] * 3 for _ in range(3)]
    im = [[None] * 3 for _ in range(3)]
    for j in range(3):
        re[j][j] = ar - bi * h[j] - cr * diag[j]
        im[j][j] = ai + br * h[j] - ci * diag[j]
    for j, k in line:
        x, s = line[j, k], square[j, k]
        even_r, odd_r = br * x[0], bi * x[1]
        even_i, odd_i = br * x[1], bi * x[0]
        cs = (cr * s[0], ci * s[1], cr * s[1], ci * s[0])
        re[j][k] = (even_r - odd_r) + (cs[0] - cs[1])
        im[j][k] = (even_i + odd_i) + (cs[2] + cs[3])
        re[k][j] = -(even_r + odd_r) + (cs[0] + cs[1])
        im[k][j] = (even_i - odd_i) + (cs[3] - cs[2])
    return (
        jnp.stack([jnp.stack(row) for row in re]),
        jnp.stack([jnp.stack(row) for row in im]),
    )


def chart(x, rest):
    length = sum(y * y for y in rest)
    first = jnp.where(length < 1e-30, 1e-15, rest[0])
    length = jnp.maximum(length, 1e-30)
    scale = jnp.where(x < 0.0, 1.0 - x, 1.0) / jnp.where(x < 0.0, length, 1.0 + x)
    return [scale * y for y in [first] + rest[1:]]


def frame(y):
    q = 2.0 / (1.0 + sum(v * v for v in y))
    return q, q / (1.0 + y[0] * y[0])


def encode(w):
    r, i = w
    y = chart(r[0, 0], [i[0, 0], r[0, 1], i[0, 1], r[0, 2], i[0, 2]])
    f = frame(y)[1]
    kr = r[1, 0] + y[0] * i[1, 0] + y[1] * r[1, 1] + y[2] * i[1, 1] + y[3] * r[1, 2] + y[4] * i[1, 2]
    ki = i[1, 0] - y[0] * r[1, 0] + y[1] * i[1, 1] - y[2] * r[1, 1] + y[3] * i[1, 2] - y[4] * r[1, 2]
    mr, mi = f * (kr + y[0] * ki), f * (ki - y[0] * kr)
    g = []
    for k in (1, 2):
        u, v = y[2 * k - 1], y[2 * k]
        g += [r[1, k] - (u * mr - v * mi), i[1, k] - (u * mi + v * mr)]
    return jnp.stack(y + chart(g[0], g[1:]))


def decode(code):
    y, z = [code[k] for k in range(5)], [code[k] for k in range(5, 8)]
    q, f = frame(y)
    t = 2.0 / (1.0 + sum(v * v for v in z))
    g = [t - 1.0] + [t * v for v in z]
    kr = y[1] * g[0] + y[2] * g[1] + y[3] * g[2] + y[4] * g[3]
    ki = y[1] * g[1] - y[2] * g[0] + y[3] * g[3] - y[4] * g[2]
    mr, mi = f * (kr - y[0] * ki), f * (ki + y[0] * kr)
    r = [[q - 1.0, q * y[1], q * y[3]], [y[0] * mi - mr]]
    i = [[q * y[0], q * y[2], q * y[4]], [-mi - y[0] * mr]]
    for k in (1, 2):
        u, v = y[2 * k - 1], y[2 * k]
        r[1].append(g[2 * k - 2] - (u * mr - v * mi))
        i[1].append(g[2 * k - 1] - (u * mi + v * mr))
    r.append([])
    i.append([])
    for j in range(3):
        k, l = (j + 1) % 3, (j + 2) % 3
        r[2].append(
            (r[0][k] * r[1][l] - i[0][k] * i[1][l]) - (r[0][l] * r[1][k] - i[0][l] * i[1][k])
        )
        i[2].append(
            (r[0][l] * i[1][k] + i[0][l] * r[1][k]) - (r[0][k] * i[1][l] + i[0][k] * r[1][l])
        )
    return (
        jnp.stack([jnp.stack(row) for row in r]),
        jnp.stack([jnp.stack(row) for row in i]),
    )


def runs(pairs):
    out = []
    for to, frm in pairs:
        if out and to == out[-1][0] + out[-1][2] and frm == out[-1][1] + out[-1][2]:
            out[-1][2] += 1
        else:
            out.append([to, frm, 1])
    return out


def neighbour_rows(block, offset):
    lx, ly, lt = block
    found = {}
    for row in range(lx * ly * lt):
        site = (row // (ly * lt), row // lt % ly, row % lt)
        moved = [site[k] + offset[k] for k in range(3)]
        step = tuple(moved[k] // block[k] for k in range(3))
        at = [moved[k] % block[k] for k in range(3)]
        frm = (at[0] * ly + at[1]) * lt + at[2]
        found.setdefault(step, []).append((row, frm))
    return found


def unit(k, sign):
    return tuple(sign if j == k else 0 for j in range(3))


X, Y, T, Z = 0, 1, 2, 3
PLACE = {X: (0, 0), T: (0, 1), Y: (1, 0), Z: (1, 1)}
BEHIND = {T: 0, Y: 6}
T_AHEAD, X_PACK, MIXED, Y_AHEAD, XT = 2, 3, 5, 8, 10
SLOTS = 11
SEND_ORDER = ("xt", "yt", "xy", "ahead", "behind a", "behind b", "x", "y")


def cover(pairs):
    to, frm = min(pairs)
    assert all(a - b == to - frm for a, b in pairs)
    return to, frm, max(pairs)[0] - to + 1


def local_runs(block, k, sign):
    return runs(neighbour_rows(block, unit(k, sign)).get((0, 0, 0), []))


def plan_of(block):
    rows = block[0] * block[1] * block[2]
    n = rows // block[0]
    assert block[0] > 1 and block[1] > 1 and block[2] == 1
    remote, fills, corners = [], [], {}

    def send(group, pair, pairs, frm, count, slot, to, step):
        remote.append((group, pair, pairs, frm, count, slot, to, step))

    for k in range(3):
        for half, sign in ((0, -1), (1, 1)):
            for step, pairs in neighbour_rows(block, unit(k, sign)).items():
                if not any(step):
                    continue
                to, frm, count = cover(pairs)
                if k == Y:
                    slot = Y_AHEAD if half else BEHIND[Y]
                    send("y", 0, 2, frm, rows + count, slot, to, step)
                elif k == X and half:
                    send("x", 0, 2, rows + frm, n, X_PACK, 3 * n, step)
                    send("x", 1, 1, frm, n, X_PACK + 1, 2 * n, step)
                elif k == X:
                    send("x", 0, 2, frm, n, X_PACK, 0, step)
                    send("x", 0, 2, rows + frm, n, X_PACK, n, step)
                elif half:
                    send("ahead", 0, 1, frm, rows, MIXED, 0, step)
                    send("ahead", 1, 1, frm, 2 * rows, T_AHEAD, 0, step)
                else:
                    send("behind a", 0, 1, frm, 2 * rows, BEHIND[T], 0, step)
                    send("behind b", 1, 1, frm, 2 * rows, BEHIND[T] + 1, 0, step)
    for half, sign in ((0, -1), (1, 1)):
        for d, (pair, at) in PLACE.items():
            for to, frm, count in local_runs(block, Y, sign):
                slot = (Y_AHEAD if half else BEHIND[Y]) + pair
                fills.append(("y", None, pair, at * rows + frm, slot, at * rows + to, count))
    free = {"xy": (X_PACK, 2 * n, 3 * n), "t": (XT, 0, 2 * rows)}
    for m, n_dir in ((X, T), (T, X), (X, Y), (Y, X), (T, Y), (Y, T)):
        ahead, behind = unit(m, 1), unit(n_dir, -1)
        rows_ahead = dict(neighbour_rows(block, ahead).get((0, 0, 0), []))
        rows_behind = dict(neighbour_rows(block, behind).get((0, 0, 0), []))
        offset = tuple(ahead[j] + behind[j] for j in range(3))
        group = "xt" if Y not in (m, n_dir) else "yt" if T in (m, n_dir) else "xy"
        pair, at = PLACE[n_dir]
        from_minus, from_plus, placed = [], [], []
        for step, pairs in neighbour_rows(block, offset).items():
            outer = []
            for to, frm in pairs:
                if to in rows_ahead:
                    from_minus.append((to, rows_ahead[to]))
                elif to in rows_behind:
                    from_plus.append((to, rows_behind[to]))
                else:
                    outer.append((to, frm))
            for to, frm, count in runs(outer):
                space = "xy" if group == "xy" else "t"
                slot, row, end = free[space]
                free[space] = slot, row + count, end
                assert row + count <= end
                placed.append((to, slot, row, count))
                send(group, pair, 1, at * rows + frm, count, slot, row, step)
        corners[m, n_dir] = placed, runs(sorted(from_minus)), runs(sorted(from_plus))
    remote.sort(key=lambda item: SEND_ORDER.index(item[0]))
    return remote, fills, corners


def kernel(
    block,
    sizes,
    plan,
    partners,
    w_hbm,
    out_ref,
    act_ref,
    first_ref,
    cur_ref,
    halo_ref,
    gen_ref,
    gen_halo_ref,
    stack_ref,
    flux_ref,
    part_ref,
    slot_ref,
    send_sem,
    recv_sem,
    act_sem,
    load_sem,
):
    remote, fills, corners = plan
    rows = block[0] * block[1] * block[2]
    n = rows // block[0]
    lanes = w_hbm.shape[-1]
    here = [lax.axis_index(axis) for axis in AXES]

    def device(step):
        return tuple(lax.rem(here[k] + step[k] + sizes[k], sizes[k]) for k in range(3))

    steps = [item[-1] for item in remote] + partners
    greeted = sorted({tuple(s % size for s, size in zip(step, sizes)) for step in steps})
    barrier = pltpu.get_barrier_semaphore()
    for step in reversed(greeted):
        pl.semaphore_signal(barrier, inc=1, device_id=device(step), device_id_type=MESH)
    for d, (pair, pos) in PLACE.items():
        load = pltpu.make_async_copy(
            w_hbm.at[d], first_ref.at[pair, :, :, :, pl.ds(pos * rows, rows), :], load_sem.at[0]
        )
        load.start()
    pltpu.make_async_copy(first_ref, first_ref, load_sem.at[0]).wait()
    for pair in range(2):
        gen_ref[0, pair] = encode((first_ref[pair, 0], first_ref[pair, 1]))
    pl.semaphore_wait(barrier, len(greeted))

    units, stacks = {}, {}

    def wait_bytes(count, sem):
        depth = max(k for k in range(1, 2 * rows + 1) if count % k == 0 and count // k <= SLOTS)
        span = gen_halo_ref.at[0, pl.ds(0, count // depth), :, pl.ds(0, depth), :]
        pltpu.make_async_copy(span, span, sem).wait()

    def wait_sent(units, stage):
        for group, count in units.items():
            wait_bytes(count, send_sem.at[stage % 2, SEND_ORDER.index(group)])


    def low(pos):
        return slice(pos * rows, (pos + 1) * rows)

    def whole(ref, index):
        return ref[index, 0], ref[index, 1]

    def half(ref, index, pos):
        return ref[index, 0, :, :, low(pos), :], ref[index, 1, :, :, low(pos), :]

    def stack(name):
        return stacks.setdefault(name, len(stacks))

    def keep(name, value):
        index = stack(name)
        stack_ref[index, 0], stack_ref[index, 1] = value

    def keep_half(name, pos, value):
        index = stack(name)
        stack_ref[index, 0, :, :, low(pos), :] = value[0]
        stack_ref[index, 1, :, :, low(pos), :] = value[1]

    def twice(name, value):
        keep_half(name, 0, value)
        keep_half(name, 1, value)

    def kept(name):
        return whole(stack_ref, stacks[name])

    def kept_half(name, pos):
        return half(stack_ref, stacks[name], pos)

    def roll(pair, shift):
        return tuple(pltpu.roll(x, shift % lanes, axis=3) for x in pair)

    def face(k, side, d):
        pair, pos = PLACE[d]
        return half(halo_ref, (Y_AHEAD if side else BEHIND[k]) + pair, pos)

    def copy_rows(name, to, ref, index, frm, count):
        slot = stack(name)
        stack_ref[slot, :, :, :, to : to + count, :] = ref[index, :, :, :, frm : frm + count, :]

    for stage in range(3):
        base = first_ref if stage == 0 else cur_ref
        sent, units = units, {}
        for group, pair, pairs, frm, count, slot, to, step in remote:
            span, into = pl.ds(pair, pairs), pl.ds(slot, pairs)
            src = gen_ref.at[stage, span, :, pl.ds(frm, count), :]
            dst = gen_halo_ref.at[stage, into, :, pl.ds(to, count), :]
            copy = pltpu.make_async_remote_copy(
                src_ref=src,
                dst_ref=dst,
                send_sem=send_sem.at[stage % 2, SEND_ORDER.index(group)],
                recv_sem=recv_sem.at[stage % 2, SEND_ORDER.index(group)],
                device_id=device(tuple(-s for s in step)),
                device_id_type=MESH,
            )
            units[group] = units.get(group, 0) + pairs * count
            copy.start()

        if stage == 1:
            lt = block[2]
            for t in range(lt):
                part_ref[t : t + 1, :] = sum(action[r : r + 1] for r in range(t, rows, lt))
            mine = here[0] * sizes[1] + here[1]
            for step in partners:
                copy = pltpu.make_async_remote_copy(
                    src_ref=part_ref,
                    dst_ref=slot_ref.at[mine],
                    send_sem=act_sem.at[0],
                    recv_sem=act_sem.at[1],
                    device_id=device(step),
                    device_id_type=MESH,
                )
                copy.start()
            slot_ref[mine] = part_ref[...]

        def fill(wanted):
            for group, source, pair, frm, slot, to, count in fills:
                if group != wanted:
                    continue
                ref = gen_ref.at[stage, pair] if source is None else gen_halo_ref.at[stage, source]
                gen_halo_ref[stage, slot, :, to : to + count, :] = ref[:, frm : frm + count, :]

        def renew(slot, count=2 * rows):
            code = gen_halo_ref[stage, slot, :, 0:count, :]
            if stage == 0:
                new = decode(code)
            else:
                old = halo_ref[slot, :, :, :, 0:count, :]
                new = mul(exponential(code), (old[0], old[1]))
            halo_ref[slot, 0, :, :, 0:count, :] = new[0]
            halo_ref[slot, 1, :, :, 0:count, :] = new[1]

        def arrive(group, slots):
            if group in units:
                wait_bytes(units[group], recv_sem.at[stage % 2, SEND_ORDER.index(group)])
            fill(group)
            for slot in slots:
                renew(slot)

        def count_action(plaq):
            trace = plaq[0][0, 0] + plaq[0][1, 1] + plaq[0][2, 2]
            term = 1.0 - trace / 3.0
            return term if term.shape[0] == rows else term[:rows] + term[rows:]

        action_terms = []

        def flux_of(one, two):
            plaq = mul_right_adjoint(one, two)
            if stage == 0:
                action_terms.append(count_action(plaq))
            return projected(plaq)

        def centre(d):
            return half(base, *PLACE[d])

        if stage:
            for pair in range(2):
                before = whole(first_ref if stage == 1 else cur_ref, pair)
                moved = mul(exponential(gen_ref[stage, pair]), before)
                cur_ref[pair, 0], cur_ref[pair, 1] = moved
        for d, name in ((X, "x x"), (T, "t t"), (Z, "z z")):
            twice(name, centre(d))
        for d, name in ((X, "x ahead"), (T, "t ahead"), (Y, "y z ahead")):
            keep_half(name, 1, roll(centre(d), -1))

        for d, (pair, pos) in PLACE.items():
            for to, frm, count in local_runs(block, X, -1):
                copy_rows(("xb a", "xb b")[pair], pos * rows + to, base, pair, pos * rows + frm, count)
            if d == X:
                continue
            for to, frm, count in local_runs(block, X, 1):
                name, at = ("t x", 0) if d == T else ("xa yz", pos * rows)
                copy_rows(name, at + to, base, pair, pos * rows + frm, count)

        wait_sent(sent, stage - 1)
        arrive("y", range(BEHIND[Y], Y_AHEAD + 2))
        for d, name in ((X, "x ahead"), (T, "t ahead"), (Z, "y z ahead")):
            keep_half(name, 0, face(Y, 1, d))
        behind = face(Y, 0, Y)
        twice("y behind", behind)
        yz = whole(base, 1)
        keep("yx zx", mul(yz, kept("x ahead")))
        keep("yt zt", mul(yz, kept("t ahead")))
        keep("yz zy", mul(yz, kept("y z ahead")))
        one = kept_half("yz zy", 0)
        flux = flux_of(one, kept_half("yz zy", 1))
        flux_ref[1, :, low(0), :] = flux
        flux_ref[1, :, low(1), :] = -flux
        keep_half("lower b", 0, roll(mul_left_adjoint(one, centre(Z)), 1))
        one = mul(face(Y, 0, Z), roll(behind, -1))
        keep_half("lower b", 1, mul_left_adjoint(one, behind))

        def sum_into(name, value):
            keep(name, add(kept(name) if name in begun else None, value))
            begun.add(name)

        begun = {"lower b"}

        def x_faces():
            for slot in (X_PACK, X_PACK + 1):
                renew(slot)
            to = cover(sum((p for q, p in neighbour_rows(block, unit(X, 1)).items() if any(q)), []))[0]
            copy_rows("xa yz", to, halo_ref, X_PACK + 1, 2 * n, n)
            copy_rows("xa yz", rows + to, halo_ref, X_PACK + 1, 3 * n, n)
            copy_rows("t x", to, halo_ref, X_PACK, 3 * n, n)
            to = cover(sum((p for q, p in neighbour_rows(block, unit(X, -1)).items() if any(q)), []))[0]
            for pos in range(2):
                copy_rows("xb a", pos * rows + to, halo_ref, X_PACK, pos * n, n)
                copy_rows("xb b", pos * rows + to, halo_ref, X_PACK + 1, pos * n, n)
            keep("xy xz", mul(kept("x x"), kept("xa yz")))
            flux_ref[3] = flux_of(kept("xy xz"), kept("yx zx"))
            keep_half("xz tz", 0, kept_half("xy xz", 1))
            behind = kept_half("xb a", 0)
            twice("x behind", behind)
            keep_half("x corner", 1, roll(behind, -1))
            keep_half("behind n", 1, behind)
            keep_half("behind m", 1, kept_half("xb a", 1))

        def outer(name, at, m, n_dir):
            for to, slot, row, count in corners[m, n_dir][0]:
                copy_rows(name, at + to, halo_ref, slot, row, count)

        def inner(name, at, m, n_dir, minus, plus):
            for found, source in zip(corners[m, n_dir][1:], (minus, plus)):
                for to, frm, count in found:
                    copy_rows(name, at + to, source[0], source[1], source[2] + frm, count)

        def xy_corner():
            outer("y corner", 0, X, Y)
            outer("x corner", 0, Y, X)
            inner("y corner", 0, X, Y, (halo_ref, BEHIND[Y] + 1, 0), (stack_ref, stacks["xa yz"], 0))
            inner("x corner", 0, Y, X, (stack_ref, stacks["xb a"], 0), (halo_ref, Y_AHEAD, 0))
            one = mul(kept("xb b"), kept("x corner"))
            sum_into("lower b", mul_left_adjoint(one, kept("x behind")))

        def t_ahead():
            renew(T_AHEAD)
            renew(MIXED, rows)
            keep("ty tz", mul(kept("t t"), whole(halo_ref, T_AHEAD)))
            flux_ref[2] = flux_of(kept("ty tz"), kept("yt zt"))
            keep_half("xz tz", 1, kept_half("ty tz", 1))
            keep_half("t x", 1, half(halo_ref, MIXED, 0))
            inner("y corner", rows, T, Y, None, (halo_ref, T_AHEAD, 0))
            inner("xt corner", rows, T, X, None, (halo_ref, MIXED, 0))

        def x_and_t_ahead():
            keep("xt tx", mul(whole(base, 0), kept("t x")))
            flux = flux_of(kept_half("xt tx", 0), kept_half("xt tx", 1))
            flux_ref[0, :, low(0), :] = flux_ref[3, :, low(0), :] + flux_ref[3, :, low(1), :] + flux
            flux_ref[0, :, low(1), :] = flux_ref[2, :, low(0), :] + flux_ref[2, :, low(1), :] - flux
            flux_ref[1] = flux_ref[1] - flux_ref[2] - flux_ref[3]
            sum_into("lower a", roll(mul_left_adjoint(kept("xz tz"), kept("z z")), 1))

        def t_behind():
            renew(BEHIND[T])
            behind = face(T, 0, T)
            twice("t behind", behind)
            keep_half("t corner", 1, roll(behind, -1))
            keep_half("behind n", 0, behind)
            keep_half("behind m", 0, face(T, 0, X))
            inner("t corner", 0, Y, T, (halo_ref, BEHIND[T], rows), None)
            inner("xt corner", 0, X, T, (halo_ref, BEHIND[T], rows), None)

        def t_corners():
            renew(XT)
            outer("y corner", rows, T, Y)
            outer("t corner", 0, Y, T)
            outer("xt corner", 0, X, T)
            outer("xt corner", rows, T, X)

        def y_lower():
            one = mul(whole(halo_ref, BEHIND[Y]), kept("y corner"))
            sum_into("lower a", mul_left_adjoint(one, kept("y behind")))

        def t_lower():
            renew(BEHIND[T] + 1)
            one = mul(whole(halo_ref, BEHIND[T] + 1), kept("t corner"))
            sum_into("lower b", mul_left_adjoint(one, kept("t behind")))

        def xt_lower():
            one = mul(kept("behind m"), kept("xt corner"))
            sum_into("lower a", mul_left_adjoint(one, kept("behind n")))

        def finish(pair, name):
            own = whole(base, pair)
            omega = projected(mul(own, kept(name))) + flux_ref[pair]
            gen = (-flow_eps * FRESH[stage]) * omega
            if stage:
                gen = gen + KEPT[stage] * gen_ref[stage, pair]
            if stage < 2:
                gen_ref[stage + 1, pair] = gen
            else:
                keep("moved", mul(exponential(gen), own))
                for d, (p, pos) in PLACE.items():
                    if p == pair:
                        out_ref[d, 0], out_ref[d, 1] = kept_half("moved", pos)

        late = {"x", "xy", "ahead", "behind a", "behind b", "yt", "xt"}
        tasks = [
            (t_ahead, {"ahead"}),
            (x_faces, {"x", "xy"}),
            (x_and_t_ahead, {"x", "xy", "ahead"}),
            (xy_corner, {"x", "xy"}),
            (t_behind, {"behind a", "ahead"}),
            (t_corners, {"yt", "xt"}),
            (y_lower, late - {"behind b"}),
            (xt_lower, late - {"behind b"}),
            (lambda: finish(0, "lower a"), late - {"behind b"}),
            (t_lower, late),
            (lambda: finish(1, "lower b"), late),
        ]
        here_now = set()
        for groups in ORDER[stage]:
            for group in groups:
                arrive(group, ())
                here_now.add(group)
            ready = [task for task, needs in tasks if needs <= here_now]
            tasks = [(task, needs) for task, needs in tasks if not needs <= here_now]
            for task in ready:
                task()
        assert not tasks
        if stage == 0:
            action = sum(action_terms)
    assert len(stacks) <= stack_ref.shape[0]
    wait_sent(units, 2)
    for k in range(2 if partners else 0):
        span = slot_ref.at[pl.ds(0, len(partners))]
        pltpu.make_async_copy(span, span, act_sem.at[k]).wait()
    total = sum(slot_ref[j] for j in range(sizes[0] * sizes[1]))
    scale = 1.0 / (6.0 * sizes[0] * sizes[1] * block[0] * block[1] * lanes)
    total = jnp.sum(total, axis=1, keepdims=True) * scale
    act_ref[...] = jnp.broadcast_to(total, act_ref.shape)


STACKS = 30
STEPS = (("ahead",), ("x", "xy"), ("behind a", "yt", "xt"), ("behind b",))
ORDER = (STEPS, STEPS, STEPS)
VMEM_LIMIT = 55000 * 1024


def solution(mesh):
    sizes = tuple(mesh.shape[axis] for axis in AXES)

    def local(links):
        block = links.shape[4:7]
        lanes = links.shape[7]
        rows = block[0] * block[1] * block[2]
        plan = plan_of(block)
        partners = [
            (i, j, 0) for i in range(sizes[0]) for j in range(sizes[1]) if i or j
        ]
        matrix = (2, 3, 3, rows, lanes)
        both = (2, 3, 3, 2 * rows, lanes)
        f32 = jnp.float32
        vmem = pl.BlockSpec(memory_space=pltpu.VMEM)
        flowed, action = pl.pallas_call(
            functools.partial(kernel, block, sizes, plan, partners),
            out_shape=(
                jax.ShapeDtypeStruct((4,) + matrix, f32),
                jax.ShapeDtypeStruct((block[2], lanes), f32),
            ),
            in_specs=[pl.BlockSpec(memory_space=pltpu.HBM)],
            out_specs=(vmem, vmem),
            scratch_shapes=[
                pltpu.VMEM((2,) + both, f32),
                pltpu.VMEM((2,) + both, f32),
                pltpu.VMEM((SLOTS,) + both, f32),
                pltpu.VMEM((3, 2, 8, 2 * rows, lanes), f32),
                pltpu.VMEM((3, SLOTS, 8, 2 * rows, lanes), f32),
                pltpu.VMEM((STACKS,) + both, f32),
                pltpu.VMEM((4, 8, 2 * rows, lanes), f32),
                pltpu.VMEM((block[2], lanes), f32),
                pltpu.VMEM((sizes[0] * sizes[1], block[2], lanes), f32),
                pltpu.SemaphoreType.DMA((2, len(SEND_ORDER))),
                pltpu.SemaphoreType.DMA((2, len(SEND_ORDER))),
                pltpu.SemaphoreType.DMA((2,)),
                pltpu.SemaphoreType.DMA((1,)),
            ],
            compiler_params=pltpu.CompilerParams(
                collective_id=0, has_side_effects=True, vmem_limit_bytes=VMEM_LIMIT
            ),
        )(links.reshape((4,) + matrix))
        return flowed.reshape(links.shape), action[:, 0]

    spec = P(None, None, None, None, "gx", "gy", "ta", None)
    return jax.shard_map(
        local, mesh=mesh, in_specs=(spec,), out_specs=(spec, P("ta")), check_vma=False
    )
```
